32 devices in a mesh: comp: 2 (over core), blk: 16 (over z, y, x).
Axes of the slice: x: 2, y: 2, z: 4, core: 2. Of those that a mesh axis runs over, the one named last changes fastest.
Arguments:
- initial: float32 [2, 5, 128, 2048], P('comp', None, 'blk'), may hold values from -3 to 3
- ice_forcing: float32 [5, 128, 2048], P(None, 'blk'), may hold values from -2 to 4, as said below
- ocean_current: float32 [2, 128, 2048], P(None, 'blk'), may hold values from -1 to 1
- ice_cover: int32 [128, 2048], P('blk'), may hold values from 0 to 1, as said below
- targets: int32 [2, 128, 2048], P(None, 'blk'), may hold values from 0 to 32767, as said below
- weights: int32 [2, 128, 2048], P(None, 'blk'), may hold values from 1 to 4
Outputs:
- state_out: float32 [2, 5, 128, 2048], P('comp', None, 'blk')
- coupled: float32 [2, 3, 128, 2048], P('comp', None, 'blk')
The draws below stay inside these ranges and needn't reach their ends.
Inputs may be any that keep to these rules, and one draw needn't show every extreme that they name: `ice_forcing`: channel 0 (mass) lies in 0.5 to 4, channel 1 (strength) and channel 4 (melt rate) in 0.2 to 2, channels 2 and 3 (wind stress) in -2 to 2. `ice_cover`: the share of ice-covered cells differs from strip to strip of 8 rows. `targets`: an entry of an ice cell at row r of its strip names an ocean row of the window no earlier than r.
All inputs are finite; a program needn't handle non-finite values.
Results may differ from the reference program's by a relative error of at most 0.0003.
Values sent between devices are 32-bit elements; how exact they have to be, the bound alone decides.
A program may use at most 128 MiB of HBM per device.

```python
import math
import jax
import jax.numpy as jnp
from jax import lax

CX = 8
NY = 2048
SUBCYCLES = 16
INTERSECTIONS = 2
NX = 128


def smooth_field(key, channels):
    row_pos = jnp.arange(NX, dtype=jnp.float32)[None, :, None]
    col_pos = jnp.arange(NY, dtype=jnp.float32)[None, None, :]
    summed = jnp.zeros((channels, NX, NY), jnp.float32)
    for wave_index in range(3):
        wave_key = jax.random.fold_in(key, 100 + wave_index)
        picks = jax.random.uniform(wave_key, (3, channels), jnp.float32)
        row_length = jnp.exp(math.log(48.0) + (math.log(160.0) - math.log(48.0)) * picks[0])[:, None, None]
        col_length = jnp.exp(math.log(32.0) + (math.log(512.0) - math.log(32.0)) * picks[1])[:, None, None]
        summed = summed + jnp.sin(2.0 * math.pi * (row_pos / row_length + col_pos / col_length + picks[2][:, None, None]))
    return summed / 2.0


def draw_initial(key, part):
    smooth = smooth_field(jax.random.fold_in(key, 31), 10).reshape(2, 5, NX, NY)
    noise = jax.random.normal(jax.random.fold_in(key, 32), (2, 5, NX, NY), jnp.float32)
    values = 0.8 * smooth + 0.35 * noise
    return jnp.clip(values, -3.0, 3.0).astype(jnp.float32)


def draw_ice_forcing(key, part):
    shape = (NX, NY)
    keys = jax.random.split(key, 5)
    smooth = smooth_field(jax.random.fold_in(key, 51), 2)
    mass = jnp.exp(jax.random.uniform(keys[0], shape, jnp.float32, math.log(0.5), math.log(4.0)))
    strength = jnp.exp(jax.random.uniform(keys[1], shape, jnp.float32, math.log(0.2), math.log(2.0)))
    wind_x = jnp.clip(0.6 * smooth[0] + 0.3 * jax.random.normal(keys[2], shape, jnp.float32), -2.0, 2.0)
    wind_y = jnp.clip(0.6 * smooth[1] + 0.3 * jax.random.normal(keys[3], shape, jnp.float32), -2.0, 2.0)
    melt = jnp.exp(jax.random.uniform(keys[4], shape, jnp.float32, math.log(0.2), math.log(2.0)))
    return jnp.stack([mass, strength, wind_x, wind_y, melt]).astype(jnp.float32)


def draw_ocean_current(key, part):
    smooth = smooth_field(jax.random.fold_in(key, 41), 2)
    noise = jax.random.uniform(jax.random.fold_in(key, 42), (2, NX, NY), jnp.float32, -1.0, 1.0)
    along = 0.6 * jnp.tanh(3.0 * smooth[0]) + 0.35 * noise[0]
    sideways = 0.5 * smooth[1] + 0.4 * noise[1]
    return jnp.clip(jnp.stack([along, sideways]), -1.0, 1.0).astype(jnp.float32)


def draw_ice_cover(key, part):
    level = jnp.minimum(jax.random.randint(jax.random.fold_in(key, 11), (NX // CX,), 0, 24), 8)
    cells = jax.random.randint(jax.random.fold_in(key, 12), (NX, NY), 0, 8)
    strip = jnp.arange(NX, dtype=jnp.int32) // CX
    return (cells < level[strip][:, None]).astype(jnp.int32)


def draw_targets(key, part):
    offset = jax.random.randint(jax.random.fold_in(key, 21), (INTERSECTIONS, NX, NY), 0, CX + 1)
    jitter = jax.random.randint(jax.random.fold_in(key, 22), (INTERSECTIONS, NX, NY), -2, 3)
    local_row = (jnp.arange(NX, dtype=jnp.int32) % CX)[None, :, None]
    column = jnp.arange(NY, dtype=jnp.int32)[None, None, :]
    return ((local_row + offset) * NY + (column + jitter) % NY).astype(jnp.int32)


def with_ends(array, stream_key, least, high):
    place = [jax.random.randint(jax.random.fold_in(stream_key, axis), (), 0, length) for axis, length in enumerate(array.shape)]
    main_axis = array.shape.index(max(array.shape))
    beside = place[:main_axis] + [(place[main_axis] + 1) % array.shape[main_axis]] + place[main_axis + 1:]
    return array.at[tuple(place)].set(least).at[tuple(beside)].set(high)


def setup_inputs(seed: int = 0) -> dict:
    key_list = jax.random.split(jax.random.key(seed), 7)
    initial = draw_initial(jax.random.fold_in(key_list[6], 71), 0)
    ice_forcing = draw_ice_forcing(jax.random.fold_in(key_list[6], 71), 0)
    ocean_current = draw_ocean_current(jax.random.fold_in(key_list[6], 71), 0)
    ice_cover = draw_ice_cover(jax.random.fold_in(key_list[6], 71), 0)
    targets = draw_targets(jax.random.fold_in(key_list[6], 71), 0)
    weights = with_ends(jax.random.randint(key_list[5], (INTERSECTIONS, NX, NY), 1, 5), jax.random.fold_in(key_list[5], 1), 1, 4).astype(jnp.int32)
    return dict(initial=initial, ice_forcing=ice_forcing, ocean_current=ocean_current, ice_cover=ice_cover, targets=targets, weights=weights)


relax_rate = 0.5
ecc_sq = 4.0
delta_floor = 0.1
coriolis = 0.1
drag_coef = 1.0
inertia = 4.0
courant = 0.2
dilution = 0.5
weight_norm = 4.0
level_speed = (1.0, 0.8, 0.6, 0.45, 0.3)

def along_rows(field):
    return 0.5 * (field[..., 2:, :] - field[..., :-2, :])

def across(field):
    padded = jnp.pad(field, [(0, 0)] * (field.ndim - 1) + [(1, 1)])
    return 0.5 * (padded[..., 2:] - padded[..., :-2])

def ice_step(fields, forcing, current, covered):
    vel_x = fields[0]
    vel_y = fields[1]
    strain_d = along_rows(vel_x) + across(vel_y[1:-1])
    strain_t = along_rows(vel_x) - across(vel_y[1:-1])
    strain_s = across(vel_x[1:-1]) + along_rows(vel_y)
    delta = jnp.sqrt(strain_d * strain_d + (strain_t * strain_t + strain_s * strain_s) / ecc_sq + delta_floor * delta_floor)
    press = forcing[1, 1:-1] * covered[1:-1]
    sig_one = (fields[2, 1:-1] + relax_rate * press * (strain_d / delta - 1.0)) / (1.0 + relax_rate)
    sig_two = (fields[3, 1:-1] + relax_rate * press * strain_t / (ecc_sq * delta)) / (1.0 + relax_rate)
    sig_shear = (fields[4, 1:-1] + relax_rate * press * strain_s / (2.0 * ecc_sq * delta)) / (1.0 + relax_rate)
    sig_xx = 0.5 * (sig_one + sig_two)
    sig_yy = 0.5 * (sig_one - sig_two)
    force_x = along_rows(sig_xx) + across(sig_shear[1:-1])
    force_y = along_rows(sig_shear) + across(sig_yy[1:-1])
    beta = inertia * forcing[0, 2:-2]
    old_x = vel_x[2:-2]
    old_y = vel_y[2:-2]
    denom = beta + drag_coef
    new_x = covered[2:-2] * (beta * old_x + coriolis * beta * old_y + force_x + forcing[2, 2:-2] + drag_coef * current[0, 2:-2]) / denom
    new_y = covered[2:-2] * (beta * old_y - coriolis * beta * old_x + force_y + forcing[3, 2:-2] + drag_coef * current[1, 2:-2]) / denom
    return jnp.stack([new_x, new_y, sig_one[1:-1], sig_two[1:-1], sig_shear[1:-1]])

def ocean_step(tracer, current):
    speed = jnp.asarray(level_speed, jnp.float32)[:, None, None]
    centre = tracer[:, 2:-2]
    below = centre - tracer[:, 1:-3]
    above = tracer[:, 3:-1] - centre
    padded = jnp.pad(centre, ((0, 0), (0, 0), (1, 1)))
    left_diff = centre - padded[:, :, :-2]
    right_diff = padded[:, :, 2:] - centre
    speed_x = speed * current[0, 2:-2][None]
    speed_y = speed * current[1, 2:-2][None]
    change = jnp.maximum(speed_x, 0.0) * below + jnp.minimum(speed_x, 0.0) * above + jnp.maximum(speed_y, 0.0) * left_diff + jnp.minimum(speed_y, 0.0) * right_diff
    return centre - courant * change

def coupling_terms(fields, forcing, current, covered):
    stress_x = covered * drag_coef * (fields[0] - current[0])
    stress_y = covered * drag_coef * (fields[1] - current[1])
    fresh = forcing[4] * covered * jnp.sqrt(1.0 + fields[0] * fields[0] + fields[1] * fields[1])
    return jnp.stack([stress_x, stress_y, fresh])

def pad_rows(values):
    return jnp.pad(values, [(0, 0)] * (values.ndim - 2) + [(2, 2), (0, 0)])

def reference(initial, ice_forcing, ocean_current, ice_cover, targets, weights):
    covered = ice_cover.astype(jnp.float32)
    forcing_pad = pad_rows(ice_forcing)
    current_pad = pad_rows(ocean_current)
    cover_pad = pad_rows(covered)

    def one_turn(carry, unused):
        ice_fields, salinity, total = carry
        ice_fields = ice_step(pad_rows(ice_fields), forcing_pad, current_pad, cover_pad)
        salinity = ocean_step(pad_rows(salinity), current_pad)
        total = total + coupling_terms(ice_fields, ice_forcing, ocean_current, covered)
        return ((ice_fields, salinity, total), None)
    start = (initial[0], initial[1], jnp.zeros((3, NX, NY), jnp.float32))
    (ice_fields, salinity, total), unused = lax.scan(one_turn, start, None, length=SUBCYCLES)
    average = total / SUBCYCLES
    row_index = jnp.arange(NX, dtype=jnp.int32)[:, None]
    base = row_index // CX * (CX * NY)
    glob = (targets + base[None]) % (NX * NY)
    scaled = weights.astype(jnp.float32) / weight_norm
    flat_glob = glob.reshape(-1)

    def spread(single):
        return jax.ops.segment_sum((single[None] * scaled).reshape(-1), flat_glob, num_segments=NX * NY)
    flux = jax.vmap(spread)(average).reshape(3, NX, NY)
    salinity = jnp.concatenate([salinity[:1] - dilution * flux[2][None], salinity[1:]], axis=0)
    state_out = jnp.stack([ice_fields, salinity])
    coupled = jnp.stack([average, flux])
    return (state_out, coupled)
```

```python
import functools

import jax
import jax.numpy as jnp
from jax import lax
from jax.experimental import pallas as pl
from jax.experimental.pallas import tpu as pltpu
from jax.sharding import PartitionSpec as P

SUBCYCLES = 16
MESH = pl.DeviceIdType.MESH
PAD = 128
PARTS = 2

coriolis = 0.1
inertia = 4.0
courant = 0.2
dilution = 0.5
weight_norm = 4.0
level_speed = (1.0, 0.8, 0.6, 0.45, 0.3)


def rolled(value, steps, axis):
    return pltpu.roll(value, steps % value.shape[axis], axis)


def rows_diff(value):
    return rolled(value, -1, 0) - rolled(value, 1, 0)


def chunk_width(cols):
    return 256 if cols % 256 == 0 else 128


def stress_stage(work, stat, start, width):
    wide = pl.ds(start, width + 2 * PAD)
    mid = pl.ds(start + PAD, width)
    inner = slice(PAD, PAD + width)
    vel_x, vel_y = work[0, :, wide], work[1, :, wide]
    cx = (rolled(vel_x, -1, 1) - rolled(vel_x, 1, 1))[:, inner]
    cy = (rolled(vel_y, -1, 1) - rolled(vel_y, 1, 1))[:, inner]
    rx = rows_diff(vel_x[:, inner])
    ry = rows_diff(vel_y[:, inner])
    e_d = rx + cy
    e_t = rx - cy
    e_s = cx + ry
    inv = lax.rsqrt(0.25 * (e_d * e_d) + 0.0625 * (e_t * e_t + e_s * e_s) + 0.01)
    third = stat[0, :, pl.ds(start, width)]
    scaled = third * inv
    work[2, :, mid] = work[2, :, mid] * (2.0 / 3.0) + (0.5 * scaled * e_d - third)
    work[3, :, mid] = work[3, :, mid] * (2.0 / 3.0) + 0.125 * scaled * e_t
    work[4, :, mid] = work[4, :, mid] * (2.0 / 3.0) + 0.0625 * scaled * e_s


def velocity_stage(work, stat, total, start, width, rows):
    wide = pl.ds(start, width + 2 * PAD)
    mid = pl.ds(start + PAD, width)
    here = pl.ds(start, width)
    inner = slice(PAD, PAD + width)
    shear = work[4, :, wide]
    one, two = work[2, :, wide], work[3, :, wide]
    across_shear = (rolled(shear, -1, 1) - rolled(shear, 1, 1))[:, inner]
    lower = one - two
    across_yy = (rolled(lower, -1, 1) - rolled(lower, 1, 1))[:, inner]
    force_x = rows_diff((one + two)[:, inner]) + 2.0 * across_shear
    force_y = 2.0 * rows_diff(shear[:, inner]) + across_yy
    old_x, old_y = work[0, :, mid], work[1, :, mid]
    keep, push = stat[1, :, here], stat[2, :, here]
    new_x = keep * (old_x + coriolis * old_y) + push * force_x + stat[3, :, here]
    new_y = keep * (old_y - coriolis * old_x) + push * force_y + stat[4, :, here]
    work[0, :, mid] = new_x
    work[1, :, mid] = new_y
    own_x, own_y = new_x[rows : 2 * rows], new_y[rows : 2 * rows]
    total[0, :, here] += own_x
    total[1, :, here] += own_y
    total[2, :, here] += jnp.sqrt(1.0 + own_x * own_x + own_y * own_y)


def ocean_stage(source, target, coef, start, width):
    wide = pl.ds(start, width + 2 * PAD)
    mid = pl.ds(start + PAD, width)
    here = pl.ds(start, width)
    inner = slice(PAD, PAD + width)
    up, down, east, west = (coef[i, :, here] for i in range(4))
    for level, speed in enumerate(level_speed):
        tracer = source[level, :, wide]
        centre = tracer[:, inner]
        right = rolled(tracer, -1, 1)[:, inner] - centre
        left = centre - rolled(tracer, 1, 1)[:, inner]
        above = rolled(centre, -1, 0) - centre
        below = centre - rolled(centre, 1, 0)
        change = up * below + down * above + east * left + west * right
        target[level, :, mid] = centre - speed * change


def turns_kernel(
    initial_in, forcing_in, current_in, cover_in, state, average,
    initial, forcing, current, cover,
    own, own_stat, halo, halo_stat, work, spare, stat, total, mean,
    load, near_send, near_recv, far_send, far_recv,
    stat_near_send, stat_near_recv, stat_far_send, stat_far_recv,
    mean_send, mean_recv, go,
):
    me = lax.axis_index("blk")
    comp = lax.axis_index("comp")
    count = lax.axis_size("blk")
    fields, rows, cols = initial.shape
    width = chunk_width(cols)
    chunks = cols // width
    near = 1 - lax.rem(me, 2)
    far = 1 - near
    partner = me + 2 * near - 1
    relay_to = me + 4 * near - 2
    relay_from = me - 4 * near + 2
    can_send = jnp.logical_and(relay_to >= 0, relay_to < count)
    can_recv = jnp.logical_and(relay_from >= 0, relay_from < count)
    relay_to = lax.rem(relay_to + count, count)
    relay_from = lax.rem(relay_from + count, count)

    barrier = pltpu.get_barrier_semaphore()

    def greet(where):
        pl.semaphore_signal(barrier, inc=1, device_id=where, device_id_type=MESH)

    greet({"blk": partner})
    greet({"comp": 1 - comp})
    pl.when(can_send)(lambda: greet({"blk": relay_to}))
    pl.when(can_recv)(lambda: greet({"blk": relay_from}))
    loads = [
        pltpu.make_async_copy(source, target, load.at[i])
        for i, (source, target) in enumerate(
            (
                (initial_in, initial),
                (current_in, current),
                (forcing_in, forcing),
                (cover_in, cover),
            )
        )
    ]
    for copy in loads:
        copy.start()

    work[...] = jnp.zeros_like(work)
    total[...] = jnp.zeros_like(total)

    def enter():
        pl.semaphore_wait(barrier, 2 + can_send.astype(jnp.int32) + can_recv.astype(jnp.int32))

    def copies(source, target, pieces, near_sems, far_sems):
        first, second = [], []
        wide = cols // PARTS
        for index in range(pieces * PARTS):
            piece, place = index // PARTS, pl.ds(index % PARTS * wide, wide)
            first.append(
                pltpu.make_async_remote_copy(
                    source.at[piece, :, place], target.at[far, piece, :, place],
                    near_sems[0].at[index], near_sems[1].at[index],
                    device_id={"blk": partner}, device_id_type=MESH,
                )
            )
            second.append(
                pltpu.make_async_remote_copy(
                    target.at[near, piece, :, place], target.at[far, piece, :, place],
                    far_sems[0].at[index], far_sems[1].at[index],
                    device_id={"blk": relay_to}, device_id_type=MESH,
                )
            )
        return first, second

    def start(pair):
        for copy in pair[0]:
            copy.start()

    def relay(pair):
        for first, second in zip(*pair):
            first.wait_recv()
            pl.when(can_send)(second.start)

    def arrive(pair):
        @pl.when(can_recv)
        def _():
            for copy in pair[1]:
                copy.wait_recv()

    def sent(pair):
        for copy in pair[0]:
            copy.wait_send()

        @pl.when(can_send)
        def _():
            for copy in pair[1]:
                copy.wait_send()

    def clear_edges(turns):
        @pl.when(jnp.logical_not(can_recv))
        def _():
            halo_stat[far] = jnp.zeros(halo_stat.shape[1:], jnp.float32)
            for turn in range(turns):
                halo[turn, far] = jnp.zeros(halo.shape[2:], jnp.float32)

    inside = slice(PAD, PAD + cols)

    def fill_own(source):
        for field in range(fields):
            work[field, rows : 2 * rows, inside] = source[field]

    def fill_sides(turn):
        for field in range(fields):
            work[field, 0:rows, inside] = halo[turn, 0, field]
            work[field, 2 * rows : 3 * rows, inside] = halo[turn, 1, field]

    def exchange_of(turn, source):
        return copies(
            source, halo.at[turn], fields,
            (near_send.at[turn], near_recv.at[turn]), (far_send.at[turn], far_recv.at[turn]),
        )

    def stats_of(source, pieces):
        return copies(
            source, halo_stat, pieces,
            (stat_near_send, stat_near_recv), (stat_far_send, stat_far_recv),
        )

    mean_copy = pltpu.make_async_remote_copy(
        mean, average, mean_send, mean_recv,
        device_id={"comp": 1 - comp}, device_id_type=MESH,
    )

    @pl.when(comp == 0)
    def _():
        depth = rows // 2
        turns = SUBCYCLES // depth
        clear_edges(turns)
        loads[0].wait()
        enter()
        pairs = [exchange_of(0, initial)]
        start(pairs[0])
        for copy in loads[1:]:
            copy.wait()
        covered = cover[...].astype(jnp.float32)
        push = covered / (inertia * forcing[0] + 1.0)
        own_stat[0] = forcing[1] * covered * (1.0 / 3.0)
        own_stat[1] = push
        own_stat[2] = push * (forcing[2] + current[0])
        own_stat[3] = push * (forcing[3] + current[1])
        stat_pair = stats_of(own_stat, 4)
        start(stat_pair)
        for turn in range(turns):
            source = initial if turn == 0 else own.at[turn - 1]
            if turn > 0:
                pairs.append(exchange_of(turn, source))
                start(pairs[turn])
            relay(pairs[turn])
            if turn == 0:
                relay(stat_pair)
                pl.semaphore_signal(
                    go, inc=1, device_id={"comp": 1 - comp}, device_id_type=MESH
                )
            fill_own(source)
            arrive(pairs[turn])
            if turn == 0:
                arrive(stat_pair)
                for place, block in enumerate((halo_stat.at[0], own_stat, halo_stat.at[1])):
                    span = slice(place * rows, (place + 1) * rows)
                    push = block[1]
                    stat[0, span] = block[0]
                    stat[1, span] = jnp.where(push > 0.0, 1.0 - push, 0.0)
                    stat[2, span] = 0.25 * push
                    stat[3, span] = block[2]
                    stat[4, span] = block[3]
            fill_sides(turn)

            def subcycle(step, carry):
                for chunk in range(chunks):
                    stress_stage(work, stat, chunk * width, width)
                for chunk in range(chunks):
                    velocity_stage(work, stat, total, chunk * width, width, rows)
                return carry

            lax.fori_loop(0, depth, subcycle, 0)
            final = state if turn == turns - 1 else own.at[turn]
            for field in range(fields):
                final[field] = work[field, rows : 2 * rows, inside]
        share = 1.0 / SUBCYCLES
        covered = cover[...].astype(jnp.float32)
        mean[0] = total[0] * share - covered * current[0]
        mean[1] = total[1] * share - covered * current[1]
        mean[2] = forcing[4] * covered * (total[2] * share)
        mean_copy.start()
        average[...] = mean[...]
        sent(stat_pair)
        for pair in pairs:
            sent(pair)
        mean_copy.wait_send()

    @pl.when(comp == 1)
    def _():
        depth = rows
        turns = SUBCYCLES // depth
        clear_edges(turns)
        spare[...] = jnp.zeros_like(spare)
        for copy in loads:
            copy.wait()
        enter()
        pl.semaphore_wait(go, 1)
        pairs = [exchange_of(0, initial)]
        start(pairs[0])
        stat_pair = stats_of(current, 2)
        start(stat_pair)
        for turn in range(turns):
            source = initial if turn == 0 else own.at[turn - 1]
            if turn > 0:
                pairs.append(exchange_of(turn, source))
                start(pairs[turn])
            relay(pairs[turn])
            if turn == 0:
                relay(stat_pair)
            fill_own(source)
            arrive(pairs[turn])
            if turn == 0:
                arrive(stat_pair)
                for place in range(3):
                    span = slice(place * rows, (place + 1) * rows)
                    for axis in range(2):
                        if place == 1:
                            speed = current[axis]
                        else:
                            speed = halo_stat[place // 2, axis]
                        stat[2 * axis, span] = courant * jnp.maximum(speed, 0.0)
                        stat[2 * axis + 1, span] = courant * jnp.minimum(speed, 0.0)
            fill_sides(turn)

            def substeps(step, carry):
                for chunk in range(chunks):
                    ocean_stage(work, spare, stat, chunk * width, width)
                for chunk in range(chunks):
                    ocean_stage(spare, work, stat, chunk * width, width)
                return carry

            lax.fori_loop(0, depth // 2, substeps, 0)
            final = state if turn == turns - 1 else own.at[turn]
            for field in range(fields):
                final[field] = work[field, rows : 2 * rows, inside]
        sent(stat_pair)
        for pair in pairs:
            sent(pair)
        mean_copy.wait_recv()


def run_turns(initial, forcing, current, cover):
    fields, rows, cols = initial.shape
    most = SUBCYCLES // (rows // 2)
    f32 = jnp.float32
    vmem = pl.BlockSpec(memory_space=pltpu.VMEM)
    dma = pltpu.SemaphoreType.DMA
    return pl.pallas_call(
        turns_kernel,
        out_shape=(
            jax.ShapeDtypeStruct((fields, rows, cols), f32),
            jax.ShapeDtypeStruct((3, rows, cols), f32),
        ),
        in_specs=[pl.BlockSpec(memory_space=pl.ANY)] * 4,
        out_specs=(vmem, vmem),
        scratch_shapes=[
            pltpu.VMEM(initial.shape, f32),
            pltpu.VMEM(forcing.shape, f32),
            pltpu.VMEM(current.shape, f32),
            pltpu.VMEM(cover.shape, cover.dtype),
            pltpu.VMEM((most, fields, rows, cols), f32),
            pltpu.VMEM((4, rows, cols), f32),
            pltpu.VMEM((most, 2, fields, rows, cols), f32),
            pltpu.VMEM((2, 4, rows, cols), f32),
            pltpu.VMEM((fields, 3 * rows, cols + 2 * PAD), f32),
            pltpu.VMEM((fields, 3 * rows, cols + 2 * PAD), f32),
            pltpu.VMEM((5, 3 * rows, cols), f32),
            pltpu.VMEM((3, rows, cols), f32),
            pltpu.VMEM((3, rows, cols), f32),
            dma((4,)),
            *[dma((most, fields * PARTS)) for _ in range(4)],
            *[dma((4 * PARTS,)) for _ in range(4)],
            dma, dma, pltpu.SemaphoreType.REGULAR,
        ],
        compiler_params=pltpu.CompilerParams(
            collective_id=0, has_side_effects=True
        ),
        name="turns",
    )(initial, forcing, current, cover)


LANES = 128
LEAD = 8
ICE_REACH = 2 * SUBCYCLES
SEA_REACH = SUBCYCLES


def fits_tiles(count, rows, cols):
    return count * rows == LANES and cols == count * LANES and count > 1


def lane_index(shape):
    return lax.broadcasted_iota(jnp.int32, shape, len(shape) - 1)


def lane_diff(value):
    lane = lane_index(value.shape)
    after = jnp.where(lane == LANES - 1, 0.0, pltpu.roll(value, LANES - 1, 1))
    before = jnp.where(lane == 0, 0.0, pltpu.roll(value, 1, 1))
    return after - before


def tile_stress(work, stat, low, size):
    here, up, down = (pl.ds(low + shift, size) for shift in (0, 1, -1))
    vel_x, vel_y = work[0, here], work[1, here]
    cx = work[0, up] - work[0, down]
    cy = work[1, up] - work[1, down]
    rx, ry = lane_diff(vel_x), lane_diff(vel_y)
    e_d = rx + cy
    e_t = rx - cy
    e_s = cx + ry
    inv = lax.rsqrt(0.25 * (e_d * e_d) + 0.0625 * (e_t * e_t + e_s * e_s) + 0.01)
    third = stat[0, here]
    scaled = third * inv
    one = 0.5 * scaled * e_d - third
    two = 0.125 * scaled * e_t
    work[2, here] = work[2, here] * (2.0 / 3.0) + (one + two)
    work[3, here] = work[3, here] * (2.0 / 3.0) + (one - two)
    work[4, here] = work[4, here] * (2.0 / 3.0) + 0.0625 * scaled * e_s


def tile_velocity(work, stat, total, low, size, own):
    here, up, down = (pl.ds(low + shift, size) for shift in (0, 1, -1))
    force_x = lane_diff(work[2, here]) + 2.0 * (work[4, up] - work[4, down])
    force_y = 2.0 * lane_diff(work[4, here]) + (work[3, up] - work[3, down])
    old_x, old_y = work[0, here], work[1, here]
    keep, push = stat[1, here], stat[2, here]
    new_x = keep * (old_x + coriolis * old_y) + push * force_x + stat[3, here]
    new_y = keep * (old_y - coriolis * old_x) + push * force_y + stat[4, here]
    work[0, here] = new_x
    work[1, here] = new_y
    if own is not None:
        place = pl.ds(own, size)
        total[0, place] += new_x
        total[1, place] += new_y
        square = 1.0 + new_x * new_x + new_y * new_y
        total[2, place] += square * lax.rsqrt(square)


def tile_ocean(source, target, stat, low, size):
    here, up, down = (pl.ds(low + shift, size) for shift in (0, 1, -1))
    before, after, left, right, drain = (stat[i, here] for i in range(5))
    for level, speed in enumerate(level_speed):
        centre = source[level, here]
        inflow = before * pltpu.roll(centre, 1, 1) + after * pltpu.roll(centre, LANES - 1, 1)
        inflow += left * source[level, down] + right * source[level, up]
        target[level, here] = centre + speed * (inflow - drain * centre)


def pieces(low, high, step):
    return [(start, min(step, high - start)) for start in range(low, high, step)]


def tiles_kernel(
    initial_in, forcing_in, current_in, cover_in, state, average,
    pack, forcing, current, cover, recv, work, spare, stat, total, back, home, mean,
    load, first_send, first_recv, second_send, second_recv,
    total_send, total_recv, state_send, state_recv, mean_send, mean_recv, go,
):
    me = lax.axis_index("blk")
    comp = lax.axis_index("comp")
    count = lax.axis_size("blk")
    fields, rows, cols = initial_in.shape
    barrier = pltpu.get_barrier_semaphore()

    def greet(where):
        pl.semaphore_signal(barrier, inc=1, device_id=where, device_id_type=MESH)

    def other(step):
        return lax.rem(me + step, count)

    steps = range(1, count)
    for step in steps:
        greet({"blk": other(step)})
    greet({"comp": 1 - comp})

    loads = [
        pltpu.make_async_copy(source, target, load.at[i])
        for i, (source, target) in enumerate(
            (
                (initial_in, pack.at[0:fields]),
                (current_in, current),
                (forcing_in, forcing),
                (cover_in, cover),
            )
        )
    ]
    for copy in loads:
        copy.start()

    def lanes_of(block):
        return pl.ds(pl.multiple_of(block * LANES, LANES), LANES)

    def rows_of(block):
        return pl.ds(pl.multiple_of(block * rows, rows), rows)

    def outward(low, high, sems):
        return [
            pltpu.make_async_remote_copy(
                pack.at[low:high, :, lanes_of(other(step))],
                recv.at[low:high, rows_of(me), :],
                sems[0].at[step], sems[1].at[step],
                device_id={"blk": other(step)}, device_id_type=MESH,
            )
            for step in steps
        ]

    def homeward(source, target, sems):
        return [
            pltpu.make_async_remote_copy(
                source.at[:, rows_of(other(step)), :],
                target.at[:, :, lanes_of(me)],
                sems[0].at[step], sems[1].at[step],
                device_id={"blk": other(step)}, device_id_type=MESH,
            )
            for step in steps
        ]

    def start(copies):
        for copy in copies:
            copy.start()

    def arrive(copies):
        for copy in copies:
            copy.wait_recv()

    def sent(copies):
        for copy in copies:
            copy.wait_send()

    def spread_edges(base, filled, reach):
        group = LANES // (2 * reach)
        lane = lane_index((rows, LANES))
        slot = lane // (2 * reach)
        leading = lane % (2 * reach) < reach
        zero = jnp.zeros((rows, LANES), jnp.float32)
        for tile in range(-(-filled // group)):
            members = range(tile * group, min(filled, (tile + 1) * group))
            turned = []
            for block in range(count):
                here = slice(block * LANES, (block + 1) * LANES)
                merged = zero
                for place, field in enumerate(members):
                    shift = (2 * place + 1) * reach % LANES
                    value = pack[field, :, here]
                    moved = pltpu.roll(value, shift, 1) if shift else value
                    merged = jnp.where(slot == place, moved, merged)
                turned.append(merged)
            for block in range(count):
                before = turned[block - 1] if block > 0 else zero
                after = turned[block + 1] if block < count - 1 else zero
                here = slice(block * LANES, (block + 1) * LANES)
                pack[base + tile, :, here] = jnp.where(leading, before, after)

    def unpack(field, base, reach):
        group = LANES // (2 * reach)
        value = recv[field].T
        edge = recv[base + field // group].T
        low = field % group * 2 * reach
        return jnp.concatenate(
            [edge[low : low + reach], value, edge[low + reach : low + 2 * reach]], axis=0
        )

    mean_copy = pltpu.make_async_remote_copy(
        mean, average, mean_send, mean_recv,
        device_id={"comp": 1 - comp}, device_id_type=MESH,
    )

    @pl.when(comp == 0)
    def _():
        filled = fields + 4
        packed = filled + -(-filled // (LANES // (2 * ICE_REACH)))
        span = LANES + 2 * ICE_REACH
        loads[0].wait()
        pl.semaphore_wait(barrier, count)
        first = outward(0, fields, (first_send, first_recv))
        start(first)
        for copy in loads[1:]:
            copy.wait()
        covered = cover[...].astype(jnp.float32)
        push = covered / (inertia * forcing[0] + 1.0)
        pack[fields] = forcing[1] * covered * (1.0 / 3.0)
        pack[fields + 1] = push
        pack[fields + 2] = push * (forcing[2] + current[0])
        pack[fields + 3] = push * (forcing[3] + current[1])
        spread_edges(filled, filled, ICE_REACH)
        second = outward(fields, packed, (second_send, second_recv))
        start(second)
        recv[0:packed, rows_of(me), :] = pack[0:packed, :, lanes_of(me)]
        total[...] = jnp.zeros_like(total)
        for array in (work, stat):
            for edge in (0, LEAD + span):
                array[:, edge : edge + LEAD] = jnp.zeros((array.shape[0], LEAD, LANES), jnp.float32)
        sent(first)
        sent(second)
        pl.semaphore_signal(go, inc=1, device_id={"comp": 1 - comp}, device_id_type=MESH)
        arrive(first)
        arrive(second)
        whole = slice(LEAD, LEAD + span)
        for field in range(2):
            work[field, whole] = unpack(field, filled, ICE_REACH)
        one, two = unpack(2, filled, ICE_REACH), unpack(3, filled, ICE_REACH)
        work[2, whole] = one + two
        work[3, whole] = one - two
        work[4, whole] = unpack(4, filled, ICE_REACH)
        stat[0, whole] = unpack(fields, filled, ICE_REACH)
        push = unpack(fields + 1, filled, ICE_REACH)
        stat[1, whole] = jnp.where(push > 0.0, 1.0 - push, 0.0)
        stat[2, whole] = 0.25 * push
        stat[3, whole] = unpack(fields + 2, filled, ICE_REACH)
        stat[4, whole] = unpack(fields + 3, filled, ICE_REACH)

        for group in range(SUBCYCLES // 4):
            low, high = LEAD + 8 * group, LEAD + span - 8 * group
            inner, outer = LEAD + ICE_REACH, LEAD + ICE_REACH + LANES

            def subcycle(step, carry, low=low, high=high):
                for begin, size in pieces(low, high, 16):
                    tile_stress(work, stat, begin, size)
                for begin, size in pieces(low, inner, 16) + pieces(outer, high, 16):
                    tile_velocity(work, stat, total, begin, size, None)
                for begin, size in pieces(inner, outer, 16):
                    tile_velocity(work, stat, total, begin, size, begin - inner)
                return carry

            lax.fori_loop(0, 4, subcycle, 0)

        own = slice(LEAD + ICE_REACH, LEAD + ICE_REACH + LANES)
        for channel in range(3):
            back[channel] = total[channel].T
        totals = homeward(back.at[0:3], home, (total_send, total_recv))
        start(totals)
        one, two = work[2, own], work[3, own]
        for field, value in enumerate(
            (work[0, own], work[1, own], 0.5 * (one + two), 0.5 * (one - two), work[4, own])
        ):
            back[3 + field] = value.T
        states = homeward(back.at[3 : 3 + fields], state, (state_send, state_recv))
        start(states)
        home[:, :, lanes_of(me)] = back[0:3, rows_of(me), :]
        state[:, :, lanes_of(me)] = back[3 : 3 + fields, rows_of(me), :]
        share = 1.0 / SUBCYCLES
        covered = cover[...].astype(jnp.float32)
        arrive(totals)
        mean[0] = home[0] * share - covered * current[0]
        mean[1] = home[1] * share - covered * current[1]
        mean[2] = forcing[4] * covered * (home[2] * share)
        mean_copy.start()
        average[...] = mean[...]
        sent(totals)
        arrive(states)
        sent(states)
        mean_copy.wait_send()

    @pl.when(comp == 1)
    def _():
        filled = fields + 2
        packed = filled + -(-filled // (LANES // (2 * SEA_REACH)))
        span = LANES + 2 * SEA_REACH
        for copy in loads:
            copy.wait()
        for axis in range(2):
            pack[fields + axis] = current[axis]
        spread_edges(filled, filled, SEA_REACH)
        for array in (work, spare):
            for edge in (0, LEAD + span):
                array[:, edge : edge + LEAD] = jnp.zeros((array.shape[0], LEAD, LANES), jnp.float32)
        recv[0:packed, rows_of(me), :] = pack[0:packed, :, lanes_of(me)]
        pl.semaphore_wait(barrier, count)
        pl.semaphore_wait(go, 1)
        first = outward(0, packed, (first_send, first_recv))
        start(first)
        arrive(first)
        whole = slice(LEAD, LEAD + span)
        for field in range(fields):
            work[field, whole] = unpack(field, filled, SEA_REACH)
        lane = lane_index((span, LANES))
        speed = courant * unpack(fields, filled, SEA_REACH)
        drain = jnp.abs(speed)
        stat[0, whole] = jnp.where(lane == 0, 0.0, jnp.maximum(speed, 0.0))
        stat[1, whole] = jnp.where(lane == LANES - 1, 0.0, -jnp.minimum(speed, 0.0))
        speed = courant * unpack(fields + 1, filled, SEA_REACH)
        stat[2, whole] = jnp.maximum(speed, 0.0)
        stat[3, whole] = -jnp.minimum(speed, 0.0)
        stat[4, whole] = drain + jnp.abs(speed)
        for group in range(SUBCYCLES // 8):
            low, high = LEAD + 8 * group, LEAD + span - 8 * group

            def substeps(step, carry, low=low, high=high):
                for begin, size in pieces(low, high, 16):
                    tile_ocean(work, spare, stat, begin, size)
                for begin, size in pieces(low, high, 16):
                    tile_ocean(spare, work, stat, begin, size)
                return carry

            lax.fori_loop(0, 4, substeps, 0)
        own = slice(LEAD + SEA_REACH, LEAD + SEA_REACH + LANES)
        for field in range(fields):
            back[3 + field] = work[field, own].T
        states = homeward(back.at[3 : 3 + fields], state, (state_send, state_recv))
        start(states)
        state[:, :, lanes_of(me)] = back[3 : 3 + fields, rows_of(me), :]
        sent(first)
        mean_copy.wait_recv()
        arrive(states)
        sent(states)


def run_tiles(initial, forcing, current, cover, count):
    fields, rows, cols = initial.shape
    f32 = jnp.float32
    most = fields + 4
    packed = most + -(-most // (LANES // (2 * ICE_REACH)))
    tall = LANES + 2 * ICE_REACH + 2 * LEAD
    vmem = pl.BlockSpec(memory_space=pltpu.VMEM)
    dma = pltpu.SemaphoreType.DMA
    return pl.pallas_call(
        tiles_kernel,
        out_shape=(
            jax.ShapeDtypeStruct((fields, rows, cols), f32),
            jax.ShapeDtypeStruct((3, rows, cols), f32),
        ),
        in_specs=[pl.BlockSpec(memory_space=pl.ANY)] * 4,
        out_specs=(vmem, vmem),
        scratch_shapes=[
            pltpu.VMEM((packed, rows, cols), f32),
            pltpu.VMEM(forcing.shape, f32),
            pltpu.VMEM(current.shape, f32),
            pltpu.VMEM(cover.shape, cover.dtype),
            pltpu.VMEM((packed, LANES, LANES), f32),
            pltpu.VMEM((fields, tall, LANES), f32),
            pltpu.VMEM((fields, tall, LANES), f32),
            pltpu.VMEM((5, tall, LANES), f32),
            pltpu.VMEM((3, LANES, LANES), f32),
            pltpu.VMEM((3 + fields, LANES, LANES), f32),
            pltpu.VMEM((3, rows, cols), f32),
            pltpu.VMEM((3, rows, cols), f32),
            dma((4,)),
            *[dma((count,)) for _ in range(8)],
            dma, dma, pltpu.SemaphoreType.REGULAR,
        ],
        compiler_params=pltpu.CompilerParams(
            collective_id=0, has_side_effects=True, vmem_limit_bytes=40 * 1024 * 1024
        ),
        name="tiles",
    )(initial, forcing, current, cover)


def remap_kernel(average, targets, weights, window, acc, low_index, high_index):
    comp = lax.axis_index("comp")
    channels, rows, cols = average.shape
    span = low_index.shape[1]
    low_count, high_count = low_index.shape[0], high_index.shape[0]
    bf16 = jnp.bfloat16
    blocks = cols // low_count
    low_index[...] = lax.broadcasted_iota(jnp.int32, low_index.shape, 0).astype(bf16)
    high_index[...] = lax.broadcasted_iota(jnp.int32, high_index.shape, 0).astype(bf16)
    acc[...] = jnp.zeros_like(acc)

    def one_row(row, carry):
        for piece in range(cols // span):
            place = pl.ds(piece * span, span)
            target = targets[comp, pl.ds(row, 1), place]
            scale = weights[comp, pl.ds(row, 1), place].astype(jnp.float32) * (1.0 / weight_norm)
            low = lax.rem(target, low_count)
            block = lax.rem(lax.div(target, low_count), blocks)
            line = lax.div(target, cols)
            high = (lax.div(line, rows) * blocks + block) * rows + lax.rem(line, rows)
            low_hot = jnp.where(low_index[...] == low.astype(bf16), bf16(1), bf16(0))
            match = high_index[...] == high.astype(bf16)
            parts = []
            for channel in range(channels):
                value = average[channel, pl.ds(row, 1), place] * scale
                coarse = value.astype(bf16)
                fine = (value - coarse.astype(jnp.float32)).astype(bf16)
                parts.append(jnp.where(match, coarse, bf16(0)))
                parts.append(jnp.where(match, fine, bf16(0)))
            spread = jnp.concatenate(parts, axis=0)
            acc[...] += lax.dot_general(
                spread, low_hot, (((1,), (1,)), ((), ())), preferred_element_type=jnp.float32
            )
        return carry

    lax.fori_loop(0, rows, one_row, 0)
    for channel in range(channels):
        for half in range(2):
            for block in range(blocks):
                base = 2 * channel * high_count + (half * blocks + block) * rows
                window[channel, half, :, block * low_count : (block + 1) * low_count] = (
                    acc[base : base + rows] + acc[base + high_count : base + high_count + rows]
                )


def run_remap(average, targets, weights):
    channels, rows, cols = average.shape
    low_count = 256 if cols % 256 == 0 else 128
    high_count = 2 * rows * cols // low_count
    span = min(1024, cols)
    vmem = pl.BlockSpec(memory_space=pltpu.VMEM)
    return pl.pallas_call(
        remap_kernel,
        out_shape=jax.ShapeDtypeStruct((channels, 2, rows, cols), jnp.float32),
        in_specs=[vmem] * 3,
        out_specs=vmem,
        scratch_shapes=[
            pltpu.VMEM((2 * channels * high_count, low_count), jnp.float32),
            pltpu.VMEM((low_count, span), jnp.bfloat16),
            pltpu.VMEM((high_count, span), jnp.bfloat16),
        ],
        compiler_params=pltpu.CompilerParams(vmem_limit_bytes=40 * 1024 * 1024),
        name="remap",
    )(average, targets, weights)


def join_kernel(
    window, state, average, out_state, out_pair, beside, carry, before,
    side_send, side_recv, next_send, next_recv,
):
    me = lax.axis_index("blk")
    comp = lax.axis_index("comp")
    count = lax.axis_size("blk")
    right, left = lax.rem(me + 1, count), lax.rem(me + count - 1, count)
    barrier = pltpu.get_barrier_semaphore()
    pl.semaphore_signal(barrier, inc=1, device_id={"blk": right}, device_id_type=MESH)
    pl.semaphore_signal(barrier, inc=1, device_id={"blk": left}, device_id_type=MESH)
    pl.semaphore_signal(barrier, inc=1, device_id={"comp": 1 - comp}, device_id_type=MESH)
    pl.semaphore_wait(barrier, 3)
    channels = window.shape[0]
    sides, onward = [], []
    for half in (1, 0):
        for channel in range(channels):
            sides.append(
                pltpu.make_async_remote_copy(
                    window.at[channel, half], beside.at[channel, half],
                    side_send.at[half, channel], side_recv.at[half, channel],
                    device_id={"comp": 1 - comp}, device_id_type=MESH,
                )
            )
    for channel in range(channels):
        onward.append(
            pltpu.make_async_remote_copy(
                carry.at[channel], before.at[channel],
                next_send.at[channel], next_recv.at[channel],
                device_id={"blk": right}, device_id_type=MESH,
            )
        )

    @pl.when(comp == 0)
    def _():
        for copy in sides:
            copy.start()
        out_state[...] = state[...]
        out_pair[...] = average[...]
        for copy in sides:
            copy.wait_send()

    @pl.when(comp == 1)
    def _():
        for channel in range(channels):
            sides[channel].wait_recv()
            carry[channel] = window[channel, 1] + beside[channel, 1]
            onward[channel].start()
        for channel in range(channels):
            sides[channels + channel].wait_recv()
            out_pair[channel] = window[channel, 0] + beside[channel, 0]
        out_state[...] = state[...]
        for channel in range(channels):
            onward[channel].wait_recv()
            out_pair[channel] += before[channel]
        out_state[0] -= dilution * out_pair[2]
        for channel in range(channels):
            onward[channel].wait_send()


def run_join(window, state, average):
    channels, rows, cols = average.shape
    vmem = pl.BlockSpec(memory_space=pltpu.VMEM)
    dma = pltpu.SemaphoreType.DMA
    return pl.pallas_call(
        join_kernel,
        out_shape=(
            jax.ShapeDtypeStruct(state.shape, jnp.float32),
            jax.ShapeDtypeStruct(average.shape, jnp.float32),
        ),
        in_specs=[vmem] * 3,
        out_specs=(vmem, vmem),
        scratch_shapes=[
            pltpu.VMEM(window.shape, jnp.float32),
            pltpu.VMEM(average.shape, jnp.float32),
            pltpu.VMEM(average.shape, jnp.float32),
            dma((2, channels)), dma((2, channels)), dma((channels,)), dma((channels,)),
        ],
        compiler_params=pltpu.CompilerParams(
            collective_id=1, has_side_effects=True, vmem_limit_bytes=40 * 1024 * 1024
        ),
        name="join",
    )(window, state, average)


def body(count, initial, ice_forcing, ocean_current, ice_cover, targets, weights):
    if fits_tiles(count, *initial.shape[2:]):
        state, average = run_tiles(initial[0], ice_forcing, ocean_current, ice_cover, count)
    else:
        state, average = run_turns(initial[0], ice_forcing, ocean_current, ice_cover)
    window = run_remap(average, targets, weights)
    state, coupled = run_join(window, state, average)
    return (state[None], coupled[None])


def solution(mesh):
    placed = (
        P("comp", None, "blk", None),
        P(None, "blk", None),
        P(None, "blk", None),
        P("blk", None),
        P(None, "blk", None),
        P(None, "blk", None),
    )
    return jax.shard_map(
        functools.partial(body, mesh.shape["blk"]),
        mesh=mesh,
        in_specs=placed,
        out_specs=(P("comp", None, "blk", None), P("comp", None, "blk", None)),
        check_vma=False,
    )
```

```python
import functools

import jax
import jax.numpy as jnp
from jax import lax
from jax.experimental import pallas as pl
from jax.experimental.pallas import tpu as pltpu
from jax.sharding import PartitionSpec as P

SUBCYCLES = 16
MESH = pl.DeviceIdType.MESH
PAD = 128
PARTS = 2

coriolis = 0.1
inertia = 4.0
courant = 0.2
dilution = 0.5
weight_norm = 4.0
level_speed = (1.0, 0.8, 0.6, 0.45, 0.3)


def rolled(value, steps, axis):
    return pltpu.roll(value, steps % value.shape[axis], axis)


def rows_diff(value):
    return rolled(value, -1, 0) - rolled(value, 1, 0)


def chunk_width(cols):
    return 256 if cols % 256 == 0 else 128


def stress_stage(work, stat, start, width):
    wide = pl.ds(start, width + 2 * PAD)
    mid = pl.ds(start + PAD, width)
    inner = slice(PAD, PAD + width)
    vel_x, vel_y = work[0, :, wide], work[1, :, wide]
    cx = (rolled(vel_x, -1, 1) - rolled(vel_x, 1, 1))[:, inner]
    cy = (rolled(vel_y, -1, 1) - rolled(vel_y, 1, 1))[:, inner]
    rx = rows_diff(vel_x[:, inner])
    ry = rows_diff(vel_y[:, inner])
    e_d = rx + cy
    e_t = rx - cy
    e_s = cx + ry
    inv = lax.rsqrt(0.25 * (e_d * e_d) + 0.0625 * (e_t * e_t + e_s * e_s) + 0.01)
    third = stat[0, :, pl.ds(start, width)]
    scaled = third * inv
    work[2, :, mid] = work[2, :, mid] * (2.0 / 3.0) + (0.5 * scaled * e_d - third)
    work[3, :, mid] = work[3, :, mid] * (2.0 / 3.0) + 0.125 * scaled * e_t
    work[4, :, mid] = work[4, :, mid] * (2.0 / 3.0) + 0.0625 * scaled * e_s


def velocity_stage(work, stat, total, start, width, rows):
    wide = pl.ds(start, width + 2 * PAD)
    mid = pl.ds(start + PAD, width)
    here = pl.ds(start, width)
    inner = slice(PAD, PAD + width)
    shear = work[4, :, wide]
    one, two = work[2, :, wide], work[3, :, wide]
    across_shear = (rolled(shear, -1, 1) - rolled(shear, 1, 1))[:, inner]
    lower = one - two
    across_yy = (rolled(lower, -1, 1) - rolled(lower, 1, 1))[:, inner]
    force_x = rows_diff((one + two)[:, inner]) + 2.0 * across_shear
    force_y = 2.0 * rows_diff(shear[:, inner]) + across_yy
    old_x, old_y = work[0, :, mid], work[1, :, mid]
    keep, push = stat[1, :, here], stat[2, :, here]
    new_x = keep * (old_x + coriolis * old_y) + push * force_x + stat[3, :, here]
    new_y = keep * (old_y - coriolis * old_x) + push * force_y + stat[4, :, here]
    work[0, :, mid] = new_x
    work[1, :, mid] = new_y
    own_x, own_y = new_x[rows : 2 * rows], new_y[rows : 2 * rows]
    total[0, :, here] += own_x
    total[1, :, here] += own_y
    total[2, :, here] += jnp.sqrt(1.0 + own_x * own_x + own_y * own_y)


def ocean_stage(source, target, coef, start, width):
    wide = pl.ds(start, width + 2 * PAD)
    mid = pl.ds(start + PAD, width)
    here = pl.ds(start, width)
    inner = slice(PAD, PAD + width)
    up, down, east, west = (coef[i, :, here] for i in range(4))
    for level, speed in enumerate(level_speed):
        tracer = source[level, :, wide]
        centre = tracer[:, inner]
        right = rolled(tracer, -1, 1)[:, inner] - centre
        left = centre - rolled(tracer, 1, 1)[:, inner]
        above = rolled(centre, -1, 0) - centre
        below = centre - rolled(centre, 1, 0)
        change = up * below + down * above + east * left + west * right
        target[level, :, mid] = centre - speed * change


def turns_kernel(
    initial_in, forcing_in, current_in, cover_in, state, average,
    initial, forcing, current, cover,
    own, own_stat, halo, halo_stat, work, spare, stat, total, mean,
    load, near_send, near_recv, far_send, far_recv,
    stat_near_send, stat_near_recv, stat_far_send, stat_far_recv,
    mean_send, mean_recv, go,
):
    me = lax.axis_index("blk")
    comp = lax.axis_index("comp")
    count = lax.axis_size("blk")
    fields, rows, cols = initial.shape
    width = chunk_width(cols)
    chunks = cols // width
    near = 1 - lax.rem(me, 2)
    far = 1 - near
    partner = me + 2 * near - 1
    relay_to = me + 4 * near - 2
    relay_from = me - 4 * near + 2
    can_send = jnp.logical_and(relay_to >= 0, relay_to < count)
    can_recv = jnp.logical_and(relay_from >= 0, relay_from < count)
    relay_to = lax.rem(relay_to + count, count)
    relay_from = lax.rem(relay_from + count, count)

    barrier = pltpu.get_barrier_semaphore()

    def greet(where):
        pl.semaphore_signal(barrier, inc=1, device_id=where, device_id_type=MESH)

    greet({"blk": partner})
    greet({"comp": 1 - comp})
    pl.when(can_send)(lambda: greet({"blk": relay_to}))
    pl.when(can_recv)(lambda: greet({"blk": relay_from}))
    loads = [
        pltpu.make_async_copy(source, target, load.at[i])
        for i, (source, target) in enumerate(
            (
                (initial_in, initial),
                (current_in, current),
                (forcing_in, forcing),
                (cover_in, cover),
            )
        )
    ]
    for copy in loads:
        copy.start()

    work[...] = jnp.zeros_like(work)
    total[...] = jnp.zeros_like(total)

    def enter():
        pl.semaphore_wait(barrier, 2 + can_send.astype(jnp.int32) + can_recv.astype(jnp.int32))

    def copies(source, target, pieces, near_sems, far_sems):
        first, second = [], []
        wide = cols // PARTS
        for index in range(pieces * PARTS):
            piece, place = index // PARTS, pl.ds(index % PARTS * wide, wide)
            first.append(
                pltpu.make_async_remote_copy(
                    source.at[piece, :, place], target.at[far, piece, :, place],
                    near_sems[0].at[index], near_sems[1].at[index],
                    device_id={"blk": partner}, device_id_type=MESH,
                )
            )
            second.append(
                pltpu.make_async_remote_copy(
                    target.at[near, piece, :, place], target.at[far, piece, :, place],
                    far_sems[0].at[index], far_sems[1].at[index],
                    device_id={"blk": relay_to}, device_id_type=MESH,
                )
            )
        return first, second

    def start(pair):
        for copy in pair[0]:
            copy.start()

    def relay(pair):
        for first, second in zip(*pair):
            first.wait_recv()
            pl.when(can_send)(second.start)

    def arrive(pair):
        @pl.when(can_recv)
        def _():
            for copy in pair[1]:
                copy.wait_recv()

    def sent(pair):
        for copy in pair[0]:
            copy.wait_send()

        @pl.when(can_send)
        def _():
            for copy in pair[1]:
                copy.wait_send()

    def clear_edges(turns):
        @pl.when(jnp.logical_not(can_recv))
        def _():
            halo_stat[far] = jnp.zeros(halo_stat.shape[1:], jnp.float32)
            for turn in range(turns):
                halo[turn, far] = jnp.zeros(halo.shape[2:], jnp.float32)

    inside = slice(PAD, PAD + cols)

    def fill_own(source):
        for field in range(fields):
            work[field, rows : 2 * rows, inside] = source[field]

    def fill_sides(turn):
        for field in range(fields):
            work[field, 0:rows, inside] = halo[turn, 0, field]
            work[field, 2 * rows : 3 * rows, inside] = halo[turn, 1, field]

    def exchange_of(turn, source):
        return copies(
            source, halo.at[turn], fields,
            (near_send.at[turn], near_recv.at[turn]), (far_send.at[turn], far_recv.at[turn]),
        )

    def stats_of(source, pieces):
        return copies(
            source, halo_stat, pieces,
            (stat_near_send, stat_near_recv), (stat_far_send, stat_far_recv),
        )

    mean_copy = pltpu.make_async_remote_copy(
        mean, average, mean_send, mean_recv,
        device_id={"comp": 1 - comp}, device_id_type=MESH,
    )

    @pl.when(comp == 0)
    def _():
        depth = rows // 2
        turns = SUBCYCLES // depth
        clear_edges(turns)
        loads[0].wait()
        enter()
        pairs = [exchange_of(0, initial)]
        start(pairs[0])
        for copy in loads[1:]:
            copy.wait()
        covered = cover[...].astype(jnp.float32)
        push = covered / (inertia * forcing[0] + 1.0)
        own_stat[0] = forcing[1] * covered * (1.0 / 3.0)
        own_stat[1] = push
        own_stat[2] = push * (forcing[2] + current[0])
        own_stat[3] = push * (forcing[3] + current[1])
        stat_pair = stats_of(own_stat, 4)
        start(stat_pair)
        for turn in range(turns):
            source = initial if turn == 0 else own.at[turn - 1]
            if turn > 0:
                pairs.append(exchange_of(turn, source))
                start(pairs[turn])
            relay(pairs[turn])
            if turn == 0:
                relay(stat_pair)
                pl.semaphore_signal(
                    go, inc=1, device_id={"comp": 1 - comp}, device_id_type=MESH
                )
            fill_own(source)
            arrive(pairs[turn])
            if turn == 0:
                arrive(stat_pair)
                for place, block in enumerate((halo_stat.at[0], own_stat, halo_stat.at[1])):
                    span = slice(place * rows, (place + 1) * rows)
                    push = block[1]
                    stat[0, span] = block[0]
                    stat[1, span] = jnp.where(push > 0.0, 1.0 - push, 0.0)
                    stat[2, span] = 0.25 * push
                    stat[3, span] = block[2]
                    stat[4, span] = block[3]
            fill_sides(turn)

            def subcycle(step, carry):
                for chunk in range(chunks):
                    stress_stage(work, stat, chunk * width, width)
                for chunk in range(chunks):
                    velocity_stage(work, stat, total, chunk * width, width, rows)
                return carry

            lax.fori_loop(0, depth, subcycle, 0)
            final = state if turn == turns - 1 else own.at[turn]
            for field in range(fields):
                final[field] = work[field, rows : 2 * rows, inside]
        share = 1.0 / SUBCYCLES
        covered = cover[...].astype(jnp.float32)
        mean[0] = total[0] * share - covered * current[0]
        mean[1] = total[1] * share - covered * current[1]
        mean[2] = forcing[4] * covered * (total[2] * share)
        mean_copy.start()
        average[...] = mean[...]
        sent(stat_pair)
        for pair in pairs:
            sent(pair)
        mean_copy.wait_send()

    @pl.when(comp == 1)
    def _():
        depth = rows
        turns = SUBCYCLES // depth
        clear_edges(turns)
        spare[...] = jnp.zeros_like(spare)
        for copy in loads:
            copy.wait()
        enter()
        pl.semaphore_wait(go, 1)
        pairs = [exchange_of(0, initial)]
        start(pairs[0])
        stat_pair = stats_of(current, 2)
        start(stat_pair)
        for turn in range(turns):
            source = initial if turn == 0 else own.at[turn - 1]
            if turn > 0:
                pairs.append(exchange_of(turn, source))
                start(pairs[turn])
            relay(pairs[turn])
            if turn == 0:
                relay(stat_pair)
            fill_own(source)
            arrive(pairs[turn])
            if turn == 0:
                arrive(stat_pair)
                for place in range(3):
                    span = slice(place * rows, (place + 1) * rows)
                    for axis in range(2):
                        if place == 1:
                            speed = current[axis]
                        else:
                            speed = halo_stat[place // 2, axis]
                        stat[2 * axis, span] = courant * jnp.maximum(speed, 0.0)
                        stat[2 * axis + 1, span] = courant * jnp.minimum(speed, 0.0)
            fill_sides(turn)

            def substeps(step, carry):
                for chunk in range(chunks):
                    ocean_stage(work, spare, stat, chunk * width, width)
                for chunk in range(chunks):
                    ocean_stage(spare, work, stat, chunk * width, width)
                return carry

            lax.fori_loop(0, depth // 2, substeps, 0)
            final = state if turn == turns - 1 else own.at[turn]
            for field in range(fields):
                final[field] = work[field, rows : 2 * rows, inside]
        sent(stat_pair)
        for pair in pairs:
            sent(pair)
        mean_copy.wait_recv()


def run_turns(initial, forcing, current, cover):
    fields, rows, cols = initial.shape
    most = SUBCYCLES // (rows // 2)
    f32 = jnp.float32
    vmem = pl.BlockSpec(memory_space=pltpu.VMEM)
    dma = pltpu.SemaphoreType.DMA
    return pl.pallas_call(
        turns_kernel,
        out_shape=(
            jax.ShapeDtypeStruct((fields, rows, cols), f32),
            jax.ShapeDtypeStruct((3, rows, cols), f32),
        ),
        in_specs=[pl.BlockSpec(memory_space=pl.ANY)] * 4,
        out_specs=(vmem, vmem),
        scratch_shapes=[
            pltpu.VMEM(initial.shape, f32),
            pltpu.VMEM(forcing.shape, f32),
            pltpu.VMEM(current.shape, f32),
            pltpu.VMEM(cover.shape, cover.dtype),
            pltpu.VMEM((most, fields, rows, cols), f32),
            pltpu.VMEM((4, rows, cols), f32),
            pltpu.VMEM((most, 2, fields, rows, cols), f32),
            pltpu.VMEM((2, 4, rows, cols), f32),
            pltpu.VMEM((fields, 3 * rows, cols + 2 * PAD), f32),
            pltpu.VMEM((fields, 3 * rows, cols + 2 * PAD), f32),
            pltpu.VMEM((5, 3 * rows, cols), f32),
            pltpu.VMEM((3, rows, cols), f32),
            pltpu.VMEM((3, rows, cols), f32),
            dma((4,)),
            *[dma((most, fields * PARTS)) for _ in range(4)],
            *[dma((4 * PARTS,)) for _ in range(4)],
            dma, dma, pltpu.SemaphoreType.REGULAR,
        ],
        compiler_params=pltpu.CompilerParams(
            collective_id=0, has_side_effects=True
        ),
        name="turns",
    )(initial, forcing, current, cover)


LANES = 128
LEAD = 8
ICE_REACH = 2 * SUBCYCLES
SEA_REACH = SUBCYCLES


def fits_tiles(count, rows, cols):
    return count * rows == LANES and cols == count * LANES and count > 1


def lane_index(shape):
    return lax.broadcasted_iota(jnp.int32, shape, len(shape) - 1)


def lane_diff(value):
    lane = lane_index(value.shape)
    after = jnp.where(lane == LANES - 1, 0.0, pltpu.roll(value, LANES - 1, 1))
    before = jnp.where(lane == 0, 0.0, pltpu.roll(value, 1, 1))
    return after - before


def tile_stress(work, stat, low, size):
    here, up, down = (pl.ds(low + shift, size) for shift in (0, 1, -1))
    vel_x, vel_y = work[0, here], work[1, here]
    cx = work[0, up] - work[0, down]
    cy = work[1, up] - work[1, down]
    rx, ry = lane_diff(vel_x), lane_diff(vel_y)
    e_d = rx + cy
    e_t = rx - cy
    e_s = cx + ry
    inv = lax.rsqrt(0.25 * (e_d * e_d) + 0.0625 * (e_t * e_t + e_s * e_s) + 0.01)
    third = stat[0, here]
    scaled = third * inv
    one = 0.5 * scaled * e_d - third
    two = 0.125 * scaled * e_t
    work[2, here] = work[2, here] * (2.0 / 3.0) + (one + two)
    work[3, here] = work[3, here] * (2.0 / 3.0) + (one - two)
    work[4, here] = work[4, here] * (2.0 / 3.0) + 0.0625 * scaled * e_s


def tile_velocity(work, stat, total, low, size, own):
    here, up, down = (pl.ds(low + shift, size) for shift in (0, 1, -1))
    force_x = lane_diff(work[2, here]) + 2.0 * (work[4, up] - work[4, down])
    force_y = 2.0 * lane_diff(work[4, here]) + (work[3, up] - work[3, down])
    old_x, old_y = work[0, here], work[1, here]
    keep, push = stat[1, here], stat[2, here]
    new_x = keep * (old_x + coriolis * old_y) + push * force_x + stat[3, here]
    new_y = keep * (old_y - coriolis * old_x) + push * force_y + stat[4, here]
    work[0, here] = new_x
    work[1, here] = new_y
    if own is not None:
        place = pl.ds(own, size)
        total[0, place] += new_x
        total[1, place] += new_y
        square = 1.0 + new_x * new_x + new_y * new_y
        total[2, place] += square * lax.rsqrt(square)


def tile_ocean(source, target, stat, low, size):
    here, up, down = (pl.ds(low + shift, size) for shift in (0, 1, -1))
    before, after, left, right, drain = (stat[i, here] for i in range(5))
    for level, speed in enumerate(level_speed):
        centre = source[level, here]
        inflow = before * pltpu.roll(centre, 1, 1) + after * pltpu.roll(centre, LANES - 1, 1)
        inflow += left * source[level, down] + right * source[level, up]
        target[level, here] = centre + speed * (inflow - drain * centre)


def pieces(low, high, step):
    return [(start, min(step, high - start)) for start in range(low, high, step)]


def tiles_kernel(
    initial_in, forcing_in, current_in, cover_in, targets_in, weights_in, state, pair,
    pack, forcing, current, cover, targets, weights,
    recv, work, spare, stat, total, back, home, mean, acc, window, beside, before,
    low_index, high_index,
    load, first_send, first_recv, second_send, second_recv,
    total_send, total_recv, state_send, state_recv, mean_send, mean_recv,
    side_send, side_recv, next_send, next_recv, go,
):
    me = lax.axis_index("blk")
    comp = lax.axis_index("comp")
    count = lax.axis_size("blk")
    fields, rows, cols = initial_in.shape
    barrier = pltpu.get_barrier_semaphore()

    def greet(where):
        pl.semaphore_signal(barrier, inc=1, device_id=where, device_id_type=MESH)

    def other(step):
        return lax.rem(me + step, count)

    steps = range(1, count)
    for step in steps:
        greet({"blk": other(step)})
    greet({"comp": 1 - comp})

    loads = [
        pltpu.make_async_copy(source, target, load.at[i])
        for i, (source, target) in enumerate(
            (
                (initial_in, pack.at[0:fields]),
                (current_in, current),
                (forcing_in, forcing),
                (cover_in, cover),
                (targets_in.at[comp], targets),
                (weights_in.at[comp], weights),
            )
        )
    ]
    for copy in loads:
        copy.start()

    def lanes_of(block):
        return pl.ds(pl.multiple_of(block * LANES, LANES), LANES)

    def rows_of(block):
        return pl.ds(pl.multiple_of(block * rows, rows), rows)

    def outward(low, high, sems):
        return [
            pltpu.make_async_remote_copy(
                pack.at[low:high, :, lanes_of(other(step))],
                recv.at[low:high, rows_of(me), :],
                sems[0].at[step], sems[1].at[step],
                device_id={"blk": other(step)}, device_id_type=MESH,
            )
            for step in steps
        ]

    def homeward(source, target, sems):
        return [
            pltpu.make_async_remote_copy(
                source.at[:, rows_of(other(step)), :],
                target.at[:, :, lanes_of(me)],
                sems[0].at[step], sems[1].at[step],
                device_id={"blk": other(step)}, device_id_type=MESH,
            )
            for step in steps
        ]

    def start(copies):
        for copy in copies:
            copy.start()

    def arrive(copies):
        for copy in copies:
            copy.wait_recv()

    def sent(copies):
        for copy in copies:
            copy.wait_send()

    def spread_edges(base, filled, reach):
        group = LANES // (2 * reach)
        lane = lane_index((rows, LANES))
        slot = lane // (2 * reach)
        leading = lane % (2 * reach) < reach
        zero = jnp.zeros((rows, LANES), jnp.float32)
        for tile in range(-(-filled // group)):
            members = range(tile * group, min(filled, (tile + 1) * group))
            turned = []
            for block in range(count):
                here = slice(block * LANES, (block + 1) * LANES)
                merged = zero
                for place, field in enumerate(members):
                    shift = (2 * place + 1) * reach % LANES
                    value = pack[field, :, here]
                    moved = pltpu.roll(value, shift, 1) if shift else value
                    merged = jnp.where(slot == place, moved, merged)
                turned.append(merged)
            for block in range(count):
                before = turned[block - 1] if block > 0 else zero
                after = turned[block + 1] if block < count - 1 else zero
                here = slice(block * LANES, (block + 1) * LANES)
                pack[base + tile, :, here] = jnp.where(leading, before, after)

    def unpack(field, base, reach):
        group = LANES // (2 * reach)
        value = recv[field].T
        edge = recv[base + field // group].T
        low = field % group * 2 * reach
        return jnp.concatenate(
            [edge[low : low + reach], value, edge[low + reach : low + 2 * reach]], axis=0
        )

    channels = pair.shape[0]
    mean_copy = pltpu.make_async_remote_copy(
        mean, home, mean_send, mean_recv,
        device_id={"comp": 1 - comp}, device_id_type=MESH,
    )
    sides = [
        [
            pltpu.make_async_remote_copy(
                window.at[half, channel], beside.at[half, channel],
                side_send.at[half, channel], side_recv.at[half, channel],
                device_id={"comp": 1 - comp}, device_id_type=MESH,
            )
            for channel in range(channels)
        ]
        for half in range(2)
    ]
    onward = [
        pltpu.make_async_remote_copy(
            window.at[1, channel], before.at[channel],
            next_send.at[channel], next_recv.at[channel],
            device_id={"blk": other(1)}, device_id_type=MESH,
        )
        for channel in range(channels)
    ]

    def prepare_remap():
        low_index[...] = lax.broadcasted_iota(jnp.int32, low_index.shape, 0).astype(low_index.dtype)
        high_index[...] = lax.broadcasted_iota(jnp.int32, high_index.shape, 0).astype(high_index.dtype)

    def remap(values, half):
        low_count, high_count = low_index.shape[0], high_index.shape[0]
        blocks = cols // low_count
        bf16 = jnp.bfloat16
        acc[...] = jnp.zeros_like(acc)

        def one_row(row, carry):
            place = pl.ds(row, 1)
            target = targets[place, :]
            scale = weights[place, :].astype(jnp.float32) * (1.0 / weight_norm)
            low = lax.rem(target, low_count)
            block = lax.rem(lax.div(target, low_count), blocks)
            line = lax.div(target, cols) - half * rows
            high = block * rows + line
            high = jnp.where(jnp.logical_and(line >= 0, line < rows), high, high_count)
            low_hot = jnp.where(low_index[...] == low.astype(bf16), bf16(1), bf16(0))
            match = high_index[...] == high.astype(bf16)
            parts = []
            for channel in range(channels):
                value = values[channel, place, :] * scale
                coarse = value.astype(bf16)
                fine = (value - coarse.astype(jnp.float32)).astype(bf16)
                parts.append(jnp.where(match, coarse, bf16(0)))
                parts.append(jnp.where(match, fine, bf16(0)))
            spread = jnp.concatenate(parts, axis=0)
            acc[...] += lax.dot_general(
                spread, low_hot, (((1,), (1,)), ((), ())), preferred_element_type=jnp.float32
            )
            return carry

        lax.fori_loop(0, rows, one_row, 0)
        for channel in range(channels):
            for block in range(blocks):
                base = 2 * channel * high_count + block * rows
                window[half, channel, :, block * low_count : (block + 1) * low_count] = (
                    acc[base : base + rows] + acc[base + high_count : base + high_count + rows]
                )

    @pl.when(comp == 0)
    def _():
        filled = fields + 4
        packed = filled + -(-filled // (LANES // (2 * ICE_REACH)))
        span = LANES + 2 * ICE_REACH
        loads[0].wait()
        pl.semaphore_wait(barrier, count)
        first = outward(0, fields, (first_send, first_recv))
        start(first)
        for copy in loads[1:4]:
            copy.wait()
        covered = cover[...].astype(jnp.float32)
        push = covered / (inertia * forcing[0] + 1.0)
        pack[fields] = forcing[1] * covered * (1.0 / 3.0)
        pack[fields + 1] = push
        pack[fields + 2] = push * (forcing[2] + current[0])
        pack[fields + 3] = push * (forcing[3] + current[1])
        spread_edges(filled, filled, ICE_REACH)
        second = outward(fields, packed, (second_send, second_recv))
        start(second)
        recv[0:packed, rows_of(me), :] = pack[0:packed, :, lanes_of(me)]
        total[...] = jnp.zeros_like(total)
        for array in (work, stat):
            for edge in (0, LEAD + span):
                array[:, edge : edge + LEAD] = jnp.zeros((array.shape[0], LEAD, LANES), jnp.float32)
        prepare_remap()
        for copy in loads[4:]:
            copy.wait()
        sent(first)
        sent(second)
        pl.semaphore_signal(go, inc=1, device_id={"comp": 1 - comp}, device_id_type=MESH)
        arrive(first)
        arrive(second)
        whole = slice(LEAD, LEAD + span)
        for field in range(2):
            work[field, whole] = unpack(field, filled, ICE_REACH)
        one, two = unpack(2, filled, ICE_REACH), unpack(3, filled, ICE_REACH)
        work[2, whole] = one + two
        work[3, whole] = one - two
        work[4, whole] = unpack(4, filled, ICE_REACH)
        stat[0, whole] = unpack(fields, filled, ICE_REACH)
        push = unpack(fields + 1, filled, ICE_REACH)
        stat[1, whole] = jnp.where(push > 0.0, 1.0 - push, 0.0)
        stat[2, whole] = 0.25 * push
        stat[3, whole] = unpack(fields + 2, filled, ICE_REACH)
        stat[4, whole] = unpack(fields + 3, filled, ICE_REACH)

        for group in range(SUBCYCLES // 4):
            low, high = LEAD + 8 * group, LEAD + span - 8 * group
            inner, outer = LEAD + ICE_REACH, LEAD + ICE_REACH + LANES

            def subcycle(step, carry, low=low, high=high):
                for begin, size in pieces(low, high, 16):
                    tile_stress(work, stat, begin, size)
                for begin, size in pieces(low, inner, 16) + pieces(outer, high, 16):
                    tile_velocity(work, stat, total, begin, size, None)
                for begin, size in pieces(inner, outer, 16):
                    tile_velocity(work, stat, total, begin, size, begin - inner)
                return carry

            lax.fori_loop(0, 4, subcycle, 0)

        own = slice(LEAD + ICE_REACH, LEAD + ICE_REACH + LANES)
        for channel in range(3):
            back[channel] = total[channel].T
        totals = homeward(back.at[0:3], home, (total_send, total_recv))
        start(totals)
        one, two = work[2, own], work[3, own]
        for field, value in enumerate(
            (work[0, own], work[1, own], 0.5 * (one + two), 0.5 * (one - two), work[4, own])
        ):
            back[3 + field] = value.T
        states = homeward(back.at[3 : 3 + fields], state, (state_send, state_recv))
        start(states)
        home[:, :, lanes_of(me)] = back[0:3, rows_of(me), :]
        state[:, :, lanes_of(me)] = back[3 : 3 + fields, rows_of(me), :]
        share = 1.0 / SUBCYCLES
        covered = cover[...].astype(jnp.float32)
        arrive(totals)
        mean[0] = home[0] * share - covered * current[0]
        mean[1] = home[1] * share - covered * current[1]
        mean[2] = forcing[4] * covered * (home[2] * share)
        mean_copy.start()
        pair[...] = mean[...]
        for half in (1, 0):
            remap(mean, half)
            start(sides[half])
        sent(totals)
        arrive(states)
        sent(states)
        mean_copy.wait_send()
        sent(sides[0] + sides[1])

    @pl.when(comp == 1)
    def _():
        filled = fields + 2
        packed = filled + -(-filled // (LANES // (2 * SEA_REACH)))
        span = LANES + 2 * SEA_REACH
        for copy in loads:
            copy.wait()
        for axis in range(2):
            pack[fields + axis] = current[axis]
        spread_edges(filled, filled, SEA_REACH)
        for array in (work, spare):
            for edge in (0, LEAD + span):
                array[:, edge : edge + LEAD] = jnp.zeros((array.shape[0], LEAD, LANES), jnp.float32)
        recv[0:packed, rows_of(me), :] = pack[0:packed, :, lanes_of(me)]
        prepare_remap()
        pl.semaphore_wait(barrier, count)
        pl.semaphore_wait(go, 1)
        first = outward(0, packed, (first_send, first_recv))
        start(first)
        arrive(first)
        whole = slice(LEAD, LEAD + span)
        for field in range(fields):
            work[field, whole] = unpack(field, filled, SEA_REACH)
        lane = lane_index((span, LANES))
        speed = courant * unpack(fields, filled, SEA_REACH)
        drain = jnp.abs(speed)
        stat[0, whole] = jnp.where(lane == 0, 0.0, jnp.maximum(speed, 0.0))
        stat[1, whole] = jnp.where(lane == LANES - 1, 0.0, -jnp.minimum(speed, 0.0))
        speed = courant * unpack(fields + 1, filled, SEA_REACH)
        stat[2, whole] = jnp.maximum(speed, 0.0)
        stat[3, whole] = -jnp.minimum(speed, 0.0)
        stat[4, whole] = drain + jnp.abs(speed)
        for group in range(SUBCYCLES // 8):
            low, high = LEAD + 8 * group, LEAD + span - 8 * group

            def substeps(step, carry, low=low, high=high):
                for begin, size in pieces(low, high, 16):
                    tile_ocean(work, spare, stat, begin, size)
                for begin, size in pieces(low, high, 16):
                    tile_ocean(spare, work, stat, begin, size)
                return carry

            lax.fori_loop(0, 4, substeps, 0)
        own = slice(LEAD + SEA_REACH, LEAD + SEA_REACH + LANES)
        for field in range(fields):
            back[3 + field] = work[field, own].T
        states = homeward(back.at[3 : 3 + fields], state, (state_send, state_recv))
        start(states)
        state[:, :, lanes_of(me)] = back[3 : 3 + fields, rows_of(me), :]
        sent(first)
        mean_copy.wait_recv()
        remap(home, 1)
        for channel in range(channels):
            sides[1][channel].wait_recv()
            window[1, channel] += beside[1, channel]
            onward[channel].start()
        remap(home, 0)
        for channel in range(channels):
            sides[0][channel].wait_recv()
            pair[channel] = window[0, channel] + beside[0, channel]
        arrive(states)
        arrive(onward)
        pair[...] += before[...]
        state[0] -= dilution * pair[2]
        sent(states)
        sent(onward)


def run_tiles(initial, forcing, current, cover, targets, weights, count):
    fields, rows, cols = initial.shape
    f32 = jnp.float32
    most = fields + 4
    packed = most + -(-most // (LANES // (2 * ICE_REACH)))
    tall = LANES + 2 * ICE_REACH + 2 * LEAD
    low_count = 256 if cols % 256 == 0 else 128
    high_count = rows * cols // low_count
    vmem = pl.BlockSpec(memory_space=pltpu.VMEM)
    dma = pltpu.SemaphoreType.DMA
    return pl.pallas_call(
        tiles_kernel,
        out_shape=(
            jax.ShapeDtypeStruct((fields, rows, cols), f32),
            jax.ShapeDtypeStruct((3, rows, cols), f32),
        ),
        in_specs=[pl.BlockSpec(memory_space=pl.ANY)] * 6,
        out_specs=(vmem, vmem),
        scratch_shapes=[
            pltpu.VMEM((packed, rows, cols), f32),
            pltpu.VMEM(forcing.shape, f32),
            pltpu.VMEM(current.shape, f32),
            pltpu.VMEM(cover.shape, cover.dtype),
            pltpu.VMEM(targets.shape[1:], targets.dtype),
            pltpu.VMEM(weights.shape[1:], weights.dtype),
            pltpu.VMEM((packed, LANES, LANES), f32),
            pltpu.VMEM((fields, tall, LANES), f32),
            pltpu.VMEM((fields, tall, LANES), f32),
            pltpu.VMEM((5, tall, LANES), f32),
            pltpu.VMEM((3, LANES, LANES), f32),
            pltpu.VMEM((3 + fields, LANES, LANES), f32),
            pltpu.VMEM((3, rows, cols), f32),
            pltpu.VMEM((3, rows, cols), f32),
            pltpu.VMEM((6 * high_count, low_count), f32),
            pltpu.VMEM((2, 3, rows, cols), f32),
            pltpu.VMEM((2, 3, rows, cols), f32),
            pltpu.VMEM((3, rows, cols), f32),
            pltpu.VMEM((low_count, cols), jnp.bfloat16),
            pltpu.VMEM((high_count, cols), jnp.bfloat16),
            dma((6,)),
            *[dma((count,)) for _ in range(8)],
            dma, dma, dma((2, 3)), dma((2, 3)), dma((3,)), dma((3,)),
            pltpu.SemaphoreType.REGULAR,
        ],
        compiler_params=pltpu.CompilerParams(
            collective_id=0, has_side_effects=True, vmem_limit_bytes=40 * 1024 * 1024
        ),
        name="tiles",
    )(initial, forcing, current, cover, targets, weights)


def remap_kernel(average, targets, weights, window, acc, low_index, high_index):
    comp = lax.axis_index("comp")
    channels, rows, cols = average.shape
    span = low_index.shape[1]
    low_count, high_count = low_index.shape[0], high_index.shape[0]
    bf16 = jnp.bfloat16
    blocks = cols // low_count
    low_index[...] = lax.broadcasted_iota(jnp.int32, low_index.shape, 0).astype(bf16)
    high_index[...] = lax.broadcasted_iota(jnp.int32, high_index.shape, 0).astype(bf16)
    acc[...] = jnp.zeros_like(acc)

    def one_row(row, carry):
        for piece in range(cols // span):
            place = pl.ds(piece * span, span)
            target = targets[comp, pl.ds(row, 1), place]
            scale = weights[comp, pl.ds(row, 1), place].astype(jnp.float32) * (1.0 / weight_norm)
            low = lax.rem(target, low_count)
            block = lax.rem(lax.div(target, low_count), blocks)
            line = lax.div(target, cols)
            high = (lax.div(line, rows) * blocks + block) * rows + lax.rem(line, rows)
            low_hot = jnp.where(low_index[...] == low.astype(bf16), bf16(1), bf16(0))
            match = high_index[...] == high.astype(bf16)
            parts = []
            for channel in range(channels):
                value = average[channel, pl.ds(row, 1), place] * scale
                coarse = value.astype(bf16)
                fine = (value - coarse.astype(jnp.float32)).astype(bf16)
                parts.append(jnp.where(match, coarse, bf16(0)))
                parts.append(jnp.where(match, fine, bf16(0)))
            spread = jnp.concatenate(parts, axis=0)
            acc[...] += lax.dot_general(
                spread, low_hot, (((1,), (1,)), ((), ())), preferred_element_type=jnp.float32
            )
        return carry

    lax.fori_loop(0, rows, one_row, 0)
    for channel in range(channels):
        for half in range(2):
            for block in range(blocks):
                base = 2 * channel * high_count + (half * blocks + block) * rows
                window[channel, half, :, block * low_count : (block + 1) * low_count] = (
                    acc[base : base + rows] + acc[base + high_count : base + high_count + rows]
                )


def run_remap(average, targets, weights):
    channels, rows, cols = average.shape
    low_count = 256 if cols % 256 == 0 else 128
    high_count = 2 * rows * cols // low_count
    span = min(1024, cols)
    vmem = pl.BlockSpec(memory_space=pltpu.VMEM)
    return pl.pallas_call(
        remap_kernel,
        out_shape=jax.ShapeDtypeStruct((channels, 2, rows, cols), jnp.float32),
        in_specs=[vmem] * 3,
        out_specs=vmem,
        scratch_shapes=[
            pltpu.VMEM((2 * channels * high_count, low_count), jnp.float32),
            pltpu.VMEM((low_count, span), jnp.bfloat16),
            pltpu.VMEM((high_count, span), jnp.bfloat16),
        ],
        compiler_params=pltpu.CompilerParams(vmem_limit_bytes=40 * 1024 * 1024),
        name="remap",
    )(average, targets, weights)


def join_kernel(
    window, state, average, out_state, out_pair, beside, carry, before,
    side_send, side_recv, next_send, next_recv,
):
    me = lax.axis_index("blk")
    comp = lax.axis_index("comp")
    count = lax.axis_size("blk")
    right, left = lax.rem(me + 1, count), lax.rem(me + count - 1, count)
    barrier = pltpu.get_barrier_semaphore()
    pl.semaphore_signal(barrier, inc=1, device_id={"blk": right}, device_id_type=MESH)
    pl.semaphore_signal(barrier, inc=1, device_id={"blk": left}, device_id_type=MESH)
    pl.semaphore_signal(barrier, inc=1, device_id={"comp": 1 - comp}, device_id_type=MESH)
    pl.semaphore_wait(barrier, 3)
    channels = window.shape[0]
    sides, onward = [], []
    for half in (1, 0):
        for channel in range(channels):
            sides.append(
                pltpu.make_async_remote_copy(
                    window.at[channel, half], beside.at[channel, half],
                    side_send.at[half, channel], side_recv.at[half, channel],
                    device_id={"comp": 1 - comp}, device_id_type=MESH,
                )
            )
    for channel in range(channels):
        onward.append(
            pltpu.make_async_remote_copy(
                carry.at[channel], before.at[channel],
                next_send.at[channel], next_recv.at[channel],
                device_id={"blk": right}, device_id_type=MESH,
            )
        )

    @pl.when(comp == 0)
    def _():
        for copy in sides:
            copy.start()
        out_state[...] = state[...]
        out_pair[...] = average[...]
        for copy in sides:
            copy.wait_send()

    @pl.when(comp == 1)
    def _():
        for channel in range(channels):
            sides[channel].wait_recv()
            carry[channel] = window[channel, 1] + beside[channel, 1]
            onward[channel].start()
        for channel in range(channels):
            sides[channels + channel].wait_recv()
            out_pair[channel] = window[channel, 0] + beside[channel, 0]
        out_state[...] = state[...]
        for channel in range(channels):
            onward[channel].wait_recv()
            out_pair[channel] += before[channel]
        out_state[0] -= dilution * out_pair[2]
        for channel in range(channels):
            onward[channel].wait_send()


def run_join(window, state, average):
    channels, rows, cols = average.shape
    vmem = pl.BlockSpec(memory_space=pltpu.VMEM)
    dma = pltpu.SemaphoreType.DMA
    return pl.pallas_call(
        join_kernel,
        out_shape=(
            jax.ShapeDtypeStruct(state.shape, jnp.float32),
            jax.ShapeDtypeStruct(average.shape, jnp.float32),
        ),
        in_specs=[vmem] * 3,
        out_specs=(vmem, vmem),
        scratch_shapes=[
            pltpu.VMEM(window.shape, jnp.float32),
            pltpu.VMEM(average.shape, jnp.float32),
            pltpu.VMEM(average.shape, jnp.float32),
            dma((2, channels)), dma((2, channels)), dma((channels,)), dma((channels,)),
        ],
        compiler_params=pltpu.CompilerParams(
            collective_id=1, has_side_effects=True, vmem_limit_bytes=40 * 1024 * 1024
        ),
        name="join",
    )(window, state, average)


def body(count, initial, ice_forcing, ocean_current, ice_cover, targets, weights):
    if fits_tiles(count, *initial.shape[2:]):
        state, coupled = run_tiles(
            initial[0], ice_forcing, ocean_current, ice_cover, targets, weights, count
        )
    else:
        state, average = run_turns(initial[0], ice_forcing, ocean_current, ice_cover)
        window = run_remap(average, targets, weights)
        state, coupled = run_join(window, state, average)
    return (state[None], coupled[None])


def solution(mesh):
    placed = (
        P("comp", None, "blk", None),
        P(None, "blk", None),
        P(None, "blk", None),
        P("blk", None),
        P(None, "blk", None),
        P(None, "blk", None),
    )
    return jax.shard_map(
        functools.partial(body, mesh.shape["blk"]),
        mesh=mesh,
        in_specs=placed,
        out_specs=(P("comp", None, "blk", None), P("comp", None, "blk", None)),
        check_vma=False,
    )
```

```python
import functools

import jax
import jax.numpy as jnp
from jax import lax
from jax.experimental import pallas as pl
from jax.experimental.pallas import tpu as pltpu
from jax.sharding import PartitionSpec as P

SUBCYCLES = 16
MESH = pl.DeviceIdType.MESH
PAD = 128
PARTS = 2

coriolis = 0.1
inertia = 4.0
courant = 0.2
dilution = 0.5
weight_norm = 4.0
level_speed = (1.0, 0.8, 0.6, 0.45, 0.3)


def rolled(value, steps, axis):
    return pltpu.roll(value, steps % value.shape[axis], axis)


def rows_diff(value):
    return rolled(value, -1, 0) - rolled(value, 1, 0)


def chunk_width(cols):
    return 256 if cols % 256 == 0 else 128


def stress_stage(work, stat, start, width):
    wide = pl.ds(start, width + 2 * PAD)
    mid = pl.ds(start + PAD, width)
    inner = slice(PAD, PAD + width)
    vel_x, vel_y = work[0, :, wide], work[1, :, wide]
    cx = (rolled(vel_x, -1, 1) - rolled(vel_x, 1, 1))[:, inner]
    cy = (rolled(vel_y, -1, 1) - rolled(vel_y, 1, 1))[:, inner]
    rx = rows_diff(vel_x[:, inner])
    ry = rows_diff(vel_y[:, inner])
    e_d = rx + cy
    e_t = rx - cy
    e_s = cx + ry
    inv = lax.rsqrt(0.25 * (e_d * e_d) + 0.0625 * (e_t * e_t + e_s * e_s) + 0.01)
    third = stat[0, :, pl.ds(start, width)]
    scaled = third * inv
    work[2, :, mid] = work[2, :, mid] * (2.0 / 3.0) + (0.5 * scaled * e_d - third)
    work[3, :, mid] = work[3, :, mid] * (2.0 / 3.0) + 0.125 * scaled * e_t
    work[4, :, mid] = work[4, :, mid] * (2.0 / 3.0) + 0.0625 * scaled * e_s


def velocity_stage(work, stat, total, start, width, rows):
    wide = pl.ds(start, width + 2 * PAD)
    mid = pl.ds(start + PAD, width)
    here = pl.ds(start, width)
    inner = slice(PAD, PAD + width)
    shear = work[4, :, wide]
    one, two = work[2, :, wide], work[3, :, wide]
    across_shear = (rolled(shear, -1, 1) - rolled(shear, 1, 1))[:, inner]
    lower = one - two
    across_yy = (rolled(lower, -1, 1) - rolled(lower, 1, 1))[:, inner]
    force_x = rows_diff((one + two)[:, inner]) + 2.0 * across_shear
    force_y = 2.0 * rows_diff(shear[:, inner]) + across_yy
    old_x, old_y = work[0, :, mid], work[1, :, mid]
    keep, push = stat[1, :, here], stat[2, :, here]
    new_x = keep * (old_x + coriolis * old_y) + push * force_x + stat[3, :, here]
    new_y = keep * (old_y - coriolis * old_x) + push * force_y + stat[4, :, here]
    work[0, :, mid] = new_x
    work[1, :, mid] = new_y
    own_x, own_y = new_x[rows : 2 * rows], new_y[rows : 2 * rows]
    total[0, :, here] += own_x
    total[1, :, here] += own_y
    total[2, :, here] += jnp.sqrt(1.0 + own_x * own_x + own_y * own_y)


def ocean_stage(source, target, coef, start, width):
    wide = pl.ds(start, width + 2 * PAD)
    mid = pl.ds(start + PAD, width)
    here = pl.ds(start, width)
    inner = slice(PAD, PAD + width)
    up, down, east, west = (coef[i, :, here] for i in range(4))
    for level, speed in enumerate(level_speed):
        tracer = source[level, :, wide]
        centre = tracer[:, inner]
        right = rolled(tracer, -1, 1)[:, inner] - centre
        left = centre - rolled(tracer, 1, 1)[:, inner]
        above = rolled(centre, -1, 0) - centre
        below = centre - rolled(centre, 1, 0)
        change = up * below + down * above + east * left + west * right
        target[level, :, mid] = centre - speed * change


def turns_kernel(
    initial_in, forcing_in, current_in, cover_in, state, average,
    initial, forcing, current, cover,
    own, own_stat, halo, halo_stat, work, spare, stat, total, mean,
    load, near_send, near_recv, far_send, far_recv,
    stat_near_send, stat_near_recv, stat_far_send, stat_far_recv,
    mean_send, mean_recv, go,
):
    me = lax.axis_index("blk")
    comp = lax.axis_index("comp")
    count = lax.axis_size("blk")
    fields, rows, cols = initial.shape
    width = chunk_width(cols)
    chunks = cols // width
    near = 1 - lax.rem(me, 2)
    far = 1 - near
    partner = me + 2 * near - 1
    relay_to = me + 4 * near - 2
    relay_from = me - 4 * near + 2
    can_send = jnp.logical_and(relay_to >= 0, relay_to < count)
    can_recv = jnp.logical_and(relay_from >= 0, relay_from < count)
    relay_to = lax.rem(relay_to + count, count)
    relay_from = lax.rem(relay_from + count, count)

    barrier = pltpu.get_barrier_semaphore()

    def greet(where):
        pl.semaphore_signal(barrier, inc=1, device_id=where, device_id_type=MESH)

    greet({"blk": partner})
    greet({"comp": 1 - comp})
    pl.when(can_send)(lambda: greet({"blk": relay_to}))
    pl.when(can_recv)(lambda: greet({"blk": relay_from}))
    loads = [
        pltpu.make_async_copy(source, target, load.at[i])
        for i, (source, target) in enumerate(
            (
                (initial_in, initial),
                (current_in, current),
                (forcing_in, forcing),
                (cover_in, cover),
            )
        )
    ]
    for copy in loads:
        copy.start()

    work[...] = jnp.zeros_like(work)
    total[...] = jnp.zeros_like(total)

    def enter():
        pl.semaphore_wait(barrier, 2 + can_send.astype(jnp.int32) + can_recv.astype(jnp.int32))

    def copies(source, target, pieces, near_sems, far_sems):
        first, second = [], []
        wide = cols // PARTS
        for index in range(pieces * PARTS):
            piece, place = index // PARTS, pl.ds(index % PARTS * wide, wide)
            first.append(
                pltpu.make_async_remote_copy(
                    source.at[piece, :, place], target.at[far, piece, :, place],
                    near_sems[0].at[index], near_sems[1].at[index],
                    device_id={"blk": partner}, device_id_type=MESH,
                )
            )
            second.append(
                pltpu.make_async_remote_copy(
                    target.at[near, piece, :, place], target.at[far, piece, :, place],
                    far_sems[0].at[index], far_sems[1].at[index],
                    device_id={"blk": relay_to}, device_id_type=MESH,
                )
            )
        return first, second

    def start(pair):
        for copy in pair[0]:
            copy.start()

    def relay(pair):
        for first, second in zip(*pair):
            first.wait_recv()
            pl.when(can_send)(second.start)

    def arrive(pair):
        @pl.when(can_recv)
        def _():
            for copy in pair[1]:
                copy.wait_recv()

    def sent(pair):
        for copy in pair[0]:
            copy.wait_send()

        @pl.when(can_send)
        def _():
            for copy in pair[1]:
                copy.wait_send()

    def clear_edges(turns):
        @pl.when(jnp.logical_not(can_recv))
        def _():
            halo_stat[far] = jnp.zeros(halo_stat.shape[1:], jnp.float32)
            for turn in range(turns):
                halo[turn, far] = jnp.zeros(halo.shape[2:], jnp.float32)

    inside = slice(PAD, PAD + cols)

    def fill_own(source):
        for field in range(fields):
            work[field, rows : 2 * rows, inside] = source[field]

    def fill_sides(turn):
        for field in range(fields):
            work[field, 0:rows, inside] = halo[turn, 0, field]
            work[field, 2 * rows : 3 * rows, inside] = halo[turn, 1, field]

    def exchange_of(turn, source):
        return copies(
            source, halo.at[turn], fields,
            (near_send.at[turn], near_recv.at[turn]), (far_send.at[turn], far_recv.at[turn]),
        )

    def stats_of(source, pieces):
        return copies(
            source, halo_stat, pieces,
            (stat_near_send, stat_near_recv), (stat_far_send, stat_far_recv),
        )

    mean_copy = pltpu.make_async_remote_copy(
        mean, average, mean_send, mean_recv,
        device_id={"comp": 1 - comp}, device_id_type=MESH,
    )

    @pl.when(comp == 0)
    def _():
        depth = rows // 2
        turns = SUBCYCLES // depth
        clear_edges(turns)
        loads[0].wait()
        enter()
        pairs = [exchange_of(0, initial)]
        start(pairs[0])
        for copy in loads[1:]:
            copy.wait()
        covered = cover[...].astype(jnp.float32)
        push = covered / (inertia * forcing[0] + 1.0)
        own_stat[0] = forcing[1] * covered * (1.0 / 3.0)
        own_stat[1] = push
        own_stat[2] = push * (forcing[2] + current[0])
        own_stat[3] = push * (forcing[3] + current[1])
        stat_pair = stats_of(own_stat, 4)
        start(stat_pair)
        for turn in range(turns):
            source = initial if turn == 0 else own.at[turn - 1]
            if turn > 0:
                pairs.append(exchange_of(turn, source))
                start(pairs[turn])
            relay(pairs[turn])
            if turn == 0:
                relay(stat_pair)
                pl.semaphore_signal(
                    go, inc=1, device_id={"comp": 1 - comp}, device_id_type=MESH
                )
            fill_own(source)
            arrive(pairs[turn])
            if turn == 0:
                arrive(stat_pair)
                for place, block in enumerate((halo_stat.at[0], own_stat, halo_stat.at[1])):
                    span = slice(place * rows, (place + 1) * rows)
                    push = block[1]
                    stat[0, span] = block[0]
                    stat[1, span] = jnp.where(push > 0.0, 1.0 - push, 0.0)
                    stat[2, span] = 0.25 * push
                    stat[3, span] = block[2]
                    stat[4, span] = block[3]
            fill_sides(turn)

            def subcycle(step, carry):
                for chunk in range(chunks):
                    stress_stage(work, stat, chunk * width, width)
                for chunk in range(chunks):
                    velocity_stage(work, stat, total, chunk * width, width, rows)
                return carry

            lax.fori_loop(0, depth, subcycle, 0)
            final = state if turn == turns - 1 else own.at[turn]
            for field in range(fields):
                final[field] = work[field, rows : 2 * rows, inside]
        share = 1.0 / SUBCYCLES
        covered = cover[...].astype(jnp.float32)
        mean[0] = total[0] * share - covered * current[0]
        mean[1] = total[1] * share - covered * current[1]
        mean[2] = forcing[4] * covered * (total[2] * share)
        mean_copy.start()
        average[...] = mean[...]
        sent(stat_pair)
        for pair in pairs:
            sent(pair)
        mean_copy.wait_send()

    @pl.when(comp == 1)
    def _():
        depth = rows
        turns = SUBCYCLES // depth
        clear_edges(turns)
        spare[...] = jnp.zeros_like(spare)
        for copy in loads:
            copy.wait()
        enter()
        pl.semaphore_wait(go, 1)
        pairs = [exchange_of(0, initial)]
        start(pairs[0])
        stat_pair = stats_of(current, 2)
        start(stat_pair)
        for turn in range(turns):
            source = initial if turn == 0 else own.at[turn - 1]
            if turn > 0:
                pairs.append(exchange_of(turn, source))
                start(pairs[turn])
            relay(pairs[turn])
            if turn == 0:
                relay(stat_pair)
            fill_own(source)
            arrive(pairs[turn])
            if turn == 0:
                arrive(stat_pair)
                for place in range(3):
                    span = slice(place * rows, (place + 1) * rows)
                    for axis in range(2):
                        if place == 1:
                            speed = current[axis]
                        else:
                            speed = halo_stat[place // 2, axis]
                        stat[2 * axis, span] = courant * jnp.maximum(speed, 0.0)
                        stat[2 * axis + 1, span] = courant * jnp.minimum(speed, 0.0)
            fill_sides(turn)

            def substeps(step, carry):
                for chunk in range(chunks):
                    ocean_stage(work, spare, stat, chunk * width, width)
                for chunk in range(chunks):
                    ocean_stage(spare, work, stat, chunk * width, width)
                return carry

            lax.fori_loop(0, depth // 2, substeps, 0)
            final = state if turn == turns - 1 else own.at[turn]
            for field in range(fields):
                final[field] = work[field, rows : 2 * rows, inside]
        sent(stat_pair)
        for pair in pairs:
            sent(pair)
        mean_copy.wait_recv()


def run_turns(initial, forcing, current, cover):
    fields, rows, cols = initial.shape
    most = SUBCYCLES // (rows // 2)
    f32 = jnp.float32
    vmem = pl.BlockSpec(memory_space=pltpu.VMEM)
    dma = pltpu.SemaphoreType.DMA
    return pl.pallas_call(
        turns_kernel,
        out_shape=(
            jax.ShapeDtypeStruct((fields, rows, cols), f32),
            jax.ShapeDtypeStruct((3, rows, cols), f32),
        ),
        in_specs=[pl.BlockSpec(memory_space=pl.ANY)] * 4,
        out_specs=(vmem, vmem),
        scratch_shapes=[
            pltpu.VMEM(initial.shape, f32),
            pltpu.VMEM(forcing.shape, f32),
            pltpu.VMEM(current.shape, f32),
            pltpu.VMEM(cover.shape, cover.dtype),
            pltpu.VMEM((most, fields, rows, cols), f32),
            pltpu.VMEM((4, rows, cols), f32),
            pltpu.VMEM((most, 2, fields, rows, cols), f32),
            pltpu.VMEM((2, 4, rows, cols), f32),
            pltpu.VMEM((fields, 3 * rows, cols + 2 * PAD), f32),
            pltpu.VMEM((fields, 3 * rows, cols + 2 * PAD), f32),
            pltpu.VMEM((5, 3 * rows, cols), f32),
            pltpu.VMEM((3, rows, cols), f32),
            pltpu.VMEM((3, rows, cols), f32),
            dma((4,)),
            *[dma((most, fields * PARTS)) for _ in range(4)],
            *[dma((4 * PARTS,)) for _ in range(4)],
            dma, dma, pltpu.SemaphoreType.REGULAR,
        ],
        compiler_params=pltpu.CompilerParams(
            collective_id=0, has_side_effects=True
        ),
        name="turns",
    )(initial, forcing, current, cover)


LANES = 128
LEAD = 8
ICE_REACH = 2 * SUBCYCLES
SEA_REACH = SUBCYCLES


def fits_tiles(count, rows, cols):
    return count * rows == LANES and cols == count * LANES and count > 1


def lane_index(shape):
    return lax.broadcasted_iota(jnp.int32, shape, len(shape) - 1)


def lane_diff(value):
    lane = lane_index(value.shape)
    after = jnp.where(lane == LANES - 1, 0.0, pltpu.roll(value, LANES - 1, 1))
    before = jnp.where(lane == 0, 0.0, pltpu.roll(value, 1, 1))
    return after - before


def tile_stress(work, stat, low, size):
    here, up, down = (pl.ds(low + shift, size) for shift in (0, 1, -1))
    vel_x, vel_y = work[0, here], work[1, here]
    cx = work[0, up] - work[0, down]
    cy = work[1, up] - work[1, down]
    rx, ry = lane_diff(vel_x), lane_diff(vel_y)
    e_d = rx + cy
    e_t = rx - cy
    e_s = cx + ry
    inv = lax.rsqrt(0.25 * (e_d * e_d) + 0.0625 * (e_t * e_t + e_s * e_s) + 0.01)
    third = stat[0, here]
    scaled = third * inv
    one = 0.5 * scaled * e_d - third
    two = 0.125 * scaled * e_t
    work[2, here] = work[2, here] * (2.0 / 3.0) + (one + two)
    work[3, here] = work[3, here] * (2.0 / 3.0) + (one - two)
    work[4, here] = work[4, here] * (2.0 / 3.0) + 0.0625 * scaled * e_s


def tile_velocity(work, stat, total, low, size, own):
    here, up, down = (pl.ds(low + shift, size) for shift in (0, 1, -1))
    force_x = lane_diff(work[2, here]) + 2.0 * (work[4, up] - work[4, down])
    force_y = 2.0 * lane_diff(work[4, here]) + (work[3, up] - work[3, down])
    old_x, old_y = work[0, here], work[1, here]
    keep, push = stat[1, here], stat[2, here]
    new_x = keep * (old_x + coriolis * old_y) + push * force_x + stat[3, here]
    new_y = keep * (old_y - coriolis * old_x) + push * force_y + stat[4, here]
    work[0, here] = new_x
    work[1, here] = new_y
    if own is not None:
        place = pl.ds(own, size)
        total[0, place] += new_x
        total[1, place] += new_y
        square = 1.0 + new_x * new_x + new_y * new_y
        total[2, place] += square * lax.rsqrt(square)


def tile_ocean(source, target, stat, low, size):
    here, up, down = (pl.ds(low + shift, size) for shift in (0, 1, -1))
    before, after, left, right, drain = (stat[i, here] for i in range(5))
    for level, speed in enumerate(level_speed):
        centre = source[level, here]
        inflow = before * pltpu.roll(centre, 1, 1) + after * pltpu.roll(centre, LANES - 1, 1)
        inflow += left * source[level, down] + right * source[level, up]
        target[level, here] = centre + speed * (inflow - drain * centre)


def pieces(low, high, step):
    return [(start, min(step, high - start)) for start in range(low, high, step)]


def tiles_kernel(
    initial_in, forcing_in, current_in, cover_in, targets_in, weights_in, state, pair,
    pack, forcing, current, cover, targets, weights,
    recv, work, spare, stat, total, back, home, mean, acc, window, beside, before,
    low, high, hot, parts,
    load, first_send, first_recv, second_send, second_recv,
    total_send, total_recv, state_send, state_recv, mean_send, mean_recv,
    side_send, side_recv, next_send, next_recv, go,
):
    me = lax.axis_index("blk")
    comp = lax.axis_index("comp")
    count = lax.axis_size("blk")
    fields, rows, cols = initial_in.shape
    barrier = pltpu.get_barrier_semaphore()

    def greet(where):
        pl.semaphore_signal(barrier, inc=1, device_id=where, device_id_type=MESH)

    def other(step):
        return lax.rem(me + step, count)

    steps = range(1, count)
    for step in steps:
        greet({"blk": other(step)})
    greet({"comp": 1 - comp})

    loads = [
        pltpu.make_async_copy(source, target, load.at[i])
        for i, (source, target) in enumerate(
            (
                (initial_in, pack.at[0:fields]),
                (current_in, current),
                (forcing_in, forcing),
                (cover_in, cover),
                (targets_in.at[comp], targets),
                (weights_in.at[comp], weights),
            )
        )
    ]
    for copy in loads:
        copy.start()

    def lanes_of(block):
        return pl.ds(pl.multiple_of(block * LANES, LANES), LANES)

    def rows_of(block):
        return pl.ds(pl.multiple_of(block * rows, rows), rows)

    def outward(low, high, sems):
        return [
            pltpu.make_async_remote_copy(
                pack.at[low:high, :, lanes_of(other(step))],
                recv.at[low:high, rows_of(me), :],
                sems[0].at[step], sems[1].at[step],
                device_id={"blk": other(step)}, device_id_type=MESH,
            )
            for step in steps
        ]

    def homeward(source, target, sems):
        return [
            pltpu.make_async_remote_copy(
                source.at[:, rows_of(other(step)), :],
                target.at[:, :, lanes_of(me)],
                sems[0].at[step], sems[1].at[step],
                device_id={"blk": other(step)}, device_id_type=MESH,
            )
            for step in steps
        ]

    def start(copies):
        for copy in copies:
            copy.start()

    def arrive(copies):
        for copy in copies:
            copy.wait_recv()

    def sent(copies):
        for copy in copies:
            copy.wait_send()

    def spread_edges(base, filled, reach):
        group = LANES // (2 * reach)
        lane = lane_index((rows, LANES))
        slot = lane // (2 * reach)
        leading = lane % (2 * reach) < reach
        zero = jnp.zeros((rows, LANES), jnp.float32)
        for tile in range(-(-filled // group)):
            members = range(tile * group, min(filled, (tile + 1) * group))
            turned = []
            for block in range(count):
                here = slice(block * LANES, (block + 1) * LANES)
                merged = zero
                for place, field in enumerate(members):
                    shift = (2 * place + 1) * reach % LANES
                    value = pack[field, :, here]
                    moved = pltpu.roll(value, shift, 1) if shift else value
                    merged = jnp.where(slot == place, moved, merged)
                turned.append(merged)
            for block in range(count):
                before = turned[block - 1] if block > 0 else zero
                after = turned[block + 1] if block < count - 1 else zero
                here = slice(block * LANES, (block + 1) * LANES)
                pack[base + tile, :, here] = jnp.where(leading, before, after)

    def unpack(field, base, reach):
        group = LANES // (2 * reach)
        value = recv[field].T
        edge = recv[base + field // group].T
        low = field % group * 2 * reach
        return jnp.concatenate(
            [edge[low : low + reach], value, edge[low + reach : low + 2 * reach]], axis=0
        )

    channels = pair.shape[0]
    mean_copy = pltpu.make_async_remote_copy(
        mean, home, mean_send, mean_recv,
        device_id={"comp": 1 - comp}, device_id_type=MESH,
    )
    sides = [
        [
            pltpu.make_async_remote_copy(
                window.at[half, channel], beside.at[half, channel],
                side_send.at[half, channel], side_recv.at[half, channel],
                device_id={"comp": 1 - comp}, device_id_type=MESH,
            )
            for channel in range(channels)
        ]
        for half in range(2)
    ]
    onward = [
        pltpu.make_async_remote_copy(
            window.at[1, channel], before.at[channel],
            next_send.at[channel], next_recv.at[channel],
            device_id={"blk": other(1)}, device_id_type=MESH,
        )
        for channel in range(channels)
    ]

    def prepare_remap():
        low_count = hot.shape[1]
        blocks = cols // low_count
        target = targets[...]
        block = lax.rem(lax.div(target, low_count), blocks)
        line = lax.div(target, cols)
        low[...] = lax.rem(target, low_count).astype(jnp.float32)
        for half in range(2):
            inside = lax.div(line, rows) == half
            place = block * rows + line - half * rows
            high[half] = jnp.where(inside, place, blocks * rows).astype(jnp.float32)

        def one_row(row, carry):
            lane = lane_index((LANES, LANES)).astype(jnp.float32)
            line = low[pl.ds(row, 1), :]
            for start in range(0, cols, LANES):
                value = jnp.broadcast_to(line[:, start : start + LANES], (LANES, LANES)).T
                place = pl.ds(pl.multiple_of(row * cols + start, LANES), LANES)
                for first in range(0, low_count, LANES):
                    hit = jnp.where(value == lane + float(first), 1.0, 0.0)
                    hot[place, first : first + LANES] = hit.astype(hot.dtype)
            return carry

        lax.fori_loop(0, rows, one_row, 0)

    def split_values(values):
        scale = weights[...].astype(jnp.float32) * (1.0 / weight_norm)
        for channel in range(channels):
            value = values[channel] * scale
            coarse = value.astype(jnp.bfloat16).astype(jnp.float32)
            parts[2 * channel] = coarse
            parts[2 * channel + 1] = value - coarse

    def remap(half):
        low_count = hot.shape[1]
        blocks = cols // low_count
        high_count = blocks * rows
        bf16 = jnp.bfloat16
        tall = 16
        acc[...] = jnp.zeros_like(acc)

        def one_row(row, carry):
            place = pl.ds(row, 1)
            level = jnp.broadcast_to(high[half, place, :], (tall, cols)).astype(bf16)
            index = lax.broadcasted_iota(jnp.int32, (tall, cols), 0).astype(bf16)
            matches = [level == index + bf16(first) for first in range(0, high_count, tall)]
            spread = []
            for part in range(2 * channels):
                value = jnp.broadcast_to(parts[part, place, :], (tall, cols)).astype(bf16)
                spread += [jnp.where(match, value, bf16(0)) for match in matches]
            span = pl.ds(pl.multiple_of(row * cols, cols), cols)
            acc[...] += jnp.dot(
                jnp.concatenate(spread, axis=0), hot[span, :], preferred_element_type=jnp.float32
            )
            return carry

        lax.fori_loop(0, rows, one_row, 0)
        for channel in range(channels):
            for block in range(blocks):
                base = 2 * channel * high_count + block * rows
                window[half, channel, :, block * low_count : (block + 1) * low_count] = (
                    acc[base : base + rows] + acc[base + high_count : base + high_count + rows]
                )

    @pl.when(comp == 0)
    def _():
        filled = fields + 4
        packed = filled + -(-filled // (LANES // (2 * ICE_REACH)))
        span = LANES + 2 * ICE_REACH
        loads[0].wait()
        pl.semaphore_wait(barrier, count)
        first = outward(0, fields, (first_send, first_recv))
        start(first)
        for copy in loads[1:4]:
            copy.wait()
        covered = cover[...].astype(jnp.float32)
        push = covered / (inertia * forcing[0] + 1.0)
        pack[fields] = forcing[1] * covered * (1.0 / 3.0)
        pack[fields + 1] = push
        pack[fields + 2] = push * (forcing[2] + current[0])
        pack[fields + 3] = push * (forcing[3] + current[1])
        spread_edges(filled, filled, ICE_REACH)
        second = outward(fields, packed, (second_send, second_recv))
        start(second)
        recv[0:packed, rows_of(me), :] = pack[0:packed, :, lanes_of(me)]
        total[...] = jnp.zeros_like(total)
        for array in (work, stat):
            for edge in (0, LEAD + span):
                array[:, edge : edge + LEAD] = jnp.zeros((array.shape[0], LEAD, LANES), jnp.float32)
        for copy in loads[4:]:
            copy.wait()
        prepare_remap()
        sent(first)
        sent(second)
        pl.semaphore_signal(go, inc=1, device_id={"comp": 1 - comp}, device_id_type=MESH)
        arrive(first)
        arrive(second)
        whole = slice(LEAD, LEAD + span)
        for field in range(2):
            work[field, whole] = unpack(field, filled, ICE_REACH)
        one, two = unpack(2, filled, ICE_REACH), unpack(3, filled, ICE_REACH)
        work[2, whole] = one + two
        work[3, whole] = one - two
        work[4, whole] = unpack(4, filled, ICE_REACH)
        stat[0, whole] = unpack(fields, filled, ICE_REACH)
        push = unpack(fields + 1, filled, ICE_REACH)
        stat[1, whole] = jnp.where(push > 0.0, 1.0 - push, 0.0)
        stat[2, whole] = 0.25 * push
        stat[3, whole] = unpack(fields + 2, filled, ICE_REACH)
        stat[4, whole] = unpack(fields + 3, filled, ICE_REACH)

        for group in range(SUBCYCLES // 4):
            low, high = LEAD + 8 * group, LEAD + span - 8 * group
            inner, outer = LEAD + ICE_REACH, LEAD + ICE_REACH + LANES

            def subcycle(step, carry, low=low, high=high):
                for begin, size in pieces(low, high, 16):
                    tile_stress(work, stat, begin, size)
                for begin, size in pieces(low, inner, 16) + pieces(outer, high, 16):
                    tile_velocity(work, stat, total, begin, size, None)
                for begin, size in pieces(inner, outer, 16):
                    tile_velocity(work, stat, total, begin, size, begin - inner)
                return carry

            lax.fori_loop(0, 4, subcycle, 0)

        own = slice(LEAD + ICE_REACH, LEAD + ICE_REACH + LANES)
        for channel in range(3):
            back[channel] = total[channel].T
        totals = homeward(back.at[0:3], home, (total_send, total_recv))
        start(totals)
        one, two = work[2, own], work[3, own]
        for field, value in enumerate(
            (work[0, own], work[1, own], 0.5 * (one + two), 0.5 * (one - two), work[4, own])
        ):
            back[3 + field] = value.T
        states = homeward(back.at[3 : 3 + fields], state, (state_send, state_recv))
        start(states)
        home[:, :, lanes_of(me)] = back[0:3, rows_of(me), :]
        state[:, :, lanes_of(me)] = back[3 : 3 + fields, rows_of(me), :]
        share = 1.0 / SUBCYCLES
        covered = cover[...].astype(jnp.float32)
        arrive(totals)
        mean[0] = home[0] * share - covered * current[0]
        mean[1] = home[1] * share - covered * current[1]
        mean[2] = forcing[4] * covered * (home[2] * share)
        mean_copy.start()
        pair[...] = mean[...]
        split_values(mean)
        for half in (1, 0):
            remap(half)
            start(sides[half])
        sent(totals)
        arrive(states)
        sent(states)
        mean_copy.wait_send()
        sent(sides[0] + sides[1])

    @pl.when(comp == 1)
    def _():
        filled = fields + 2
        packed = filled + -(-filled // (LANES // (2 * SEA_REACH)))
        span = LANES + 2 * SEA_REACH
        for copy in loads:
            copy.wait()
        for axis in range(2):
            pack[fields + axis] = current[axis]
        spread_edges(filled, filled, SEA_REACH)
        for array in (work, spare):
            for edge in (0, LEAD + span):
                array[:, edge : edge + LEAD] = jnp.zeros((array.shape[0], LEAD, LANES), jnp.float32)
        recv[0:packed, rows_of(me), :] = pack[0:packed, :, lanes_of(me)]
        prepare_remap()
        pl.semaphore_wait(barrier, count)
        pl.semaphore_wait(go, 1)
        first = outward(0, packed, (first_send, first_recv))
        start(first)
        arrive(first)
        whole = slice(LEAD, LEAD + span)
        for field in range(fields):
            work[field, whole] = unpack(field, filled, SEA_REACH)
        lane = lane_index((span, LANES))
        speed = courant * unpack(fields, filled, SEA_REACH)
        drain = jnp.abs(speed)
        stat[0, whole] = jnp.where(lane == 0, 0.0, jnp.maximum(speed, 0.0))
        stat[1, whole] = jnp.where(lane == LANES - 1, 0.0, -jnp.minimum(speed, 0.0))
        speed = courant * unpack(fields + 1, filled, SEA_REACH)
        stat[2, whole] = jnp.maximum(speed, 0.0)
        stat[3, whole] = -jnp.minimum(speed, 0.0)
        stat[4, whole] = drain + jnp.abs(speed)
        for group in range(SUBCYCLES // 8):
            low, high = LEAD + 8 * group, LEAD + span - 8 * group

            def substeps(step, carry, low=low, high=high):
                for begin, size in pieces(low, high, 16):
                    tile_ocean(work, spare, stat, begin, size)
                for begin, size in pieces(low, high, 16):
                    tile_ocean(spare, work, stat, begin, size)
                return carry

            lax.fori_loop(0, 4, substeps, 0)
        own = slice(LEAD + SEA_REACH, LEAD + SEA_REACH + LANES)
        for field in range(fields):
            back[3 + field] = work[field, own].T
        states = homeward(back.at[3 : 3 + fields], state, (state_send, state_recv))
        start(states)
        state[:, :, lanes_of(me)] = back[3 : 3 + fields, rows_of(me), :]
        sent(first)
        mean_copy.wait_recv()
        split_values(home)
        remap(1)
        for channel in range(channels):
            sides[1][channel].wait_recv()
            window[1, channel] += beside[1, channel]
            onward[channel].start()
        remap(0)
        for channel in range(channels):
            sides[0][channel].wait_recv()
            pair[channel] = window[0, channel] + beside[0, channel]
        arrive(states)
        arrive(onward)
        pair[...] += before[...]
        state[0] -= dilution * pair[2]
        sent(states)
        sent(onward)


def run_tiles(initial, forcing, current, cover, targets, weights, count):
    fields, rows, cols = initial.shape
    f32 = jnp.float32
    most = fields + 4
    packed = most + -(-most // (LANES // (2 * ICE_REACH)))
    tall = LANES + 2 * ICE_REACH + 2 * LEAD
    low_count = 256 if cols % 256 == 0 else 128
    high_count = rows * cols // low_count
    vmem = pl.BlockSpec(memory_space=pltpu.VMEM)
    dma = pltpu.SemaphoreType.DMA
    return pl.pallas_call(
        tiles_kernel,
        out_shape=(pltpu.VMEM((fields, rows, cols), f32), pltpu.VMEM((3, rows, cols), f32)),
        in_specs=[pl.BlockSpec(memory_space=pl.ANY)] * 6,
        out_specs=(vmem, vmem),
        scratch_shapes=[
            pltpu.VMEM((packed, rows, cols), f32),
            pltpu.VMEM(forcing.shape, f32),
            pltpu.VMEM(current.shape, f32),
            pltpu.VMEM(cover.shape, cover.dtype),
            pltpu.VMEM(targets.shape[1:], targets.dtype),
            pltpu.VMEM(weights.shape[1:], weights.dtype),
            pltpu.VMEM((packed, LANES, LANES), f32),
            pltpu.VMEM((fields, tall, LANES), f32),
            pltpu.VMEM((fields, tall, LANES), f32),
            pltpu.VMEM((5, tall, LANES), f32),
            pltpu.VMEM((3, LANES, LANES), f32),
            pltpu.VMEM((3 + fields, LANES, LANES), f32),
            pltpu.VMEM((3, rows, cols), f32),
            pltpu.VMEM((3, rows, cols), f32),
            pltpu.VMEM((6 * high_count, low_count), f32),
            pltpu.VMEM((2, 3, rows, cols), f32),
            pltpu.VMEM((2, 3, rows, cols), f32),
            pltpu.VMEM((3, rows, cols), f32),
            pltpu.VMEM((rows, cols), f32),
            pltpu.VMEM((2, rows, cols), f32),
            pltpu.VMEM((rows * cols, low_count), jnp.bfloat16),
            pltpu.VMEM((6, rows, cols), f32),
            dma((6,)),
            *[dma((count,)) for _ in range(8)],
            dma, dma, dma((2, 3)), dma((2, 3)), dma((3,)), dma((3,)),
            pltpu.SemaphoreType.REGULAR,
        ],
        compiler_params=pltpu.CompilerParams(collective_id=0, has_side_effects=True),
        name="tiles",
    )(initial, forcing, current, cover, targets, weights)


def remap_kernel(average, targets, weights, window, acc, low_index, high_index):
    comp = lax.axis_index("comp")
    channels, rows, cols = average.shape
    span = low_index.shape[1]
    low_count, high_count = low_index.shape[0], high_index.shape[0]
    bf16 = jnp.bfloat16
    blocks = cols // low_count
    low_index[...] = lax.broadcasted_iota(jnp.int32, low_index.shape, 0).astype(bf16)
    high_index[...] = lax.broadcasted_iota(jnp.int32, high_index.shape, 0).astype(bf16)
    acc[...] = jnp.zeros_like(acc)

    def one_row(row, carry):
        for piece in range(cols // span):
            place = pl.ds(piece * span, span)
            target = targets[comp, pl.ds(row, 1), place]
            scale = weights[comp, pl.ds(row, 1), place].astype(jnp.float32) * (1.0 / weight_norm)
            low = lax.rem(target, low_count)
            block = lax.rem(lax.div(target, low_count), blocks)
            line = lax.div(target, cols)
            high = (lax.div(line, rows) * blocks + block) * rows + lax.rem(line, rows)
            low_hot = jnp.where(low_index[...] == low.astype(bf16), bf16(1), bf16(0))
            match = high_index[...] == high.astype(bf16)
            parts = []
            for channel in range(channels):
                value = average[channel, pl.ds(row, 1), place] * scale
                coarse = value.astype(bf16)
                fine = (value - coarse.astype(jnp.float32)).astype(bf16)
                parts.append(jnp.where(match, coarse, bf16(0)))
                parts.append(jnp.where(match, fine, bf16(0)))
            spread = jnp.concatenate(parts, axis=0)
            acc[...] += lax.dot_general(
                spread, low_hot, (((1,), (1,)), ((), ())), preferred_element_type=jnp.float32
            )
        return carry

    lax.fori_loop(0, rows, one_row, 0)
    for channel in range(channels):
        for half in range(2):
            for block in range(blocks):
                base = 2 * channel * high_count + (half * blocks + block) * rows
                window[channel, half, :, block * low_count : (block + 1) * low_count] = (
                    acc[base : base + rows] + acc[base + high_count : base + high_count + rows]
                )


def run_remap(average, targets, weights):
    channels, rows, cols = average.shape
    low_count = 256 if cols % 256 == 0 else 128
    high_count = 2 * rows * cols // low_count
    span = min(1024, cols)
    vmem = pl.BlockSpec(memory_space=pltpu.VMEM)
    return pl.pallas_call(
        remap_kernel,
        out_shape=jax.ShapeDtypeStruct((channels, 2, rows, cols), jnp.float32),
        in_specs=[vmem] * 3,
        out_specs=vmem,
        scratch_shapes=[
            pltpu.VMEM((2 * channels * high_count, low_count), jnp.float32),
            pltpu.VMEM((low_count, span), jnp.bfloat16),
            pltpu.VMEM((high_count, span), jnp.bfloat16),
        ],
        compiler_params=pltpu.CompilerParams(vmem_limit_bytes=40 * 1024 * 1024),
        name="remap",
    )(average, targets, weights)


def join_kernel(
    window, state, average, out_state, out_pair, beside, carry, before,
    side_send, side_recv, next_send, next_recv,
):
    me = lax.axis_index("blk")
    comp = lax.axis_index("comp")
    count = lax.axis_size("blk")
    right, left = lax.rem(me + 1, count), lax.rem(me + count - 1, count)
    barrier = pltpu.get_barrier_semaphore()
    pl.semaphore_signal(barrier, inc=1, device_id={"blk": right}, device_id_type=MESH)
    pl.semaphore_signal(barrier, inc=1, device_id={"blk": left}, device_id_type=MESH)
    pl.semaphore_signal(barrier, inc=1, device_id={"comp": 1 - comp}, device_id_type=MESH)
    pl.semaphore_wait(barrier, 3)
    channels = window.shape[0]
    sides, onward = [], []
    for half in (1, 0):
        for channel in range(channels):
            sides.append(
                pltpu.make_async_remote_copy(
                    window.at[channel, half], beside.at[channel, half],
                    side_send.at[half, channel], side_recv.at[half, channel],
                    device_id={"comp": 1 - comp}, device_id_type=MESH,
                )
            )
    for channel in range(channels):
        onward.append(
            pltpu.make_async_remote_copy(
                carry.at[channel], before.at[channel],
                next_send.at[channel], next_recv.at[channel],
                device_id={"blk": right}, device_id_type=MESH,
            )
        )

    @pl.when(comp == 0)
    def _():
        for copy in sides:
            copy.start()
        out_state[...] = state[...]
        out_pair[...] = average[...]
        for copy in sides:
            copy.wait_send()

    @pl.when(comp == 1)
    def _():
        for channel in range(channels):
            sides[channel].wait_recv()
            carry[channel] = window[channel, 1] + beside[channel, 1]
            onward[channel].start()
        for channel in range(channels):
            sides[channels + channel].wait_recv()
            out_pair[channel] = window[channel, 0] + beside[channel, 0]
        out_state[...] = state[...]
        for channel in range(channels):
            onward[channel].wait_recv()
            out_pair[channel] += before[channel]
        out_state[0] -= dilution * out_pair[2]
        for channel in range(channels):
            onward[channel].wait_send()


def run_join(window, state, average):
    channels, rows, cols = average.shape
    vmem = pl.BlockSpec(memory_space=pltpu.VMEM)
    dma = pltpu.SemaphoreType.DMA
    return pl.pallas_call(
        join_kernel,
        out_shape=(
            jax.ShapeDtypeStruct(state.shape, jnp.float32),
            jax.ShapeDtypeStruct(average.shape, jnp.float32),
        ),
        in_specs=[vmem] * 3,
        out_specs=(vmem, vmem),
        scratch_shapes=[
            pltpu.VMEM(window.shape, jnp.float32),
            pltpu.VMEM(average.shape, jnp.float32),
            pltpu.VMEM(average.shape, jnp.float32),
            dma((2, channels)), dma((2, channels)), dma((channels,)), dma((channels,)),
        ],
        compiler_params=pltpu.CompilerParams(
            collective_id=1, has_side_effects=True, vmem_limit_bytes=40 * 1024 * 1024
        ),
        name="join",
    )(window, state, average)


def body(count, initial, ice_forcing, ocean_current, ice_cover, targets, weights):
    if fits_tiles(count, *initial.shape[2:]):
        state, coupled = run_tiles(
            initial[0], ice_forcing, ocean_current, ice_cover, targets, weights, count
        )
    else:
        state, average = run_turns(initial[0], ice_forcing, ocean_current, ice_cover)
        window = run_remap(average, targets, weights)
        state, coupled = run_join(window, state, average)
    return (state[None], coupled[None])


def solution(mesh):
    placed = (
        P("comp", None, "blk", None),
        P(None, "blk", None),
        P(None, "blk", None),
        P("blk", None),
        P(None, "blk", None),
        P(None, "blk", None),
    )
    return jax.shard_map(
        functools.partial(body, mesh.shape["blk"]),
        mesh=mesh,
        in_specs=placed,
        out_specs=(P("comp", None, "blk", None), P("comp", None, "blk", None)),
        check_vma=False,
    )
```

```python
import functools

import jax
import jax.numpy as jnp
from jax import lax
from jax.experimental import pallas as pl
from jax.experimental.pallas import tpu as pltpu
from jax.sharding import PartitionSpec as P

SUBCYCLES = 16
MESH = pl.DeviceIdType.MESH
PAD = 128
PARTS = 2

coriolis = 0.1
inertia = 4.0
courant = 0.2
dilution = 0.5
weight_norm = 4.0
level_speed = (1.0, 0.8, 0.6, 0.45, 0.3)


def rolled(value, steps, axis):
    return pltpu.roll(value, steps % value.shape[axis], axis)


def rows_diff(value):
    return rolled(value, -1, 0) - rolled(value, 1, 0)


def chunk_width(cols):
    return 256 if cols % 256 == 0 else 128


def stress_stage(work, stat, start, width):
    wide = pl.ds(start, width + 2 * PAD)
    mid = pl.ds(start + PAD, width)
    inner = slice(PAD, PAD + width)
    vel_x, vel_y = work[0, :, wide], work[1, :, wide]
    cx = (rolled(vel_x, -1, 1) - rolled(vel_x, 1, 1))[:, inner]
    cy = (rolled(vel_y, -1, 1) - rolled(vel_y, 1, 1))[:, inner]
    rx = rows_diff(vel_x[:, inner])
    ry = rows_diff(vel_y[:, inner])
    e_d = rx + cy
    e_t = rx - cy
    e_s = cx + ry
    inv = lax.rsqrt(0.25 * (e_d * e_d) + 0.0625 * (e_t * e_t + e_s * e_s) + 0.01)
    third = stat[0, :, pl.ds(start, width)]
    scaled = third * inv
    work[2, :, mid] = work[2, :, mid] * (2.0 / 3.0) + (0.5 * scaled * e_d - third)
    work[3, :, mid] = work[3, :, mid] * (2.0 / 3.0) + 0.125 * scaled * e_t
    work[4, :, mid] = work[4, :, mid] * (2.0 / 3.0) + 0.0625 * scaled * e_s


def velocity_stage(work, stat, total, start, width, rows):
    wide = pl.ds(start, width + 2 * PAD)
    mid = pl.ds(start + PAD, width)
    here = pl.ds(start, width)
    inner = slice(PAD, PAD + width)
    shear = work[4, :, wide]
    one, two = work[2, :, wide], work[3, :, wide]
    across_shear = (rolled(shear, -1, 1) - rolled(shear, 1, 1))[:, inner]
    lower = one - two
    across_yy = (rolled(lower, -1, 1) - rolled(lower, 1, 1))[:, inner]
    force_x = rows_diff((one + two)[:, inner]) + 2.0 * across_shear
    force_y = 2.0 * rows_diff(shear[:, inner]) + across_yy
    old_x, old_y = work[0, :, mid], work[1, :, mid]
    keep, push = stat[1, :, here], stat[2, :, here]
    new_x = keep * (old_x + coriolis * old_y) + push * force_x + stat[3, :, here]
    new_y = keep * (old_y - coriolis * old_x) + push * force_y + stat[4, :, here]
    work[0, :, mid] = new_x
    work[1, :, mid] = new_y
    own_x, own_y = new_x[rows : 2 * rows], new_y[rows : 2 * rows]
    total[0, :, here] += own_x
    total[1, :, here] += own_y
    total[2, :, here] += jnp.sqrt(1.0 + own_x * own_x + own_y * own_y)


def ocean_stage(source, target, coef, start, width):
    wide = pl.ds(start, width + 2 * PAD)
    mid = pl.ds(start + PAD, width)
    here = pl.ds(start, width)
    inner = slice(PAD, PAD + width)
    up, down, east, west = (coef[i, :, here] for i in range(4))
    for level, speed in enumerate(level_speed):
        tracer = source[level, :, wide]
        centre = tracer[:, inner]
        right = rolled(tracer, -1, 1)[:, inner] - centre
        left = centre - rolled(tracer, 1, 1)[:, inner]
        above = rolled(centre, -1, 0) - centre
        below = centre - rolled(centre, 1, 0)
        change = up * below + down * above + east * left + west * right
        target[level, :, mid] = centre - speed * change


def turns_kernel(
    initial_in, forcing_in, current_in, cover_in, state, average,
    initial, forcing, current, cover,
    own, own_stat, halo, halo_stat, work, spare, stat, total, mean,
    load, near_send, near_recv, far_send, far_recv,
    stat_near_send, stat_near_recv, stat_far_send, stat_far_recv,
    mean_send, mean_recv, go,
):
    me = lax.axis_index("blk")
    comp = lax.axis_index("comp")
    count = lax.axis_size("blk")
    fields, rows, cols = initial.shape
    width = chunk_width(cols)
    chunks = cols // width
    near = 1 - lax.rem(me, 2)
    far = 1 - near
    partner = me + 2 * near - 1
    relay_to = me + 4 * near - 2
    relay_from = me - 4 * near + 2
    can_send = jnp.logical_and(relay_to >= 0, relay_to < count)
    can_recv = jnp.logical_and(relay_from >= 0, relay_from < count)
    relay_to = lax.rem(relay_to + count, count)
    relay_from = lax.rem(relay_from + count, count)

    barrier = pltpu.get_barrier_semaphore()

    def greet(where):
        pl.semaphore_signal(barrier, inc=1, device_id=where, device_id_type=MESH)

    greet({"blk": partner})
    greet({"comp": 1 - comp})
    pl.when(can_send)(lambda: greet({"blk": relay_to}))
    pl.when(can_recv)(lambda: greet({"blk": relay_from}))
    loads = [
        pltpu.make_async_copy(source, target, load.at[i])
        for i, (source, target) in enumerate(
            (
                (initial_in, initial),
                (current_in, current),
                (forcing_in, forcing),
                (cover_in, cover),
            )
        )
    ]
    for copy in loads:
        copy.start()

    work[...] = jnp.zeros_like(work)
    total[...] = jnp.zeros_like(total)

    def enter():
        pl.semaphore_wait(barrier, 2 + can_send.astype(jnp.int32) + can_recv.astype(jnp.int32))

    def copies(source, target, pieces, near_sems, far_sems):
        first, second = [], []
        wide = cols // PARTS
        for index in range(pieces * PARTS):
            piece, place = index // PARTS, pl.ds(index % PARTS * wide, wide)
            first.append(
                pltpu.make_async_remote_copy(
                    source.at[piece, :, place], target.at[far, piece, :, place],
                    near_sems[0].at[index], near_sems[1].at[index],
                    device_id={"blk": partner}, device_id_type=MESH,
                )
            )
            second.append(
                pltpu.make_async_remote_copy(
                    target.at[near, piece, :, place], target.at[far, piece, :, place],
                    far_sems[0].at[index], far_sems[1].at[index],
                    device_id={"blk": relay_to}, device_id_type=MESH,
                )
            )
        return first, second

    def start(pair):
        for copy in pair[0]:
            copy.start()

    def relay(pair):
        for first, second in zip(*pair):
            first.wait_recv()
            pl.when(can_send)(second.start)

    def arrive(pair):
        @pl.when(can_recv)
        def _():
            for copy in pair[1]:
                copy.wait_recv()

    def sent(pair):
        for copy in pair[0]:
            copy.wait_send()

        @pl.when(can_send)
        def _():
            for copy in pair[1]:
                copy.wait_send()

    def clear_edges(turns):
        @pl.when(jnp.logical_not(can_recv))
        def _():
            halo_stat[far] = jnp.zeros(halo_stat.shape[1:], jnp.float32)
            for turn in range(turns):
                halo[turn, far] = jnp.zeros(halo.shape[2:], jnp.float32)

    inside = slice(PAD, PAD + cols)

    def fill_own(source):
        for field in range(fields):
            work[field, rows : 2 * rows, inside] = source[field]

    def fill_sides(turn):
        for field in range(fields):
            work[field, 0:rows, inside] = halo[turn, 0, field]
            work[field, 2 * rows : 3 * rows, inside] = halo[turn, 1, field]

    def exchange_of(turn, source):
        return copies(
            source, halo.at[turn], fields,
            (near_send.at[turn], near_recv.at[turn]), (far_send.at[turn], far_recv.at[turn]),
        )

    def stats_of(source, pieces):
        return copies(
            source, halo_stat, pieces,
            (stat_near_send, stat_near_recv), (stat_far_send, stat_far_recv),
        )

    mean_copy = pltpu.make_async_remote_copy(
        mean, average, mean_send, mean_recv,
        device_id={"comp": 1 - comp}, device_id_type=MESH,
    )

    @pl.when(comp == 0)
    def _():
        depth = rows // 2
        turns = SUBCYCLES // depth
        clear_edges(turns)
        loads[0].wait()
        enter()
        pairs = [exchange_of(0, initial)]
        start(pairs[0])
        for copy in loads[1:]:
            copy.wait()
        covered = cover[...].astype(jnp.float32)
        push = covered / (inertia * forcing[0] + 1.0)
        own_stat[0] = forcing[1] * covered * (1.0 / 3.0)
        own_stat[1] = push
        own_stat[2] = push * (forcing[2] + current[0])
        own_stat[3] = push * (forcing[3] + current[1])
        stat_pair = stats_of(own_stat, 4)
        start(stat_pair)
        for turn in range(turns):
            source = initial if turn == 0 else own.at[turn - 1]
            if turn > 0:
                pairs.append(exchange_of(turn, source))
                start(pairs[turn])
            relay(pairs[turn])
            if turn == 0:
                relay(stat_pair)
                pl.semaphore_signal(
                    go, inc=1, device_id={"comp": 1 - comp}, device_id_type=MESH
                )
            fill_own(source)
            arrive(pairs[turn])
            if turn == 0:
                arrive(stat_pair)
                for place, block in enumerate((halo_stat.at[0], own_stat, halo_stat.at[1])):
                    span = slice(place * rows, (place + 1) * rows)
                    push = block[1]
                    stat[0, span] = block[0]
                    stat[1, span] = jnp.where(push > 0.0, 1.0 - push, 0.0)
                    stat[2, span] = 0.25 * push
                    stat[3, span] = block[2]
                    stat[4, span] = block[3]
            fill_sides(turn)

            def subcycle(step, carry):
                for chunk in range(chunks):
                    stress_stage(work, stat, chunk * width, width)
                for chunk in range(chunks):
                    velocity_stage(work, stat, total, chunk * width, width, rows)
                return carry

            lax.fori_loop(0, depth, subcycle, 0)
            final = state if turn == turns - 1 else own.at[turn]
            for field in range(fields):
                final[field] = work[field, rows : 2 * rows, inside]
        share = 1.0 / SUBCYCLES
        covered = cover[...].astype(jnp.float32)
        mean[0] = total[0] * share - covered * current[0]
        mean[1] = total[1] * share - covered * current[1]
        mean[2] = forcing[4] * covered * (total[2] * share)
        mean_copy.start()
        average[...] = mean[...]
        sent(stat_pair)
        for pair in pairs:
            sent(pair)
        mean_copy.wait_send()

    @pl.when(comp == 1)
    def _():
        depth = rows
        turns = SUBCYCLES // depth
        clear_edges(turns)
        spare[...] = jnp.zeros_like(spare)
        for copy in loads:
            copy.wait()
        enter()
        pl.semaphore_wait(go, 1)
        pairs = [exchange_of(0, initial)]
        start(pairs[0])
        stat_pair = stats_of(current, 2)
        start(stat_pair)
        for turn in range(turns):
            source = initial if turn == 0 else own.at[turn - 1]
            if turn > 0:
                pairs.append(exchange_of(turn, source))
                start(pairs[turn])
            relay(pairs[turn])
            if turn == 0:
                relay(stat_pair)
            fill_own(source)
            arrive(pairs[turn])
            if turn == 0:
                arrive(stat_pair)
                for place in range(3):
                    span = slice(place * rows, (place + 1) * rows)
                    for axis in range(2):
                        if place == 1:
                            speed = current[axis]
                        else:
                            speed = halo_stat[place // 2, axis]
                        stat[2 * axis, span] = courant * jnp.maximum(speed, 0.0)
                        stat[2 * axis + 1, span] = courant * jnp.minimum(speed, 0.0)
            fill_sides(turn)

            def substeps(step, carry):
                for chunk in range(chunks):
                    ocean_stage(work, spare, stat, chunk * width, width)
                for chunk in range(chunks):
                    ocean_stage(spare, work, stat, chunk * width, width)
                return carry

            lax.fori_loop(0, depth // 2, substeps, 0)
            final = state if turn == turns - 1 else own.at[turn]
            for field in range(fields):
                final[field] = work[field, rows : 2 * rows, inside]
        sent(stat_pair)
        for pair in pairs:
            sent(pair)
        mean_copy.wait_recv()


def run_turns(initial, forcing, current, cover):
    fields, rows, cols = initial.shape
    most = SUBCYCLES // (rows // 2)
    f32 = jnp.float32
    vmem = pl.BlockSpec(memory_space=pltpu.VMEM)
    dma = pltpu.SemaphoreType.DMA
    return pl.pallas_call(
        turns_kernel,
        out_shape=(
            jax.ShapeDtypeStruct((fields, rows, cols), f32),
            jax.ShapeDtypeStruct((3, rows, cols), f32),
        ),
        in_specs=[pl.BlockSpec(memory_space=pl.ANY)] * 4,
        out_specs=(vmem, vmem),
        scratch_shapes=[
            pltpu.VMEM(initial.shape, f32),
            pltpu.VMEM(forcing.shape, f32),
            pltpu.VMEM(current.shape, f32),
            pltpu.VMEM(cover.shape, cover.dtype),
            pltpu.VMEM((most, fields, rows, cols), f32),
            pltpu.VMEM((4, rows, cols), f32),
            pltpu.VMEM((most, 2, fields, rows, cols), f32),
            pltpu.VMEM((2, 4, rows, cols), f32),
            pltpu.VMEM((fields, 3 * rows, cols + 2 * PAD), f32),
            pltpu.VMEM((fields, 3 * rows, cols + 2 * PAD), f32),
            pltpu.VMEM((5, 3 * rows, cols), f32),
            pltpu.VMEM((3, rows, cols), f32),
            pltpu.VMEM((3, rows, cols), f32),
            dma((4,)),
            *[dma((most, fields * PARTS)) for _ in range(4)],
            *[dma((4 * PARTS,)) for _ in range(4)],
            dma, dma, pltpu.SemaphoreType.REGULAR,
        ],
        compiler_params=pltpu.CompilerParams(
            collective_id=0, has_side_effects=True
        ),
        name="turns",
    )(initial, forcing, current, cover)


LANES = 128
LEAD = 8
ICE_REACH = 2 * SUBCYCLES
SEA_REACH = SUBCYCLES


def fits_tiles(count, rows, cols):
    return count * rows == LANES and cols == count * LANES and count > 1


def lane_index(shape):
    return lax.broadcasted_iota(jnp.int32, shape, len(shape) - 1)


def lane_diff(value):
    lane = lane_index(value.shape)
    after = jnp.where(lane == LANES - 1, 0.0, pltpu.roll(value, LANES - 1, 1))
    before = jnp.where(lane == 0, 0.0, pltpu.roll(value, 1, 1))
    return after - before


def tile_stress(work, stat, low, size):
    here, up, down = (pl.ds(low + shift, size) for shift in (0, 1, -1))
    vel_x, vel_y = work[0, here], work[1, here]
    cx = work[0, up] - work[0, down]
    cy = work[1, up] - work[1, down]
    rx, ry = lane_diff(vel_x), lane_diff(vel_y)
    e_d = rx + cy
    e_t = rx - cy
    e_s = cx + ry
    inv = lax.rsqrt(0.25 * (e_d * e_d) + 0.0625 * (e_t * e_t + e_s * e_s) + 0.01)
    third = stat[0, here]
    scaled = third * inv
    one = 0.5 * scaled * e_d - third
    two = 0.125 * scaled * e_t
    work[2, here] = work[2, here] * (2.0 / 3.0) + (one + two)
    work[3, here] = work[3, here] * (2.0 / 3.0) + (one - two)
    work[4, here] = work[4, here] * (2.0 / 3.0) + 0.0625 * scaled * e_s


def tile_velocity(work, stat, total, low, size, own):
    here, up, down = (pl.ds(low + shift, size) for shift in (0, 1, -1))
    force_x = lane_diff(work[2, here]) + 2.0 * (work[4, up] - work[4, down])
    force_y = 2.0 * lane_diff(work[4, here]) + (work[3, up] - work[3, down])
    old_x, old_y = work[0, here], work[1, here]
    keep, push = stat[1, here], stat[2, here]
    new_x = keep * (old_x + coriolis * old_y) + push * force_x + stat[3, here]
    new_y = keep * (old_y - coriolis * old_x) + push * force_y + stat[4, here]
    work[0, here] = new_x
    work[1, here] = new_y
    if own is not None:
        place = pl.ds(own, size)
        total[0, place] += new_x
        total[1, place] += new_y
        square = 1.0 + new_x * new_x + new_y * new_y
        total[2, place] += square * lax.rsqrt(square)


def tile_ocean(source, target, stat, low, size):
    here, up, down = (pl.ds(low + shift, size) for shift in (0, 1, -1))
    before, after, left, right, drain = (stat[i, here] for i in range(5))
    for level, speed in enumerate(level_speed):
        centre = source[level, here]
        inflow = before * pltpu.roll(centre, 1, 1) + after * pltpu.roll(centre, LANES - 1, 1)
        inflow += left * source[level, down] + right * source[level, up]
        target[level, here] = centre + speed * (inflow - drain * centre)


def pieces(low, high, step):
    return [(start, min(step, high - start)) for start in range(low, high, step)]


def tiles_kernel(
    initial_in, forcing_in, current_in, cover_in, targets_in, weights_in, state, pair,
    pack, forcing, current, cover, targets, weights,
    recv, work, spare, stat, total, back, home, mean, acc, window, beside, before,
    low, high, hot, parts,
    load, first_send, first_recv, second_send, second_recv,
    total_send, total_recv, state_send, state_recv, mean_send, mean_recv,
    side_send, side_recv, next_send, next_recv, go,
):
    me = lax.axis_index("blk")
    comp = lax.axis_index("comp")
    count = lax.axis_size("blk")
    fields, rows, cols = initial_in.shape
    barrier = pltpu.get_barrier_semaphore()

    def greet(where):
        pl.semaphore_signal(barrier, inc=1, device_id=where, device_id_type=MESH)

    def other(step):
        return lax.bitwise_xor(me, step)

    steps = range(1, count)
    for step in steps:
        greet({"blk": other(step)})
    greet({"comp": 1 - comp})

    loads = [
        pltpu.make_async_copy(source, target, load.at[i])
        for i, (source, target) in enumerate(
            (
                (initial_in, pack.at[0:fields]),
                (current_in, current),
                (forcing_in, forcing),
                (cover_in, cover),
                (targets_in.at[comp], targets),
                (weights_in.at[comp], weights),
            )
        )
    ]
    for copy in loads:
        copy.start()

    def lanes_of(block):
        return pl.ds(pl.multiple_of(block * LANES, LANES), LANES)

    def rows_of(block):
        return pl.ds(pl.multiple_of(block * rows, rows), rows)

    def outward(low, high, sems):
        return [
            pltpu.make_async_remote_copy(
                pack.at[low:high, :, lanes_of(other(step))],
                recv.at[low:high, rows_of(me), :],
                sems[0].at[step], sems[1].at[step],
                device_id={"blk": other(step)}, device_id_type=MESH,
            )
            for step in steps
        ]

    def home_copy(source, target, sems, step):
        return pltpu.make_async_remote_copy(
            source.at[:, rows_of(other(step)), :],
            target.at[:, :, lanes_of(me)],
            sems[0].at[step], sems[1].at[step],
            device_id={"blk": other(step)}, device_id_type=MESH,
        )

    def homeward(source, target, sems):
        return [home_copy(source, target, sems, step) for step in steps]

    width = hot.shape[1]
    members = width // LANES
    chunks = cols // width

    def chunk_of(turn):
        return lax.bitwise_xor(lax.div(me, members), turn)

    def span_of(turn):
        return pl.ds(pl.multiple_of(chunk_of(turn) * width, width), width)

    def start(copies):
        for copy in copies:
            copy.start()

    def arrive(copies):
        for copy in copies:
            copy.wait_recv()

    def sent(copies):
        for copy in copies:
            copy.wait_send()

    def spread_edges(base, filled, reach):
        group = LANES // (2 * reach)
        lane = lane_index((rows, LANES))
        slot = lane // (2 * reach)
        leading = lane % (2 * reach) < reach
        zero = jnp.zeros((rows, LANES), jnp.float32)
        for tile in range(-(-filled // group)):
            members = range(tile * group, min(filled, (tile + 1) * group))
            turned = []
            for block in range(count):
                here = slice(block * LANES, (block + 1) * LANES)
                merged = zero
                for place, field in enumerate(members):
                    shift = (2 * place + 1) * reach % LANES
                    value = pack[field, :, here]
                    moved = pltpu.roll(value, shift, 1) if shift else value
                    merged = jnp.where(slot == place, moved, merged)
                turned.append(merged)
            for block in range(count):
                before = turned[block - 1] if block > 0 else zero
                after = turned[block + 1] if block < count - 1 else zero
                here = slice(block * LANES, (block + 1) * LANES)
                pack[base + tile, :, here] = jnp.where(leading, before, after)

    def unpack(field, base, reach):
        group = LANES // (2 * reach)
        value = recv[field].T
        edge = recv[base + field // group].T
        low = field % group * 2 * reach
        return jnp.concatenate(
            [edge[low : low + reach], value, edge[low + reach : low + 2 * reach]], axis=0
        )

    channels = pair.shape[0]

    def mean_copy(turn):
        return pltpu.make_async_remote_copy(
            mean.at[:, :, span_of(turn)], home.at[:, :, span_of(turn)],
            mean_send.at[turn], mean_recv.at[turn],
            device_id={"comp": 1 - comp}, device_id_type=MESH,
        )
    sides = [
        [
            pltpu.make_async_remote_copy(
                window.at[half, channel], beside.at[half, channel],
                side_send.at[half, channel], side_recv.at[half, channel],
                device_id={"comp": 1 - comp}, device_id_type=MESH,
            )
            for channel in range(channels)
        ]
        for half in range(2)
    ]
    onward = [
        pltpu.make_async_remote_copy(
            window.at[1, channel], before.at[channel],
            next_send.at[channel], next_recv.at[channel],
            device_id={"blk": lax.rem(me + 1, count)}, device_id_type=MESH,
        )
        for channel in range(channels)
    ]

    def prepare_remap():
        target = targets[...]
        block = lax.rem(lax.div(target, width), chunks)
        line = lax.div(target, cols)
        low[...] = lax.rem(target, width).astype(jnp.float32)
        for half in range(2):
            inside = lax.div(line, rows) == half
            place = block * rows + line - half * rows
            high[half] = jnp.where(inside, place, chunks * rows).astype(jnp.float32)
        acc[...] = jnp.zeros_like(acc)

        def one_row(row, carry):
            lane = lane_index((LANES, LANES)).astype(jnp.float32)
            line = low[pl.ds(row, 1), :]
            for start in range(0, cols, LANES):
                value = jnp.broadcast_to(line[:, start : start + LANES], (LANES, LANES)).T
                base = start // width * rows * width + start % width
                place = pl.ds(pl.multiple_of(base + row * width, LANES), LANES)
                for first in range(0, width, LANES):
                    hit = jnp.where(value == lane + float(first), 1.0, 0.0)
                    hot[place, first : first + LANES] = hit.astype(hot.dtype)
            return carry

        lax.fori_loop(0, rows, one_row, 0)

    def split_values(values, turn):
        span = span_of(turn)
        scale = weights[:, span].astype(jnp.float32) * (1.0 / weight_norm)
        for channel in range(channels):
            value = values[channel, :, span] * scale
            coarse = value.astype(jnp.bfloat16).astype(jnp.float32)
            parts[2 * channel, :, span] = coarse
            parts[2 * channel + 1, :, span] = value - coarse

    def remap(half, turn):
        bf16 = jnp.bfloat16
        tall = 16
        span = span_of(turn)
        index = lax.broadcasted_iota(jnp.int32, (tall, width), 0).astype(bf16)

        def lines(block):
            return [
                jnp.broadcast_to(block[row : row + 1], (tall, width)).astype(bf16)
                for row in range(rows)
            ]

        levels = lines(high[half, :, span])
        matches = [
            [level == index + bf16(first) for level in levels]
            for first in range(0, chunks * rows, tall)
        ]
        spread = []
        for part in range(2 * channels):
            values = lines(parts[part, :, span])
            for match in matches:
                kept = [jnp.where(m, v, bf16(0)) for m, v in zip(match, values)]
                spread.append(jnp.concatenate(kept, axis=1))
        depth = rows * width
        place = pl.ds(pl.multiple_of(chunk_of(turn) * depth, depth), depth)
        acc[half] += jnp.dot(
            jnp.concatenate(spread, axis=0), hot[place, :], preferred_element_type=jnp.float32
        )

    def gather_window(half):
        tall = chunks * rows
        for channel in range(channels):
            for block in range(chunks):
                base = 2 * channel * tall + block * rows
                window[half, channel, :, block * width : (block + 1) * width] = (
                    acc[half, base : base + rows] + acc[half, base + tall : base + tall + rows]
                )

    def lower_half():
        def one_chunk(turn, carry):
            remap(0, turn)
            return carry

        lax.fori_loop(0, chunks, one_chunk, 0, unroll=4)
        gather_window(0)

    @pl.when(comp == 0)
    def _():
        filled = fields + 4
        packed = filled + -(-filled // (LANES // (2 * ICE_REACH)))
        span = LANES + 2 * ICE_REACH
        loads[0].wait()
        pl.semaphore_wait(barrier, count)
        first = outward(0, fields, (first_send, first_recv))
        start(first)
        for copy in loads[1:4]:
            copy.wait()
        covered = cover[...].astype(jnp.float32)
        push = covered / (inertia * forcing[0] + 1.0)
        pack[fields] = forcing[1] * covered * (1.0 / 3.0)
        pack[fields + 1] = push
        pack[fields + 2] = push * (forcing[2] + current[0])
        pack[fields + 3] = push * (forcing[3] + current[1])
        spread_edges(filled, filled, ICE_REACH)
        second = outward(fields, packed, (second_send, second_recv))
        start(second)
        recv[0:packed, rows_of(me), :] = pack[0:packed, :, lanes_of(me)]
        total[...] = jnp.zeros_like(total)
        for array in (work, stat):
            for edge in (0, LEAD + span):
                array[:, edge : edge + LEAD] = jnp.zeros((array.shape[0], LEAD, LANES), jnp.float32)
        for copy in loads[4:]:
            copy.wait()
        prepare_remap()
        sent(first)
        sent(second)
        pl.semaphore_signal(go, inc=1, device_id={"comp": 1 - comp}, device_id_type=MESH)
        arrive(first)
        arrive(second)
        whole = slice(LEAD, LEAD + span)
        for field in range(2):
            work[field, whole] = unpack(field, filled, ICE_REACH)
        one, two = unpack(2, filled, ICE_REACH), unpack(3, filled, ICE_REACH)
        work[2, whole] = one + two
        work[3, whole] = one - two
        work[4, whole] = unpack(4, filled, ICE_REACH)
        stat[0, whole] = unpack(fields, filled, ICE_REACH)
        push = unpack(fields + 1, filled, ICE_REACH)
        stat[1, whole] = jnp.where(push > 0.0, 1.0 - push, 0.0)
        stat[2, whole] = 0.25 * push
        stat[3, whole] = unpack(fields + 2, filled, ICE_REACH)
        stat[4, whole] = unpack(fields + 3, filled, ICE_REACH)

        for group in range(SUBCYCLES // 4):
            low, high = LEAD + 8 * group, LEAD + span - 8 * group
            inner, outer = LEAD + ICE_REACH, LEAD + ICE_REACH + LANES

            def subcycle(step, carry, low=low, high=high):
                for begin, size in pieces(low, high, 16):
                    tile_stress(work, stat, begin, size)
                for begin, size in pieces(low, inner, 16) + pieces(outer, high, 16):
                    tile_velocity(work, stat, total, begin, size, None)
                for begin, size in pieces(inner, outer, 16):
                    tile_velocity(work, stat, total, begin, size, begin - inner)
                return carry

            lax.fori_loop(0, 4, subcycle, 0)

        own = slice(LEAD + ICE_REACH, LEAD + ICE_REACH + LANES)
        for channel in range(3):
            back[channel] = total[channel].T
        totals = homeward(back.at[0:3], home, (total_send, total_recv))
        start(totals)
        one, two = work[2, own], work[3, own]
        for field, value in enumerate(
            (work[0, own], work[1, own], 0.5 * (one + two), 0.5 * (one - two), work[4, own])
        ):
            back[3 + field] = value.T
        states = homeward(back.at[3 : 3 + fields], state, (state_send, state_recv))
        start(states)
        home[:, :, lanes_of(me)] = back[0:3, rows_of(me), :]
        state[:, :, lanes_of(me)] = back[3 : 3 + fields, rows_of(me), :]
        share = 1.0 / SUBCYCLES
        def upper_chunk(turn, carry):
            for place in range(members):
                step = turn * members + place

                @pl.when(step > 0)
                def _():
                    home_copy(back.at[0:3], home, (total_send, total_recv), step).wait_recv()

            span = span_of(turn)
            covered = cover[:, span].astype(jnp.float32)
            for axis in range(2):
                mean[axis, :, span] = home[axis, :, span] * share - covered * current[axis, :, span]
            mean[2, :, span] = forcing[4, :, span] * covered * (home[2, :, span] * share)
            mean_copy(turn).start()
            split_values(mean, turn)
            remap(1, turn)
            return carry

        lax.fori_loop(0, chunks, upper_chunk, 0)
        gather_window(1)
        start(sides[1])
        pair[...] = mean[...]
        lower_half()
        start(sides[0])
        sent(totals)
        arrive(states)
        sent(states)
        for turn in range(chunks):
            mean_copy(turn).wait_send()
        sent(sides[0] + sides[1])

    @pl.when(comp == 1)
    def _():
        filled = fields + 2
        packed = filled + -(-filled // (LANES // (2 * SEA_REACH)))
        span = LANES + 2 * SEA_REACH
        for copy in loads:
            copy.wait()
        for axis in range(2):
            pack[fields + axis] = current[axis]
        spread_edges(filled, filled, SEA_REACH)
        for array in (work, spare):
            for edge in (0, LEAD + span):
                array[:, edge : edge + LEAD] = jnp.zeros((array.shape[0], LEAD, LANES), jnp.float32)
        recv[0:packed, rows_of(me), :] = pack[0:packed, :, lanes_of(me)]
        prepare_remap()
        pl.semaphore_wait(barrier, count)
        pl.semaphore_wait(go, 1)
        first = outward(0, packed, (first_send, first_recv))
        start(first)
        arrive(first)
        whole = slice(LEAD, LEAD + span)
        for field in range(fields):
            work[field, whole] = unpack(field, filled, SEA_REACH)
        lane = lane_index((span, LANES))
        speed = courant * unpack(fields, filled, SEA_REACH)
        drain = jnp.abs(speed)
        stat[0, whole] = jnp.where(lane == 0, 0.0, jnp.maximum(speed, 0.0))
        stat[1, whole] = jnp.where(lane == LANES - 1, 0.0, -jnp.minimum(speed, 0.0))
        speed = courant * unpack(fields + 1, filled, SEA_REACH)
        stat[2, whole] = jnp.maximum(speed, 0.0)
        stat[3, whole] = -jnp.minimum(speed, 0.0)
        stat[4, whole] = drain + jnp.abs(speed)
        for group in range(SUBCYCLES // 8):
            low, high = LEAD + 8 * group, LEAD + span - 8 * group

            def substeps(step, carry, low=low, high=high):
                for begin, size in pieces(low, high, 16):
                    tile_ocean(work, spare, stat, begin, size)
                for begin, size in pieces(low, high, 16):
                    tile_ocean(spare, work, stat, begin, size)
                return carry

            lax.fori_loop(0, 4, substeps, 0)
        own = slice(LEAD + SEA_REACH, LEAD + SEA_REACH + LANES)
        for field in range(fields):
            back[3 + field] = work[field, own].T
        states = homeward(back.at[3 : 3 + fields], state, (state_send, state_recv))
        start(states)
        state[:, :, lanes_of(me)] = back[3 : 3 + fields, rows_of(me), :]
        sent(first)
        def upper_chunk(turn, carry):
            mean_copy(turn).wait_recv()
            split_values(home, turn)
            remap(1, turn)
            return carry

        lax.fori_loop(0, chunks, upper_chunk, 0)
        gather_window(1)
        for channel in range(channels):
            sides[1][channel].wait_recv()
            window[1, channel] += beside[1, channel]
            onward[channel].start()
        lower_half()
        for channel in range(channels):
            sides[0][channel].wait_recv()
            pair[channel] = window[0, channel] + beside[0, channel]
        arrive(states)
        arrive(onward)
        pair[...] += before[...]
        state[0] -= dilution * pair[2]
        sent(states)
        sent(onward)


def run_tiles(initial, forcing, current, cover, targets, weights, count):
    fields, rows, cols = initial.shape
    f32 = jnp.float32
    most = fields + 4
    packed = most + -(-most // (LANES // (2 * ICE_REACH)))
    tall = LANES + 2 * ICE_REACH + 2 * LEAD
    low_count = 256 if cols % 256 == 0 else 128
    high_count = rows * cols // low_count
    vmem = pl.BlockSpec(memory_space=pltpu.VMEM)
    dma = pltpu.SemaphoreType.DMA
    return pl.pallas_call(
        tiles_kernel,
        out_shape=(pltpu.VMEM((fields, rows, cols), f32), pltpu.VMEM((3, rows, cols), f32)),
        in_specs=[pl.BlockSpec(memory_space=pl.ANY)] * 6,
        out_specs=(vmem, vmem),
        scratch_shapes=[
            pltpu.VMEM((packed, rows, cols), f32),
            pltpu.VMEM(forcing.shape, f32),
            pltpu.VMEM(current.shape, f32),
            pltpu.VMEM(cover.shape, cover.dtype),
            pltpu.VMEM(targets.shape[1:], targets.dtype),
            pltpu.VMEM(weights.shape[1:], weights.dtype),
            pltpu.VMEM((packed, LANES, LANES), f32),
            pltpu.VMEM((fields, tall, LANES), f32),
            pltpu.VMEM((fields, tall, LANES), f32),
            pltpu.VMEM((5, tall, LANES), f32),
            pltpu.VMEM((3, LANES, LANES), f32),
            pltpu.VMEM((3 + fields, LANES, LANES), f32),
            pltpu.VMEM((3, rows, cols), f32),
            pltpu.VMEM((3, rows, cols), f32),
            pltpu.VMEM((2, 6 * high_count, low_count), f32),
            pltpu.VMEM((2, 3, rows, cols), f32),
            pltpu.VMEM((2, 3, rows, cols), f32),
            pltpu.VMEM((3, rows, cols), f32),
            pltpu.VMEM((rows, cols), f32),
            pltpu.VMEM((2, rows, cols), f32),
            pltpu.VMEM((rows * cols, low_count), jnp.bfloat16),
            pltpu.VMEM((6, rows, cols), f32),
            dma((6,)),
            *[dma((count,)) for _ in range(8)],
            dma((cols // low_count,)), dma((cols // low_count,)), dma((2, 3)), dma((2, 3)), dma((3,)), dma((3,)),
            pltpu.SemaphoreType.REGULAR,
        ],
        compiler_params=pltpu.CompilerParams(collective_id=0, has_side_effects=True),
        name="tiles",
    )(initial, forcing, current, cover, targets, weights)


def remap_kernel(average, targets, weights, window, acc, low_index, high_index):
    comp = lax.axis_index("comp")
    channels, rows, cols = average.shape
    span = low_index.shape[1]
    low_count, high_count = low_index.shape[0], high_index.shape[0]
    bf16 = jnp.bfloat16
    blocks = cols // low_count
    low_index[...] = lax.broadcasted_iota(jnp.int32, low_index.shape, 0).astype(bf16)
    high_index[...] = lax.broadcasted_iota(jnp.int32, high_index.shape, 0).astype(bf16)
    acc[...] = jnp.zeros_like(acc)

    def one_row(row, carry):
        for piece in range(cols // span):
            place = pl.ds(piece * span, span)
            target = targets[comp, pl.ds(row, 1), place]
            scale = weights[comp, pl.ds(row, 1), place].astype(jnp.float32) * (1.0 / weight_norm)
            low = lax.rem(target, low_count)
            block = lax.rem(lax.div(target, low_count), blocks)
            line = lax.div(target, cols)
            high = (lax.div(line, rows) * blocks + block) * rows + lax.rem(line, rows)
            low_hot = jnp.where(low_index[...] == low.astype(bf16), bf16(1), bf16(0))
            match = high_index[...] == high.astype(bf16)
            parts = []
            for channel in range(channels):
                value = average[channel, pl.ds(row, 1), place] * scale
                coarse = value.astype(bf16)
                fine = (value - coarse.astype(jnp.float32)).astype(bf16)
                parts.append(jnp.where(match, coarse, bf16(0)))
                parts.append(jnp.where(match, fine, bf16(0)))
            spread = jnp.concatenate(parts, axis=0)
            acc[...] += lax.dot_general(
                spread, low_hot, (((1,), (1,)), ((), ())), preferred_element_type=jnp.float32
            )
        return carry

    lax.fori_loop(0, rows, one_row, 0)
    for channel in range(channels):
        for half in range(2):
            for block in range(blocks):
                base = 2 * channel * high_count + (half * blocks + block) * rows
                window[channel, half, :, block * low_count : (block + 1) * low_count] = (
                    acc[base : base + rows] + acc[base + high_count : base + high_count + rows]
                )


def run_remap(average, targets, weights):
    channels, rows, cols = average.shape
    low_count = 256 if cols % 256 == 0 else 128
    high_count = 2 * rows * cols // low_count
    span = min(1024, cols)
    vmem = pl.BlockSpec(memory_space=pltpu.VMEM)
    return pl.pallas_call(
        remap_kernel,
        out_shape=jax.ShapeDtypeStruct((channels, 2, rows, cols), jnp.float32),
        in_specs=[vmem] * 3,
        out_specs=vmem,
        scratch_shapes=[
            pltpu.VMEM((2 * channels * high_count, low_count), jnp.float32),
            pltpu.VMEM((low_count, span), jnp.bfloat16),
            pltpu.VMEM((high_count, span), jnp.bfloat16),
        ],
        compiler_params=pltpu.CompilerParams(vmem_limit_bytes=40 * 1024 * 1024),
        name="remap",
    )(average, targets, weights)


def join_kernel(
    window, state, average, out_state, out_pair, beside, carry, before,
    side_send, side_recv, next_send, next_recv,
):
    me = lax.axis_index("blk")
    comp = lax.axis_index("comp")
    count = lax.axis_size("blk")
    right, left = lax.rem(me + 1, count), lax.rem(me + count - 1, count)
    barrier = pltpu.get_barrier_semaphore()
    pl.semaphore_signal(barrier, inc=1, device_id={"blk": right}, device_id_type=MESH)
    pl.semaphore_signal(barrier, inc=1, device_id={"blk": left}, device_id_type=MESH)
    pl.semaphore_signal(barrier, inc=1, device_id={"comp": 1 - comp}, device_id_type=MESH)
    pl.semaphore_wait(barrier, 3)
    channels = window.shape[0]
    sides, onward = [], []
    for half in (1, 0):
        for channel in range(channels):
            sides.append(
                pltpu.make_async_remote_copy(
                    window.at[channel, half], beside.at[channel, half],
                    side_send.at[half, channel], side_recv.at[half, channel],
                    device_id={"comp": 1 - comp}, device_id_type=MESH,
                )
            )
    for channel in range(channels):
        onward.append(
            pltpu.make_async_remote_copy(
                carry.at[channel], before.at[channel],
                next_send.at[channel], next_recv.at[channel],
                device_id={"blk": right}, device_id_type=MESH,
            )
        )

    @pl.when(comp == 0)
    def _():
        for copy in sides:
            copy.start()
        out_state[...] = state[...]
        out_pair[...] = average[...]
        for copy in sides:
            copy.wait_send()

    @pl.when(comp == 1)
    def _():
        for channel in range(channels):
            sides[channel].wait_recv()
            carry[channel] = window[channel, 1] + beside[channel, 1]
            onward[channel].start()
        for channel in range(channels):
            sides[channels + channel].wait_recv()
            out_pair[channel] = window[channel, 0] + beside[channel, 0]
        out_state[...] = state[...]
        for channel in range(channels):
            onward[channel].wait_recv()
            out_pair[channel] += before[channel]
        out_state[0] -= dilution * out_pair[2]
        for channel in range(channels):
            onward[channel].wait_send()


def run_join(window, state, average):
    channels, rows, cols = average.shape
    vmem = pl.BlockSpec(memory_space=pltpu.VMEM)
    dma = pltpu.SemaphoreType.DMA
    return pl.pallas_call(
        join_kernel,
        out_shape=(
            jax.ShapeDtypeStruct(state.shape, jnp.float32),
            jax.ShapeDtypeStruct(average.shape, jnp.float32),
        ),
        in_specs=[vmem] * 3,
        out_specs=(vmem, vmem),
        scratch_shapes=[
            pltpu.VMEM(window.shape, jnp.float32),
            pltpu.VMEM(average.shape, jnp.float32),
            pltpu.VMEM(average.shape, jnp.float32),
            dma((2, channels)), dma((2, channels)), dma((channels,)), dma((channels,)),
        ],
        compiler_params=pltpu.CompilerParams(
            collective_id=1, has_side_effects=True, vmem_limit_bytes=40 * 1024 * 1024
        ),
        name="join",
    )(window, state, average)


def body(count, initial, ice_forcing, ocean_current, ice_cover, targets, weights):
    if fits_tiles(count, *initial.shape[2:]):
        state, coupled = run_tiles(
            initial[0], ice_forcing, ocean_current, ice_cover, targets, weights, count
        )
    else:
        state, average = run_turns(initial[0], ice_forcing, ocean_current, ice_cover)
        window = run_remap(average, targets, weights)
        state, coupled = run_join(window, state, average)
    return (state[None], coupled[None])


def solution(mesh):
    placed = (
        P("comp", None, "blk", None),
        P(None, "blk", None),
        P(None, "blk", None),
        P("blk", None),
        P(None, "blk", None),
        P(None, "blk", None),
    )
    return jax.shard_map(
        functools.partial(body, mesh.shape["blk"]),
        mesh=mesh,
        in_specs=placed,
        out_specs=(P("comp", None, "blk", None), P("comp", None, "blk", None)),
        check_vma=False,
    )
```

```python
import functools

import jax
import jax.numpy as jnp
from jax import lax
from jax.experimental import pallas as pl
from jax.experimental.pallas import tpu as pltpu
from jax.sharding import PartitionSpec as P

SUBCYCLES = 16
MESH = pl.DeviceIdType.MESH
PAD = 128
PARTS = 2

coriolis = 0.1
inertia = 4.0
courant = 0.2
dilution = 0.5
weight_norm = 4.0
level_speed = (1.0, 0.8, 0.6, 0.45, 0.3)


def rolled(value, steps, axis):
    return pltpu.roll(value, steps % value.shape[axis], axis)


def rows_diff(value):
    return rolled(value, -1, 0) - rolled(value, 1, 0)


def chunk_width(cols):
    return 256 if cols % 256 == 0 else 128


def stress_stage(work, stat, start, width):
    wide = pl.ds(start, width + 2 * PAD)
    mid = pl.ds(start + PAD, width)
    inner = slice(PAD, PAD + width)
    vel_x, vel_y = work[0, :, wide], work[1, :, wide]
    cx = (rolled(vel_x, -1, 1) - rolled(vel_x, 1, 1))[:, inner]
    cy = (rolled(vel_y, -1, 1) - rolled(vel_y, 1, 1))[:, inner]
    rx = rows_diff(vel_x[:, inner])
    ry = rows_diff(vel_y[:, inner])
    e_d = rx + cy
    e_t = rx - cy
    e_s = cx + ry
    inv = lax.rsqrt(0.25 * (e_d * e_d) + 0.0625 * (e_t * e_t + e_s * e_s) + 0.01)
    third = stat[0, :, pl.ds(start, width)]
    scaled = third * inv
    work[2, :, mid] = work[2, :, mid] * (2.0 / 3.0) + (0.5 * scaled * e_d - third)
    work[3, :, mid] = work[3, :, mid] * (2.0 / 3.0) + 0.125 * scaled * e_t
    work[4, :, mid] = work[4, :, mid] * (2.0 / 3.0) + 0.0625 * scaled * e_s


def velocity_stage(work, stat, total, start, width, rows):
    wide = pl.ds(start, width + 2 * PAD)
    mid = pl.ds(start + PAD, width)
    here = pl.ds(start, width)
    inner = slice(PAD, PAD + width)
    shear = work[4, :, wide]
    one, two = work[2, :, wide], work[3, :, wide]
    across_shear = (rolled(shear, -1, 1) - rolled(shear, 1, 1))[:, inner]
    lower = one - two
    across_yy = (rolled(lower, -1, 1) - rolled(lower, 1, 1))[:, inner]
    force_x = rows_diff((one + two)[:, inner]) + 2.0 * across_shear
    force_y = 2.0 * rows_diff(shear[:, inner]) + across_yy
    old_x, old_y = work[0, :, mid], work[1, :, mid]
    keep, push = stat[1, :, here], stat[2, :, here]
    new_x = keep * (old_x + coriolis * old_y) + push * force_x + stat[3, :, here]
    new_y = keep * (old_y - coriolis * old_x) + push * force_y + stat[4, :, here]
    work[0, :, mid] = new_x
    work[1, :, mid] = new_y
    own_x, own_y = new_x[rows : 2 * rows], new_y[rows : 2 * rows]
    total[0, :, here] += own_x
    total[1, :, here] += own_y
    total[2, :, here] += jnp.sqrt(1.0 + own_x * own_x + own_y * own_y)


def ocean_stage(source, target, coef, start, width):
    wide = pl.ds(start, width + 2 * PAD)
    mid = pl.ds(start + PAD, width)
    here = pl.ds(start, width)
    inner = slice(PAD, PAD + width)
    up, down, east, west = (coef[i, :, here] for i in range(4))
    for level, speed in enumerate(level_speed):
        tracer = source[level, :, wide]
        centre = tracer[:, inner]
        right = rolled(tracer, -1, 1)[:, inner] - centre
        left = centre - rolled(tracer, 1, 1)[:, inner]
        above = rolled(centre, -1, 0) - centre
        below = centre - rolled(centre, 1, 0)
        change = up * below + down * above + east * left + west * right
        target[level, :, mid] = centre - speed * change


def turns_kernel(
    initial_in, forcing_in, current_in, cover_in, state, average,
    initial, forcing, current, cover,
    own, own_stat, halo, halo_stat, work, spare, stat, total, mean,
    load, near_send, near_recv, far_send, far_recv,
    stat_near_send, stat_near_recv, stat_far_send, stat_far_recv,
    mean_send, mean_recv, go,
):
    me = lax.axis_index("blk")
    comp = lax.axis_index("comp")
    count = lax.axis_size("blk")
    fields, rows, cols = initial.shape
    width = chunk_width(cols)
    chunks = cols // width
    near = 1 - lax.rem(me, 2)
    far = 1 - near
    partner = me + 2 * near - 1
    relay_to = me + 4 * near - 2
    relay_from = me - 4 * near + 2
    can_send = jnp.logical_and(relay_to >= 0, relay_to < count)
    can_recv = jnp.logical_and(relay_from >= 0, relay_from < count)
    relay_to = lax.rem(relay_to + count, count)
    relay_from = lax.rem(relay_from + count, count)

    barrier = pltpu.get_barrier_semaphore()

    def greet(where):
        pl.semaphore_signal(barrier, inc=1, device_id=where, device_id_type=MESH)

    greet({"blk": partner})
    greet({"comp": 1 - comp})
    pl.when(can_send)(lambda: greet({"blk": relay_to}))
    pl.when(can_recv)(lambda: greet({"blk": relay_from}))
    loads = [
        pltpu.make_async_copy(source, target, load.at[i])
        for i, (source, target) in enumerate(
            (
                (initial_in, initial),
                (current_in, current),
                (forcing_in, forcing),
                (cover_in, cover),
            )
        )
    ]
    for copy in loads:
        copy.start()

    work[...] = jnp.zeros_like(work)
    total[...] = jnp.zeros_like(total)

    def enter():
        pl.semaphore_wait(barrier, 2 + can_send.astype(jnp.int32) + can_recv.astype(jnp.int32))

    def copies(source, target, pieces, near_sems, far_sems):
        first, second = [], []
        wide = cols // PARTS
        for index in range(pieces * PARTS):
            piece, place = index // PARTS, pl.ds(index % PARTS * wide, wide)
            first.append(
                pltpu.make_async_remote_copy(
                    source.at[piece, :, place], target.at[far, piece, :, place],
                    near_sems[0].at[index], near_sems[1].at[index],
                    device_id={"blk": partner}, device_id_type=MESH,
                )
            )
            second.append(
                pltpu.make_async_remote_copy(
                    target.at[near, piece, :, place], target.at[far, piece, :, place],
                    far_sems[0].at[index], far_sems[1].at[index],
                    device_id={"blk": relay_to}, device_id_type=MESH,
                )
            )
        return first, second

    def start(pair):
        for copy in pair[0]:
            copy.start()

    def relay(pair):
        for first, second in zip(*pair):
            first.wait_recv()
            pl.when(can_send)(second.start)

    def arrive(pair):
        @pl.when(can_recv)
        def _():
            for copy in pair[1]:
                copy.wait_recv()

    def sent(pair):
        for copy in pair[0]:
            copy.wait_send()

        @pl.when(can_send)
        def _():
            for copy in pair[1]:
                copy.wait_send()

    def clear_edges(turns):
        @pl.when(jnp.logical_not(can_recv))
        def _():
            halo_stat[far] = jnp.zeros(halo_stat.shape[1:], jnp.float32)
            for turn in range(turns):
                halo[turn, far] = jnp.zeros(halo.shape[2:], jnp.float32)

    inside = slice(PAD, PAD + cols)

    def fill_own(source):
        for field in range(fields):
            work[field, rows : 2 * rows, inside] = source[field]

    def fill_sides(turn):
        for field in range(fields):
            work[field, 0:rows, inside] = halo[turn, 0, field]
            work[field, 2 * rows : 3 * rows, inside] = halo[turn, 1, field]

    def exchange_of(turn, source):
        return copies(
            source, halo.at[turn], fields,
            (near_send.at[turn], near_recv.at[turn]), (far_send.at[turn], far_recv.at[turn]),
        )

    def stats_of(source, pieces):
        return copies(
            source, halo_stat, pieces,
            (stat_near_send, stat_near_recv), (stat_far_send, stat_far_recv),
        )

    mean_copy = pltpu.make_async_remote_copy(
        mean, average, mean_send, mean_recv,
        device_id={"comp": 1 - comp}, device_id_type=MESH,
    )

    @pl.when(comp == 0)
    def _():
        depth = rows // 2
        turns = SUBCYCLES // depth
        clear_edges(turns)
        loads[0].wait()
        enter()
        pairs = [exchange_of(0, initial)]
        start(pairs[0])
        for copy in loads[1:]:
            copy.wait()
        covered = cover[...].astype(jnp.float32)
        push = covered / (inertia * forcing[0] + 1.0)
        own_stat[0] = forcing[1] * covered * (1.0 / 3.0)
        own_stat[1] = push
        own_stat[2] = push * (forcing[2] + current[0])
        own_stat[3] = push * (forcing[3] + current[1])
        stat_pair = stats_of(own_stat, 4)
        start(stat_pair)
        for turn in range(turns):
            source = initial if turn == 0 else own.at[turn - 1]
            if turn > 0:
                pairs.append(exchange_of(turn, source))
                start(pairs[turn])
            relay(pairs[turn])
            if turn == 0:
                relay(stat_pair)
                pl.semaphore_signal(
                    go, inc=1, device_id={"comp": 1 - comp}, device_id_type=MESH
                )
            fill_own(source)
            arrive(pairs[turn])
            if turn == 0:
                arrive(stat_pair)
                for place, block in enumerate((halo_stat.at[0], own_stat, halo_stat.at[1])):
                    span = slice(place * rows, (place + 1) * rows)
                    push = block[1]
                    stat[0, span] = block[0]
                    stat[1, span] = jnp.where(push > 0.0, 1.0 - push, 0.0)
                    stat[2, span] = 0.25 * push
                    stat[3, span] = block[2]
                    stat[4, span] = block[3]
            fill_sides(turn)

            def subcycle(step, carry):
                for chunk in range(chunks):
                    stress_stage(work, stat, chunk * width, width)
                for chunk in range(chunks):
                    velocity_stage(work, stat, total, chunk * width, width, rows)
                return carry

            lax.fori_loop(0, depth, subcycle, 0)
            final = state if turn == turns - 1 else own.at[turn]
            for field in range(fields):
                final[field] = work[field, rows : 2 * rows, inside]
        share = 1.0 / SUBCYCLES
        covered = cover[...].astype(jnp.float32)
        mean[0] = total[0] * share - covered * current[0]
        mean[1] = total[1] * share - covered * current[1]
        mean[2] = forcing[4] * covered * (total[2] * share)
        mean_copy.start()
        average[...] = mean[...]
        sent(stat_pair)
        for pair in pairs:
            sent(pair)
        mean_copy.wait_send()

    @pl.when(comp == 1)
    def _():
        depth = rows
        turns = SUBCYCLES // depth
        clear_edges(turns)
        spare[...] = jnp.zeros_like(spare)
        for copy in loads:
            copy.wait()
        enter()
        pl.semaphore_wait(go, 1)
        pairs = [exchange_of(0, initial)]
        start(pairs[0])
        stat_pair = stats_of(current, 2)
        start(stat_pair)
        for turn in range(turns):
            source = initial if turn == 0 else own.at[turn - 1]
            if turn > 0:
                pairs.append(exchange_of(turn, source))
                start(pairs[turn])
            relay(pairs[turn])
            if turn == 0:
                relay(stat_pair)
            fill_own(source)
            arrive(pairs[turn])
            if turn == 0:
                arrive(stat_pair)
                for place in range(3):
                    span = slice(place * rows, (place + 1) * rows)
                    for axis in range(2):
                        if place == 1:
                            speed = current[axis]
                        else:
                            speed = halo_stat[place // 2, axis]
                        stat[2 * axis, span] = courant * jnp.maximum(speed, 0.0)
                        stat[2 * axis + 1, span] = courant * jnp.minimum(speed, 0.0)
            fill_sides(turn)

            def substeps(step, carry):
                for chunk in range(chunks):
                    ocean_stage(work, spare, stat, chunk * width, width)
                for chunk in range(chunks):
                    ocean_stage(spare, work, stat, chunk * width, width)
                return carry

            lax.fori_loop(0, depth // 2, substeps, 0)
            final = state if turn == turns - 1 else own.at[turn]
            for field in range(fields):
                final[field] = work[field, rows : 2 * rows, inside]
        sent(stat_pair)
        for pair in pairs:
            sent(pair)
        mean_copy.wait_recv()


def run_turns(initial, forcing, current, cover):
    fields, rows, cols = initial.shape
    most = SUBCYCLES // (rows // 2)
    f32 = jnp.float32
    vmem = pl.BlockSpec(memory_space=pltpu.VMEM)
    dma = pltpu.SemaphoreType.DMA
    return pl.pallas_call(
        turns_kernel,
        out_shape=(
            jax.ShapeDtypeStruct((fields, rows, cols), f32),
            jax.ShapeDtypeStruct((3, rows, cols), f32),
        ),
        in_specs=[pl.BlockSpec(memory_space=pl.ANY)] * 4,
        out_specs=(vmem, vmem),
        scratch_shapes=[
            pltpu.VMEM(initial.shape, f32),
            pltpu.VMEM(forcing.shape, f32),
            pltpu.VMEM(current.shape, f32),
            pltpu.VMEM(cover.shape, cover.dtype),
            pltpu.VMEM((most, fields, rows, cols), f32),
            pltpu.VMEM((4, rows, cols), f32),
            pltpu.VMEM((most, 2, fields, rows, cols), f32),
            pltpu.VMEM((2, 4, rows, cols), f32),
            pltpu.VMEM((fields, 3 * rows, cols + 2 * PAD), f32),
            pltpu.VMEM((fields, 3 * rows, cols + 2 * PAD), f32),
            pltpu.VMEM((5, 3 * rows, cols), f32),
            pltpu.VMEM((3, rows, cols), f32),
            pltpu.VMEM((3, rows, cols), f32),
            dma((4,)),
            *[dma((most, fields * PARTS)) for _ in range(4)],
            *[dma((4 * PARTS,)) for _ in range(4)],
            dma, dma, pltpu.SemaphoreType.REGULAR,
        ],
        compiler_params=pltpu.CompilerParams(
            collective_id=0, has_side_effects=True
        ),
        name="turns",
    )(initial, forcing, current, cover)


LANES = 128
LEAD = 8
ICE_REACH = 2 * SUBCYCLES
SEA_REACH = SUBCYCLES


def fits_tiles(count, rows, cols):
    return count * rows == LANES and cols == count * LANES and count > 1


def lane_index(shape):
    return lax.broadcasted_iota(jnp.int32, shape, len(shape) - 1)


def lane_diff(value):
    lane = lane_index(value.shape)
    after = jnp.where(lane == LANES - 1, 0.0, pltpu.roll(value, LANES - 1, 1))
    before = jnp.where(lane == 0, 0.0, pltpu.roll(value, 1, 1))
    return after - before


def tile_stress(work, stat, low, size):
    here, up, down = (pl.ds(low + shift, size) for shift in (0, 1, -1))
    cx = work[0, up] - work[0, down]
    cy = work[1, up] - work[1, down]
    rx, ry = lane_diff(work[0, here]), lane_diff(work[1, here])
    e_d = rx + cy
    e_t = rx - cy
    e_s = cx + ry
    fourfold = 4.0 * e_d
    scaled = stat[0, here] * lax.rsqrt(fourfold * e_d + (e_t * e_t + e_s * e_s) + 0.16)
    rest = stat[5, here]
    work[2, here] = work[2, here] * (2.0 / 3.0) + (scaled * (fourfold + e_t) - rest)
    work[3, here] = work[3, here] * (2.0 / 3.0) + (scaled * (fourfold - e_t) - rest)
    work[4, here] = work[4, here] * (2.0 / 3.0) + scaled * e_s


def tile_velocity(work, stat, total, low, size, own):
    here, up, down = (pl.ds(low + shift, size) for shift in (0, 1, -1))
    force_x = lane_diff(work[2, here]) + (work[4, up] - work[4, down])
    force_y = lane_diff(work[4, here]) + (work[3, up] - work[3, down])
    old_x, old_y = work[0, here], work[1, here]
    keep, push = stat[1, here], stat[2, here]
    new_x = keep * (old_x + coriolis * old_y) + push * force_x + stat[3, here]
    new_y = keep * (old_y - coriolis * old_x) + push * force_y + stat[4, here]
    work[0, here] = new_x
    work[1, here] = new_y
    if own is not None:
        place = pl.ds(own, size)
        total[0, place] += new_x
        total[1, place] += new_y
        square = 1.0 + new_x * new_x + new_y * new_y
        total[2, place] += square * lax.rsqrt(square)


def tile_ocean(source, target, stat, low, size):
    here, up, down = (pl.ds(low + shift, size) for shift in (0, 1, -1))
    before, after, left, right, drain = (stat[i, here] for i in range(5))
    for level, speed in enumerate(level_speed):
        centre = source[level, here]
        inflow = before * pltpu.roll(centre, 1, 1) + after * pltpu.roll(centre, LANES - 1, 1)
        inflow += left * source[level, down] + right * source[level, up]
        target[level, here] = centre + speed * (inflow - drain * centre)


def pieces(low, high, step):
    return [(start, min(step, high - start)) for start in range(low, high, step)]


def tiles_kernel(
    initial_in, forcing_in, current_in, cover_in, targets_in, weights_in, state, pair,
    pack, forcing, current, cover, targets, weights,
    recv, work, spare, stat, total, back, home, mean, acc, window, beside, before,
    low, high, hot, parts,
    load, first_send, first_recv, second_send, second_recv,
    total_send, total_recv, state_send, state_recv, mean_send, mean_recv,
    side_send, side_recv, next_send, next_recv, edge_send, edge_recv, go,
):
    me = lax.axis_index("blk")
    comp = lax.axis_index("comp")
    count = lax.axis_size("blk")
    fields, rows, cols = initial_in.shape
    barrier = pltpu.get_barrier_semaphore()

    def greet(where):
        pl.semaphore_signal(barrier, inc=1, device_id=where, device_id_type=MESH)

    def other(step):
        return lax.bitwise_xor(me, step)

    steps = range(1, count)
    for step in steps:
        greet({"blk": other(step)})
    greet({"comp": 1 - comp})

    loads = [
        pltpu.make_async_copy(source, target, load.at[i])
        for i, (source, target) in enumerate(
            (
                (initial_in, pack.at[0:fields]),
                (current_in, current),
                (forcing_in, forcing),
                (cover_in, cover),
                (targets_in.at[comp], targets),
                (weights_in.at[comp], weights),
            )
        )
    ]
    for copy in loads:
        copy.start()

    turn_size = min(4, count)

    def mirrored(group, place):
        return place + lax.rem(group, 2) * (turn_size - 1 - 2 * place)

    def column_of(device):
        group, place = lax.div(device, turn_size), lax.rem(device, turn_size)
        return group * turn_size + mirrored(group, lax.bitwise_xor(place, lax.div(place, 2)))

    def device_of(column):
        group, place = lax.div(column, turn_size), lax.rem(column, turn_size)
        place = mirrored(group, place)
        return group * turn_size + lax.bitwise_xor(place, lax.div(place, 2))

    mine = column_of(me)

    def lanes_of(block):
        return pl.ds(pl.multiple_of(block * LANES, LANES), LANES)

    def rows_of(block):
        return pl.ds(pl.multiple_of(block * rows, rows), rows)

    def outward(low, high, sems):
        return [
            pltpu.make_async_remote_copy(
                pack.at[low:high, :, lanes_of(column_of(other(step)))],
                recv.at[low:high, rows_of(me), :],
                sems[0].at[step], sems[1].at[step],
                device_id={"blk": other(step)}, device_id_type=MESH,
            )
            for step in steps
        ]

    def home_copy(source, target, sems, step):
        return pltpu.make_async_remote_copy(
            source.at[:, rows_of(other(step)), :],
            target.at[:, :, lanes_of(mine)],
            sems[0].at[step], sems[1].at[step],
            device_id={"blk": other(step)}, device_id_type=MESH,
        )

    def homeward(source, target, sems):
        return [home_copy(source, target, sems, step) for step in steps]

    width = hot.shape[1]
    members = width // LANES
    chunks = cols // width

    def chunk_of(turn):
        device = members * lax.bitwise_xor(lax.div(me, members), turn)
        return lax.div(column_of(device), members)

    def span_of(turn):
        return pl.ds(pl.multiple_of(chunk_of(turn) * width, width), width)

    def start(copies):
        for copy in copies:
            copy.start()

    def arrive(copies):
        for copy in copies:
            copy.wait_recv()

    def sent(copies):
        for copy in copies:
            copy.wait_send()

    def spread_edges(base, low, filled, reach):
        group = LANES // (2 * reach)
        lane = lane_index((rows, LANES))
        slot = lane // (2 * reach)
        leading = lane % (2 * reach) < reach
        zero = jnp.zeros((rows, LANES), jnp.float32)
        for tile in range(-(-(filled - low) // group)):
            members = range(low + tile * group, min(filled, low + (tile + 1) * group))
            turned = []
            for block in range(count):
                here = slice(block * LANES, (block + 1) * LANES)
                merged = zero
                for place, field in enumerate(members):
                    shift = (2 * place + 1) * reach % LANES
                    value = pack[field, :, here]
                    moved = pltpu.roll(value, shift, 1) if shift else value
                    merged = jnp.where(slot == place, moved, merged)
                turned.append(merged)
            for block in range(count):
                before = turned[block - 1] if block > 0 else zero
                after = turned[block + 1] if block < count - 1 else zero
                here = slice(block * LANES, (block + 1) * LANES)
                pack[base + tile, :, here] = jnp.where(leading, before, after)

    def unpack(field, base, low, reach):
        group = LANES // (2 * reach)
        value = recv[field].T
        edge = recv[base + (field - low) // group].T
        start = (field - low) % group * 2 * reach
        return jnp.concatenate(
            [edge[start : start + reach], value, edge[start + reach : start + 2 * reach]], axis=0
        )

    channels = pair.shape[0]

    def mean_copy(turn):
        return pltpu.make_async_remote_copy(
            mean.at[:, :, span_of(turn)], home.at[:, :, span_of(turn)],
            mean_send.at[turn], mean_recv.at[turn],
            device_id={"comp": 1 - comp}, device_id_type=MESH,
        )
    sides = [
        [
            pltpu.make_async_remote_copy(
                window.at[half, channel], beside.at[half, channel],
                side_send.at[half, channel], side_recv.at[half, channel],
                device_id={"comp": 1 - comp}, device_id_type=MESH,
            )
            for channel in range(channels)
        ]
        for half in range(2)
    ]
    onward = [
        pltpu.make_async_remote_copy(
            window.at[1, channel], before.at[channel],
            next_send.at[channel], next_recv.at[channel],
            device_id={"blk": lax.rem(me + 1, count)}, device_id_type=MESH,
        )
        for channel in range(channels)
    ]

    def prepare_remap():
        target = targets[...]
        block = lax.rem(lax.div(target, width), chunks)
        line = lax.div(target, cols)
        low[...] = lax.rem(target, width).astype(jnp.float32)
        for half in range(2):
            inside = lax.div(line, rows) == half
            place = block * rows + line - half * rows
            high[half] = jnp.where(inside, place, chunks * rows).astype(jnp.float32)
        acc[...] = jnp.zeros_like(acc)

        def one_row(row, carry):
            lane = lane_index((LANES, LANES)).astype(jnp.float32)
            line = low[pl.ds(row, 1), :]
            for start in range(0, cols, LANES):
                value = jnp.broadcast_to(line[:, start : start + LANES], (LANES, LANES)).T
                base = start // width * rows * width + start % width
                place = pl.ds(pl.multiple_of(base + row * width, LANES), LANES)
                for first in range(0, width, LANES):
                    hit = jnp.where(value == lane + float(first), 1.0, 0.0)
                    hot[place, first : first + LANES] = hit.astype(hot.dtype)
            return carry

        lax.fori_loop(0, rows, one_row, 0)

    def split_values(values, turn):
        span = span_of(turn)
        scale = weights[:, span].astype(jnp.float32) * (1.0 / weight_norm)
        for channel in range(channels):
            value = values[channel, :, span] * scale
            coarse = value.astype(jnp.bfloat16).astype(jnp.float32)
            parts[2 * channel, :, span] = coarse
            parts[2 * channel + 1, :, span] = value - coarse

    def remap(half, turn):
        bf16 = jnp.bfloat16
        tall = 16
        span = span_of(turn)
        index = lax.broadcasted_iota(jnp.int32, (tall, width), 0).astype(bf16)

        def lines(block):
            return [
                jnp.broadcast_to(block[row : row + 1], (tall, width)).astype(bf16)
                for row in range(rows)
            ]

        levels = lines(high[half, :, span])
        matches = [
            [level == index + bf16(first) for level in levels]
            for first in range(0, chunks * rows, tall)
        ]
        spread = []
        for part in range(2 * channels):
            values = lines(parts[part, :, span])
            for match in matches:
                kept = [jnp.where(m, v, bf16(0)) for m, v in zip(match, values)]
                spread.append(jnp.concatenate(kept, axis=1))
        depth = rows * width
        place = pl.ds(pl.multiple_of(chunk_of(turn) * depth, depth), depth)
        acc[half] += jnp.dot(
            jnp.concatenate(spread, axis=0), hot[place, :], preferred_element_type=jnp.float32
        )

    def gather_window(half):
        tall = chunks * rows
        for channel in range(channels):
            for block in range(chunks):
                base = 2 * channel * tall + block * rows
                window[half, channel, :, block * width : (block + 1) * width] = (
                    acc[half, base : base + rows] + acc[half, base + tall : base + tall + rows]
                )

    def lower_half():
        def one_chunk(turn, carry):
            remap(0, turn)
            return carry

        lax.fori_loop(0, chunks, one_chunk, 0, unroll=4)
        gather_window(0)

    @pl.when(comp == 0)
    def _():
        filled = fields + 4
        packed = filled + -(-4 // (LANES // (2 * ICE_REACH)))
        span = LANES + 2 * ICE_REACH
        loads[0].wait()
        pl.semaphore_wait(barrier, count)
        first = outward(0, fields, (first_send, first_recv))
        start(first)
        for copy in loads[1:4]:
            copy.wait()
        covered = cover[...].astype(jnp.float32)
        push = covered / (inertia * forcing[0] + 1.0)
        pack[fields] = forcing[1] * covered * (1.0 / 3.0)
        pack[fields + 1] = push
        pack[fields + 2] = push * (forcing[2] + current[0])
        pack[fields + 3] = push * (forcing[3] + current[1])
        spread_edges(filled, fields, filled, ICE_REACH)
        second = outward(fields, packed, (second_send, second_recv))
        start(second)
        recv[0:packed, rows_of(me), :] = pack[0:packed, :, lanes_of(mine)]
        total[...] = jnp.zeros_like(total)
        for array in (work, stat):
            for edge in (0, LEAD + span):
                array[:, edge : edge + LEAD] = jnp.zeros((array.shape[0], LEAD, LANES), jnp.float32)
        for copy in loads[4:]:
            copy.wait()
        prepare_remap()
        left, middle, right = LEAD, LEAD + ICE_REACH, LEAD + ICE_REACH + LANES
        onto_right = pltpu.make_async_remote_copy(
            work.at[:, right - ICE_REACH : right], work.at[:, left:middle],
            edge_send.at[0], edge_recv.at[0],
            device_id={"blk": device_of(lax.rem(mine + 1, count))}, device_id_type=MESH,
        )
        onto_left = pltpu.make_async_remote_copy(
            work.at[:, middle : middle + ICE_REACH], work.at[:, right : right + ICE_REACH],
            edge_send.at[1], edge_recv.at[1],
            device_id={"blk": device_of(lax.rem(mine + count - 1, count))}, device_id_type=MESH,
        )
        has_left, has_right = mine > 0, mine < count - 1
        arrive(first)
        work[0, middle:right] = recv[0].T
        work[1, middle:right] = recv[1].T
        one, two = recv[2].T, recv[3].T
        work[2, middle:right] = 8.0 * (one + two)
        work[3, middle:right] = 8.0 * (one - two)
        work[4, middle:right] = 16.0 * recv[4].T
        pl.when(has_right)(onto_right.start)
        pl.when(has_left)(onto_left.start)

        blank = jnp.zeros((fields, ICE_REACH, LANES), jnp.float32)

        @pl.when(jnp.logical_not(has_left))
        def _():
            work[:, left:middle] = blank

        @pl.when(jnp.logical_not(has_right))
        def _():
            work[:, right : right + ICE_REACH] = blank

        sent(first)
        sent(second)
        pl.semaphore_signal(go, inc=1, device_id={"comp": 1 - comp}, device_id_type=MESH)
        arrive(second)
        whole = slice(LEAD, LEAD + span)
        third = unpack(fields, filled, fields, ICE_REACH)
        stat[0, whole] = 4.0 * third
        stat[5, whole] = 8.0 * third
        push = unpack(fields + 1, filled, fields, ICE_REACH)
        stat[1, whole] = jnp.where(push > 0.0, 1.0 - push, 0.0)
        stat[2, whole] = (0.25 / 8.0) * push
        stat[3, whole] = unpack(fields + 2, filled, fields, ICE_REACH)
        stat[4, whole] = unpack(fields + 3, filled, fields, ICE_REACH)
        pl.when(has_left)(onto_right.wait_recv)
        pl.when(has_right)(onto_left.wait_recv)
        pl.when(has_right)(onto_right.wait_send)
        pl.when(has_left)(onto_left.wait_send)

        for group in range(SUBCYCLES // 4):
            low, high = LEAD + 8 * group, LEAD + span - 8 * group
            inner, outer = LEAD + ICE_REACH, LEAD + ICE_REACH + LANES

            def subcycle(step, carry, low=low, high=high):
                for begin, size in pieces(low, high, 8):
                    tile_stress(work, stat, begin, size)
                for begin, size in pieces(low, inner, 8) + pieces(outer, high, 8):
                    tile_velocity(work, stat, total, begin, size, None)
                for begin, size in pieces(inner, outer, 8):
                    tile_velocity(work, stat, total, begin, size, begin - inner)
                return carry

            lax.fori_loop(0, 4, subcycle, 0)

        own = slice(LEAD + ICE_REACH, LEAD + ICE_REACH + LANES)
        for channel in range(3):
            back[channel] = total[channel].T
        totals = homeward(back.at[0:3], home, (total_send, total_recv))
        start(totals)
        one, two = work[2, own], work[3, own]
        for field, value in enumerate(
            (
                work[0, own],
                work[1, own],
                (0.5 / 8.0) * (one + two),
                (0.5 / 8.0) * (one - two),
                (1.0 / 16.0) * work[4, own],
            )
        ):
            back[3 + field] = value.T
        states = homeward(back.at[3 : 3 + fields], state, (state_send, state_recv))
        start(states)
        home[:, :, lanes_of(mine)] = back[0:3, rows_of(me), :]
        state[:, :, lanes_of(mine)] = back[3 : 3 + fields, rows_of(me), :]
        share = 1.0 / SUBCYCLES
        def upper_chunk(turn, carry):
            for place in range(members):
                step = turn * members + place

                @pl.when(step > 0)
                def _():
                    home_copy(back.at[0:3], home, (total_send, total_recv), step).wait_recv()

            span = span_of(turn)
            covered = cover[:, span].astype(jnp.float32)
            for axis in range(2):
                mean[axis, :, span] = home[axis, :, span] * share - covered * current[axis, :, span]
            mean[2, :, span] = forcing[4, :, span] * covered * (home[2, :, span] * share)
            mean_copy(turn).start()
            split_values(mean, turn)
            remap(1, turn)
            return carry

        lax.fori_loop(0, chunks, upper_chunk, 0)
        gather_window(1)
        start(sides[1])
        pair[...] = mean[...]
        lower_half()
        start(sides[0])
        sent(totals)
        arrive(states)
        sent(states)
        for turn in range(chunks):
            mean_copy(turn).wait_send()
        sent(sides[0] + sides[1])

    @pl.when(comp == 1)
    def _():
        filled = fields + 2
        packed = filled + -(-filled // (LANES // (2 * SEA_REACH)))
        span = LANES + 2 * SEA_REACH
        for copy in loads:
            copy.wait()
        for axis in range(2):
            pack[fields + axis] = current[axis]
        spread_edges(filled, 0, filled, SEA_REACH)
        for array in (work, spare):
            for edge in (0, LEAD + span):
                array[:, edge : edge + LEAD] = jnp.zeros((array.shape[0], LEAD, LANES), jnp.float32)
        recv[0:packed, rows_of(me), :] = pack[0:packed, :, lanes_of(mine)]
        prepare_remap()
        pl.semaphore_wait(barrier, count)
        pl.semaphore_wait(go, 1)
        first = outward(0, packed, (first_send, first_recv))
        start(first)
        arrive(first)
        whole = slice(LEAD, LEAD + span)
        for field in range(fields):
            work[field, whole] = unpack(field, filled, 0, SEA_REACH)
        lane = lane_index((span, LANES))
        speed = courant * unpack(fields, filled, 0, SEA_REACH)
        drain = jnp.abs(speed)
        stat[0, whole] = jnp.where(lane == 0, 0.0, jnp.maximum(speed, 0.0))
        stat[1, whole] = jnp.where(lane == LANES - 1, 0.0, -jnp.minimum(speed, 0.0))
        speed = courant * unpack(fields + 1, filled, 0, SEA_REACH)
        stat[2, whole] = jnp.maximum(speed, 0.0)
        stat[3, whole] = -jnp.minimum(speed, 0.0)
        stat[4, whole] = drain + jnp.abs(speed)
        for group in range(SUBCYCLES // 8):
            low, high = LEAD + 8 * group, LEAD + span - 8 * group

            def substeps(step, carry, low=low, high=high):
                for begin, size in pieces(low, high, 16):
                    tile_ocean(work, spare, stat, begin, size)
                for begin, size in pieces(low, high, 16):
                    tile_ocean(spare, work, stat, begin, size)
                return carry

            lax.fori_loop(0, 4, substeps, 0)
        own = slice(LEAD + SEA_REACH, LEAD + SEA_REACH + LANES)
        for field in range(fields):
            back[3 + field] = work[field, own].T
        states = homeward(back.at[3 : 3 + fields], state, (state_send, state_recv))
        start(states)
        state[:, :, lanes_of(mine)] = back[3 : 3 + fields, rows_of(me), :]
        sent(first)
        def upper_chunk(turn, carry):
            mean_copy(turn).wait_recv()
            split_values(home, turn)
            remap(1, turn)
            return carry

        lax.fori_loop(0, chunks, upper_chunk, 0)
        gather_window(1)
        for channel in range(channels):
            sides[1][channel].wait_recv()
            window[1, channel] += beside[1, channel]
            onward[channel].start()
        lower_half()
        for channel in range(channels):
            sides[0][channel].wait_recv()
            pair[channel] = window[0, channel] + beside[0, channel]
        arrive(states)
        arrive(onward)
        pair[...] += before[...]
        state[0] -= dilution * pair[2]
        sent(states)
        sent(onward)


def run_tiles(initial, forcing, current, cover, targets, weights, count):
    fields, rows, cols = initial.shape
    f32 = jnp.float32
    most = fields + 4
    packed = most + -(-4 // (LANES // (2 * ICE_REACH)))
    tall = LANES + 2 * ICE_REACH + 2 * LEAD
    low_count = 256 if cols % 256 == 0 else 128
    high_count = rows * cols // low_count
    vmem = pl.BlockSpec(memory_space=pltpu.VMEM)
    dma = pltpu.SemaphoreType.DMA
    return pl.pallas_call(
        tiles_kernel,
        out_shape=(pltpu.VMEM((fields, rows, cols), f32), pltpu.VMEM((3, rows, cols), f32)),
        in_specs=[pl.BlockSpec(memory_space=pl.ANY)] * 6,
        out_specs=(vmem, vmem),
        scratch_shapes=[
            pltpu.VMEM((packed, rows, cols), f32),
            pltpu.VMEM(forcing.shape, f32),
            pltpu.VMEM(current.shape, f32),
            pltpu.VMEM(cover.shape, cover.dtype),
            pltpu.VMEM(targets.shape[1:], targets.dtype),
            pltpu.VMEM(weights.shape[1:], weights.dtype),
            pltpu.VMEM((packed, LANES, LANES), f32),
            pltpu.VMEM((fields, tall, LANES), f32),
            pltpu.VMEM((fields, tall, LANES), f32),
            pltpu.VMEM((6, tall, LANES), f32),
            pltpu.VMEM((3, LANES, LANES), f32),
            pltpu.VMEM((3 + fields, LANES, LANES), f32),
            pltpu.VMEM((3, rows, cols), f32),
            pltpu.VMEM((3, rows, cols), f32),
            pltpu.VMEM((2, 6 * high_count, low_count), f32),
            pltpu.VMEM((2, 3, rows, cols), f32),
            pltpu.VMEM((2, 3, rows, cols), f32),
            pltpu.VMEM((3, rows, cols), f32),
            pltpu.VMEM((rows, cols), f32),
            pltpu.VMEM((2, rows, cols), f32),
            pltpu.VMEM((rows * cols, low_count), jnp.bfloat16),
            pltpu.VMEM((6, rows, cols), f32),
            dma((6,)),
            *[dma((count,)) for _ in range(8)],
            dma((cols // low_count,)), dma((cols // low_count,)), dma((2, 3)), dma((2, 3)), dma((3,)), dma((3,)), dma((2,)), dma((2,)),
            pltpu.SemaphoreType.REGULAR,
        ],
        compiler_params=pltpu.CompilerParams(collective_id=0, has_side_effects=True),
        name="tiles",
    )(initial, forcing, current, cover, targets, weights)


def remap_kernel(average, targets, weights, window, acc, low_index, high_index):
    comp = lax.axis_index("comp")
    channels, rows, cols = average.shape
    span = low_index.shape[1]
    low_count, high_count = low_index.shape[0], high_index.shape[0]
    bf16 = jnp.bfloat16
    blocks = cols // low_count
    low_index[...] = lax.broadcasted_iota(jnp.int32, low_index.shape, 0).astype(bf16)
    high_index[...] = lax.broadcasted_iota(jnp.int32, high_index.shape, 0).astype(bf16)
    acc[...] = jnp.zeros_like(acc)

    def one_row(row, carry):
        for piece in range(cols // span):
            place = pl.ds(piece * span, span)
            target = targets[comp, pl.ds(row, 1), place]
            scale = weights[comp, pl.ds(row, 1), place].astype(jnp.float32) * (1.0 / weight_norm)
            low = lax.rem(target, low_count)
            block = lax.rem(lax.div(target, low_count), blocks)
            line = lax.div(target, cols)
            high = (lax.div(line, rows) * blocks + block) * rows + lax.rem(line, rows)
            low_hot = jnp.where(low_index[...] == low.astype(bf16), bf16(1), bf16(0))
            match = high_index[...] == high.astype(bf16)
            parts = []
            for channel in range(channels):
                value = average[channel, pl.ds(row, 1), place] * scale
                coarse = value.astype(bf16)
                fine = (value - coarse.astype(jnp.float32)).astype(bf16)
                parts.append(jnp.where(match, coarse, bf16(0)))
                parts.append(jnp.where(match, fine, bf16(0)))
            spread = jnp.concatenate(parts, axis=0)
            acc[...] += lax.dot_general(
                spread, low_hot, (((1,), (1,)), ((), ())), preferred_element_type=jnp.float32
            )
        return carry

    lax.fori_loop(0, rows, one_row, 0)
    for channel in range(channels):
        for half in range(2):
            for block in range(blocks):
                base = 2 * channel * high_count + (half * blocks + block) * rows
                window[channel, half, :, block * low_count : (block + 1) * low_count] = (
                    acc[base : base + rows] + acc[base + high_count : base + high_count + rows]
                )


def run_remap(average, targets, weights):
    channels, rows, cols = average.shape
    low_count = 256 if cols % 256 == 0 else 128
    high_count = 2 * rows * cols // low_count
    span = min(1024, cols)
    vmem = pl.BlockSpec(memory_space=pltpu.VMEM)
    return pl.pallas_call(
        remap_kernel,
        out_shape=jax.ShapeDtypeStruct((channels, 2, rows, cols), jnp.float32),
        in_specs=[vmem] * 3,
        out_specs=vmem,
        scratch_shapes=[
            pltpu.VMEM((2 * channels * high_count, low_count), jnp.float32),
            pltpu.VMEM((low_count, span), jnp.bfloat16),
            pltpu.VMEM((high_count, span), jnp.bfloat16),
        ],
        compiler_params=pltpu.CompilerParams(vmem_limit_bytes=40 * 1024 * 1024),
        name="remap",
    )(average, targets, weights)


def join_kernel(
    window, state, average, out_state, out_pair, beside, carry, before,
    side_send, side_recv, next_send, next_recv,
):
    me = lax.axis_index("blk")
    comp = lax.axis_index("comp")
    count = lax.axis_size("blk")
    right, left = lax.rem(me + 1, count), lax.rem(me + count - 1, count)
    barrier = pltpu.get_barrier_semaphore()
    pl.semaphore_signal(barrier, inc=1, device_id={"blk": right}, device_id_type=MESH)
    pl.semaphore_signal(barrier, inc=1, device_id={"blk": left}, device_id_type=MESH)
    pl.semaphore_signal(barrier, inc=1, device_id={"comp": 1 - comp}, device_id_type=MESH)
    pl.semaphore_wait(barrier, 3)
    channels = window.shape[0]
    sides, onward = [], []
    for half in (1, 0):
        for channel in range(channels):
            sides.append(
                pltpu.make_async_remote_copy(
                    window.at[channel, half], beside.at[channel, half],
                    side_send.at[half, channel], side_recv.at[half, channel],
                    device_id={"comp": 1 - comp}, device_id_type=MESH,
                )
            )
    for channel in range(channels):
        onward.append(
            pltpu.make_async_remote_copy(
                carry.at[channel], before.at[channel],
                next_send.at[channel], next_recv.at[channel],
                device_id={"blk": right}, device_id_type=MESH,
            )
        )

    @pl.when(comp == 0)
    def _():
        for copy in sides:
            copy.start()
        out_state[...] = state[...]
        out_pair[...] = average[...]
        for copy in sides:
            copy.wait_send()

    @pl.when(comp == 1)
    def _():
        for channel in range(channels):
            sides[channel].wait_recv()
            carry[channel] = window[channel, 1] + beside[channel, 1]
            onward[channel].start()
        for channel in range(channels):
            sides[channels + channel].wait_recv()
            out_pair[channel] = window[channel, 0] + beside[channel, 0]
        out_state[...] = state[...]
        for channel in range(channels):
            onward[channel].wait_recv()
            out_pair[channel] += before[channel]
        out_state[0] -= dilution * out_pair[2]
        for channel in range(channels):
            onward[channel].wait_send()


def run_join(window, state, average):
    channels, rows, cols = average.shape
    vmem = pl.BlockSpec(memory_space=pltpu.VMEM)
    dma = pltpu.SemaphoreType.DMA
    return pl.pallas_call(
        join_kernel,
        out_shape=(
            jax.ShapeDtypeStruct(state.shape, jnp.float32),
            jax.ShapeDtypeStruct(average.shape, jnp.float32),
        ),
        in_specs=[vmem] * 3,
        out_specs=(vmem, vmem),
        scratch_shapes=[
            pltpu.VMEM(window.shape, jnp.float32),
            pltpu.VMEM(average.shape, jnp.float32),
            pltpu.VMEM(average.shape, jnp.float32),
            dma((2, channels)), dma((2, channels)), dma((channels,)), dma((channels,)),
        ],
        compiler_params=pltpu.CompilerParams(
            collective_id=1, has_side_effects=True, vmem_limit_bytes=40 * 1024 * 1024
        ),
        name="join",
    )(window, state, average)


def body(count, initial, ice_forcing, ocean_current, ice_cover, targets, weights):
    if fits_tiles(count, *initial.shape[2:]):
        state, coupled = run_tiles(
            initial[0], ice_forcing, ocean_current, ice_cover, targets, weights, count
        )
    else:
        state, average = run_turns(initial[0], ice_forcing, ocean_current, ice_cover)
        window = run_remap(average, targets, weights)
        state, coupled = run_join(window, state, average)
    return (state[None], coupled[None])


def solution(mesh):
    placed = (
        P("comp", None, "blk", None),
        P(None, "blk", None),
        P(None, "blk", None),
        P("blk", None),
        P(None, "blk", None),
        P(None, "blk", None),
    )
    return jax.shard_map(
        functools.partial(body, mesh.shape["blk"]),
        mesh=mesh,
        in_specs=placed,
        out_specs=(P("comp", None, "blk", None), P("comp", None, "blk", None)),
        check_vma=False,
    )
```

```python
import functools

import jax
import jax.numpy as jnp
from jax import lax
from jax.experimental import pallas as pl
from jax.experimental.pallas import tpu as pltpu
from jax.sharding import PartitionSpec as P

SUBCYCLES = 16
MESH = pl.DeviceIdType.MESH
PAD = 128
PARTS = 2

coriolis = 0.1
inertia = 4.0
courant = 0.2
dilution = 0.5
weight_norm = 4.0
level_speed = (1.0, 0.8, 0.6, 0.45, 0.3)


def rolled(value, steps, axis):
    return pltpu.roll(value, steps % value.shape[axis], axis)


def rows_diff(value):
    return rolled(value, -1, 0) - rolled(value, 1, 0)


def chunk_width(cols):
    return 256 if cols % 256 == 0 else 128


def stress_stage(work, stat, start, width):
    wide = pl.ds(start, width + 2 * PAD)
    mid = pl.ds(start + PAD, width)
    inner = slice(PAD, PAD + width)
    vel_x, vel_y = work[0, :, wide], work[1, :, wide]
    cx = (rolled(vel_x, -1, 1) - rolled(vel_x, 1, 1))[:, inner]
    cy = (rolled(vel_y, -1, 1) - rolled(vel_y, 1, 1))[:, inner]
    rx = rows_diff(vel_x[:, inner])
    ry = rows_diff(vel_y[:, inner])
    e_d = rx + cy
    e_t = rx - cy
    e_s = cx + ry
    inv = lax.rsqrt(0.25 * (e_d * e_d) + 0.0625 * (e_t * e_t + e_s * e_s) + 0.01)
    third = stat[0, :, pl.ds(start, width)]
    scaled = third * inv
    work[2, :, mid] = work[2, :, mid] * (2.0 / 3.0) + (0.5 * scaled * e_d - third)
    work[3, :, mid] = work[3, :, mid] * (2.0 / 3.0) + 0.125 * scaled * e_t
    work[4, :, mid] = work[4, :, mid] * (2.0 / 3.0) + 0.0625 * scaled * e_s


def velocity_stage(work, stat, total, start, width, rows):
    wide = pl.ds(start, width + 2 * PAD)
    mid = pl.ds(start + PAD, width)
    here = pl.ds(start, width)
    inner = slice(PAD, PAD + width)
    shear = work[4, :, wide]
    one, two = work[2, :, wide], work[3, :, wide]
    across_shear = (rolled(shear, -1, 1) - rolled(shear, 1, 1))[:, inner]
    lower = one - two
    across_yy = (rolled(lower, -1, 1) - rolled(lower, 1, 1))[:, inner]
    force_x = rows_diff((one + two)[:, inner]) + 2.0 * across_shear
    force_y = 2.0 * rows_diff(shear[:, inner]) + across_yy
    old_x, old_y = work[0, :, mid], work[1, :, mid]
    keep, push = stat[1, :, here], stat[2, :, here]
    new_x = keep * (old_x + coriolis * old_y) + push * force_x + stat[3, :, here]
    new_y = keep * (old_y - coriolis * old_x) + push * force_y + stat[4, :, here]
    work[0, :, mid] = new_x
    work[1, :, mid] = new_y
    own_x, own_y = new_x[rows : 2 * rows], new_y[rows : 2 * rows]
    total[0, :, here] += own_x
    total[1, :, here] += own_y
    total[2, :, here] += jnp.sqrt(1.0 + own_x * own_x + own_y * own_y)


def ocean_stage(source, target, coef, start, width):
    wide = pl.ds(start, width + 2 * PAD)
    mid = pl.ds(start + PAD, width)
    here = pl.ds(start, width)
    inner = slice(PAD, PAD + width)
    up, down, east, west = (coef[i, :, here] for i in range(4))
    for level, speed in enumerate(level_speed):
        tracer = source[level, :, wide]
        centre = tracer[:, inner]
        right = rolled(tracer, -1, 1)[:, inner] - centre
        left = centre - rolled(tracer, 1, 1)[:, inner]
        above = rolled(centre, -1, 0) - centre
        below = centre - rolled(centre, 1, 0)
        change = up * below + down * above + east * left + west * right
        target[level, :, mid] = centre - speed * change


def turns_kernel(
    initial_in, forcing_in, current_in, cover_in, state, average,
    initial, forcing, current, cover,
    own, own_stat, halo, halo_stat, work, spare, stat, total, mean,
    load, near_send, near_recv, far_send, far_recv,
    stat_near_send, stat_near_recv, stat_far_send, stat_far_recv,
    mean_send, mean_recv, go,
):
    me = lax.axis_index("blk")
    comp = lax.axis_index("comp")
    count = lax.axis_size("blk")
    fields, rows, cols = initial.shape
    width = chunk_width(cols)
    chunks = cols // width
    near = 1 - lax.rem(me, 2)
    far = 1 - near
    partner = me + 2 * near - 1
    relay_to = me + 4 * near - 2
    relay_from = me - 4 * near + 2
    can_send = jnp.logical_and(relay_to >= 0, relay_to < count)
    can_recv = jnp.logical_and(relay_from >= 0, relay_from < count)
    relay_to = lax.rem(relay_to + count, count)
    relay_from = lax.rem(relay_from + count, count)

    barrier = pltpu.get_barrier_semaphore()

    def greet(where):
        pl.semaphore_signal(barrier, inc=1, device_id=where, device_id_type=MESH)

    greet({"blk": partner})
    greet({"comp": 1 - comp})
    pl.when(can_send)(lambda: greet({"blk": relay_to}))
    pl.when(can_recv)(lambda: greet({"blk": relay_from}))
    loads = [
        pltpu.make_async_copy(source, target, load.at[i])
        for i, (source, target) in enumerate(
            (
                (initial_in, initial),
                (current_in, current),
                (forcing_in, forcing),
                (cover_in, cover),
            )
        )
    ]
    for copy in loads:
        copy.start()

    work[...] = jnp.zeros_like(work)
    total[...] = jnp.zeros_like(total)

    def enter():
        pl.semaphore_wait(barrier, 2 + can_send.astype(jnp.int32) + can_recv.astype(jnp.int32))

    def copies(source, target, pieces, near_sems, far_sems):
        first, second = [], []
        wide = cols // PARTS
        for index in range(pieces * PARTS):
            piece, place = index // PARTS, pl.ds(index % PARTS * wide, wide)
            first.append(
                pltpu.make_async_remote_copy(
                    source.at[piece, :, place], target.at[far, piece, :, place],
                    near_sems[0].at[index], near_sems[1].at[index],
                    device_id={"blk": partner}, device_id_type=MESH,
                )
            )
            second.append(
                pltpu.make_async_remote_copy(
                    target.at[near, piece, :, place], target.at[far, piece, :, place],
                    far_sems[0].at[index], far_sems[1].at[index],
                    device_id={"blk": relay_to}, device_id_type=MESH,
                )
            )
        return first, second

    def start(pair):
        for copy in pair[0]:
            copy.start()

    def relay(pair):
        for first, second in zip(*pair):
            first.wait_recv()
            pl.when(can_send)(second.start)

    def arrive(pair):
        @pl.when(can_recv)
        def _():
            for copy in pair[1]:
                copy.wait_recv()

    def sent(pair):
        for copy in pair[0]:
            copy.wait_send()

        @pl.when(can_send)
        def _():
            for copy in pair[1]:
                copy.wait_send()

    def clear_edges(turns):
        @pl.when(jnp.logical_not(can_recv))
        def _():
            halo_stat[far] = jnp.zeros(halo_stat.shape[1:], jnp.float32)
            for turn in range(turns):
                halo[turn, far] = jnp.zeros(halo.shape[2:], jnp.float32)

    inside = slice(PAD, PAD + cols)

    def fill_own(source):
        for field in range(fields):
            work[field, rows : 2 * rows, inside] = source[field]

    def fill_sides(turn):
        for field in range(fields):
            work[field, 0:rows, inside] = halo[turn, 0, field]
            work[field, 2 * rows : 3 * rows, inside] = halo[turn, 1, field]

    def exchange_of(turn, source):
        return copies(
            source, halo.at[turn], fields,
            (near_send.at[turn], near_recv.at[turn]), (far_send.at[turn], far_recv.at[turn]),
        )

    def stats_of(source, pieces):
        return copies(
            source, halo_stat, pieces,
            (stat_near_send, stat_near_recv), (stat_far_send, stat_far_recv),
        )

    mean_copy = pltpu.make_async_remote_copy(
        mean, average, mean_send, mean_recv,
        device_id={"comp": 1 - comp}, device_id_type=MESH,
    )

    @pl.when(comp == 0)
    def _():
        depth = rows // 2
        turns = SUBCYCLES // depth
        clear_edges(turns)
        loads[0].wait()
        enter()
        pairs = [exchange_of(0, initial)]
        start(pairs[0])
        for copy in loads[1:]:
            copy.wait()
        covered = cover[...].astype(jnp.float32)
        push = covered / (inertia * forcing[0] + 1.0)
        own_stat[0] = forcing[1] * covered * (1.0 / 3.0)
        own_stat[1] = push
        own_stat[2] = push * (forcing[2] + current[0])
        own_stat[3] = push * (forcing[3] + current[1])
        stat_pair = stats_of(own_stat, 4)
        start(stat_pair)
        for turn in range(turns):
            source = initial if turn == 0 else own.at[turn - 1]
            if turn > 0:
                pairs.append(exchange_of(turn, source))
                start(pairs[turn])
            relay(pairs[turn])
            if turn == 0:
                relay(stat_pair)
                pl.semaphore_signal(
                    go, inc=1, device_id={"comp": 1 - comp}, device_id_type=MESH
                )
            fill_own(source)
            arrive(pairs[turn])
            if turn == 0:
                arrive(stat_pair)
                for place, block in enumerate((halo_stat.at[0], own_stat, halo_stat.at[1])):
                    span = slice(place * rows, (place + 1) * rows)
                    push = block[1]
                    stat[0, span] = block[0]
                    stat[1, span] = jnp.where(push > 0.0, 1.0 - push, 0.0)
                    stat[2, span] = 0.25 * push
                    stat[3, span] = block[2]
                    stat[4, span] = block[3]
            fill_sides(turn)

            def subcycle(step, carry):
                for chunk in range(chunks):
                    stress_stage(work, stat, chunk * width, width)
                for chunk in range(chunks):
                    velocity_stage(work, stat, total, chunk * width, width, rows)
                return carry

            lax.fori_loop(0, depth, subcycle, 0)
            final = state if turn == turns - 1 else own.at[turn]
            for field in range(fields):
                final[field] = work[field, rows : 2 * rows, inside]
        share = 1.0 / SUBCYCLES
        covered = cover[...].astype(jnp.float32)
        mean[0] = total[0] * share - covered * current[0]
        mean[1] = total[1] * share - covered * current[1]
        mean[2] = forcing[4] * covered * (total[2] * share)
        mean_copy.start()
        average[...] = mean[...]
        sent(stat_pair)
        for pair in pairs:
            sent(pair)
        mean_copy.wait_send()

    @pl.when(comp == 1)
    def _():
        depth = rows
        turns = SUBCYCLES // depth
        clear_edges(turns)
        spare[...] = jnp.zeros_like(spare)
        for copy in loads:
            copy.wait()
        enter()
        pl.semaphore_wait(go, 1)
        pairs = [exchange_of(0, initial)]
        start(pairs[0])
        stat_pair = stats_of(current, 2)
        start(stat_pair)
        for turn in range(turns):
            source = initial if turn == 0 else own.at[turn - 1]
            if turn > 0:
                pairs.append(exchange_of(turn, source))
                start(pairs[turn])
            relay(pairs[turn])
            if turn == 0:
                relay(stat_pair)
            fill_own(source)
            arrive(pairs[turn])
            if turn == 0:
                arrive(stat_pair)
                for place in range(3):
                    span = slice(place * rows, (place + 1) * rows)
                    for axis in range(2):
                        if place == 1:
                            speed = current[axis]
                        else:
                            speed = halo_stat[place // 2, axis]
                        stat[2 * axis, span] = courant * jnp.maximum(speed, 0.0)
                        stat[2 * axis + 1, span] = courant * jnp.minimum(speed, 0.0)
            fill_sides(turn)

            def substeps(step, carry):
                for chunk in range(chunks):
                    ocean_stage(work, spare, stat, chunk * width, width)
                for chunk in range(chunks):
                    ocean_stage(spare, work, stat, chunk * width, width)
                return carry

            lax.fori_loop(0, depth // 2, substeps, 0)
            final = state if turn == turns - 1 else own.at[turn]
            for field in range(fields):
                final[field] = work[field, rows : 2 * rows, inside]
        sent(stat_pair)
        for pair in pairs:
            sent(pair)
        mean_copy.wait_recv()


def run_turns(initial, forcing, current, cover):
    fields, rows, cols = initial.shape
    most = SUBCYCLES // (rows // 2)
    f32 = jnp.float32
    vmem = pl.BlockSpec(memory_space=pltpu.VMEM)
    dma = pltpu.SemaphoreType.DMA
    return pl.pallas_call(
        turns_kernel,
        out_shape=(
            jax.ShapeDtypeStruct((fields, rows, cols), f32),
            jax.ShapeDtypeStruct((3, rows, cols), f32),
        ),
        in_specs=[pl.BlockSpec(memory_space=pl.ANY)] * 4,
        out_specs=(vmem, vmem),
        scratch_shapes=[
            pltpu.VMEM(initial.shape, f32),
            pltpu.VMEM(forcing.shape, f32),
            pltpu.VMEM(current.shape, f32),
            pltpu.VMEM(cover.shape, cover.dtype),
            pltpu.VMEM((most, fields, rows, cols), f32),
            pltpu.VMEM((4, rows, cols), f32),
            pltpu.VMEM((most, 2, fields, rows, cols), f32),
            pltpu.VMEM((2, 4, rows, cols), f32),
            pltpu.VMEM((fields, 3 * rows, cols + 2 * PAD), f32),
            pltpu.VMEM((fields, 3 * rows, cols + 2 * PAD), f32),
            pltpu.VMEM((5, 3 * rows, cols), f32),
            pltpu.VMEM((3, rows, cols), f32),
            pltpu.VMEM((3, rows, cols), f32),
            dma((4,)),
            *[dma((most, fields * PARTS)) for _ in range(4)],
            *[dma((4 * PARTS,)) for _ in range(4)],
            dma, dma, pltpu.SemaphoreType.REGULAR,
        ],
        compiler_params=pltpu.CompilerParams(
            collective_id=0, has_side_effects=True
        ),
        name="turns",
    )(initial, forcing, current, cover)


LANES = 128
LEAD = 8
ICE_REACH = 2 * SUBCYCLES
SEA_REACH = SUBCYCLES


def fits_tiles(count, rows, cols):
    return count * rows == LANES and cols == count * LANES and count > 1


def lane_index(shape):
    return lax.broadcasted_iota(jnp.int32, shape, len(shape) - 1)


def lane_diff(value):
    lane = lane_index(value.shape)
    after = jnp.where(lane == LANES - 1, 0.0, pltpu.roll(value, LANES - 1, 1))
    before = jnp.where(lane == 0, 0.0, pltpu.roll(value, 1, 1))
    return after - before


def tile_stress(work, stat, low, size):
    here, up, down = (pl.ds(low + shift, size) for shift in (0, 1, -1))
    cx = work[0, up] - work[0, down]
    cy = work[1, up] - work[1, down]
    rx, ry = lane_diff(work[0, here]), lane_diff(work[1, here])
    e_d = rx + cy
    e_t = rx - cy
    e_s = cx + ry
    fourfold = 4.0 * e_d
    scaled = stat[0, here] * lax.rsqrt(fourfold * e_d + (e_t * e_t + e_s * e_s) + 0.16)
    rest = stat[5, here]
    work[2, here] = work[2, here] * (2.0 / 3.0) + (scaled * (fourfold + e_t) - rest)
    work[3, here] = work[3, here] * (2.0 / 3.0) + (scaled * (fourfold - e_t) - rest)
    work[4, here] = work[4, here] * (2.0 / 3.0) + scaled * e_s


def tile_velocity(work, stat, total, low, size, own):
    here, up, down = (pl.ds(low + shift, size) for shift in (0, 1, -1))
    force_x = lane_diff(work[2, here]) + (work[4, up] - work[4, down])
    force_y = lane_diff(work[4, here]) + (work[3, up] - work[3, down])
    old_x, old_y = work[0, here], work[1, here]
    keep, push = stat[1, here], stat[2, here]
    new_x = keep * (old_x + coriolis * old_y) + push * force_x + stat[3, here]
    new_y = keep * (old_y - coriolis * old_x) + push * force_y + stat[4, here]
    work[0, here] = new_x
    work[1, here] = new_y
    if own is not None:
        place = pl.ds(own, size)
        total[0, place] += new_x
        total[1, place] += new_y
        square = 1.0 + new_x * new_x + new_y * new_y
        total[2, place] += square * lax.rsqrt(square)


def tile_ocean(source, target, stat, low, size):
    here, up, down = (pl.ds(low + shift, size) for shift in (0, 1, -1))
    before, after, left, right, drain = (stat[i, here] for i in range(5))
    for level, speed in enumerate(level_speed):
        centre = source[level, here]
        inflow = before * pltpu.roll(centre, 1, 1) + after * pltpu.roll(centre, LANES - 1, 1)
        inflow += left * source[level, down] + right * source[level, up]
        target[level, here] = centre + speed * (inflow - drain * centre)


def pieces(low, high, step):
    return [(start, min(step, high - start)) for start in range(low, high, step)]


def tiles_kernel(
    initial_in, forcing_in, current_in, cover_in, targets_in, weights_in, state, pair,
    pack, forcing, current, cover, targets, weights,
    recv, work, spare, stat, total, back, home, mean, acc, window, beside, before,
    low, high, hot, parts,
    load, first_send, first_recv, second_send, second_recv,
    total_send, total_recv, state_send, state_recv, mean_send, mean_recv,
    side_send, side_recv, next_send, next_recv, edge_send, edge_recv, go,
):
    me = lax.axis_index("blk")
    comp = lax.axis_index("comp")
    count = lax.axis_size("blk")
    fields, rows, cols = initial_in.shape
    barrier = pltpu.get_barrier_semaphore()

    def greet(where):
        pl.semaphore_signal(barrier, inc=1, device_id=where, device_id_type=MESH)

    def other(step):
        return lax.bitwise_xor(me, step)

    steps = range(1, count)
    for step in steps:
        greet({"blk": other(step)})
    greet({"comp": 1 - comp})

    loads = [
        pltpu.make_async_copy(source, target, load.at[i])
        for i, (source, target) in enumerate(
            (
                (initial_in, pack.at[0:fields]),
                (current_in, current),
                (forcing_in, forcing),
                (cover_in, cover),
                (targets_in.at[comp], targets),
                (weights_in.at[comp], weights),
            )
        )
    ]
    for copy in loads:
        copy.start()

    turn_size = min(4, count)

    def mirrored(group, place):
        return place + lax.rem(group, 2) * (turn_size - 1 - 2 * place)

    def column_of(device):
        group, place = lax.div(device, turn_size), lax.rem(device, turn_size)
        return group * turn_size + mirrored(group, lax.bitwise_xor(place, lax.div(place, 2)))

    def device_of(column):
        group, place = lax.div(column, turn_size), lax.rem(column, turn_size)
        place = mirrored(group, place)
        return group * turn_size + lax.bitwise_xor(place, lax.div(place, 2))

    mine = column_of(me)

    def lanes_of(block):
        return pl.ds(pl.multiple_of(block * LANES, LANES), LANES)

    def rows_of(block):
        return pl.ds(pl.multiple_of(block * rows, rows), rows)

    def outward(low, high, sems):
        return [
            pltpu.make_async_remote_copy(
                pack.at[low:high, :, lanes_of(column_of(other(step)))],
                recv.at[low:high, rows_of(me), :],
                sems[0], sems[1],
                device_id={"blk": other(step)}, device_id_type=MESH,
            )
            for step in steps
        ]

    width = hot.shape[1]
    members = width // LANES
    chunks = cols // width

    def home_copy(source, target, sems, step):
        return pltpu.make_async_remote_copy(
            source.at[:, rows_of(other(step)), :],
            target.at[:, :, lanes_of(mine)],
            sems[0], sems[1],
            device_id={"blk": other(step)}, device_id_type=MESH,
        )

    def homeward(source, target, sems):
        return [home_copy(source, target, sems, step) for step in steps]

    def totals_home():
        return [
            home_copy(back.at[0:3], home, (total_send, total_recv.at[step // members]), step)
            for step in steps
        ]


    def chunk_of(turn):
        device = members * lax.bitwise_xor(lax.div(me, members), turn)
        return lax.div(column_of(device), members)

    def span_of(turn):
        return pl.ds(pl.multiple_of(chunk_of(turn) * width, width), width)

    def start(copies):
        for copy in copies:
            copy.start()

    def bulk(block, sems):
        return pltpu.make_async_remote_copy(
            block, block, sems[0], sems[1],
            device_id={"comp": 1 - comp}, device_id_type=MESH,
        )

    def outward_bulk(low, high, sems):
        return bulk(recv.at[low:high, 0 : (count - 1) * rows, :], sems)

    def homeward_bulk(low, high, sems):
        return bulk(back.at[low:high, 0 : (count - 1) * rows, :], sems)

    def spread_edges(base, low, filled, reach):
        group = LANES // (2 * reach)
        lane = lane_index((rows, LANES))
        slot = lane // (2 * reach)
        leading = lane % (2 * reach) < reach
        zero = jnp.zeros((rows, LANES), jnp.float32)
        for tile in range(-(-(filled - low) // group)):
            members = range(low + tile * group, min(filled, low + (tile + 1) * group))
            turned = []
            for block in range(count):
                here = slice(block * LANES, (block + 1) * LANES)
                merged = zero
                for place, field in enumerate(members):
                    shift = (2 * place + 1) * reach % LANES
                    value = pack[field, :, here]
                    moved = pltpu.roll(value, shift, 1) if shift else value
                    merged = jnp.where(slot == place, moved, merged)
                turned.append(merged)
            for block in range(count):
                before = turned[block - 1] if block > 0 else zero
                after = turned[block + 1] if block < count - 1 else zero
                here = slice(block * LANES, (block + 1) * LANES)
                pack[base + tile, :, here] = jnp.where(leading, before, after)

    def unpack(field, base, low, reach):
        group = LANES // (2 * reach)
        value = recv[field].T
        edge = recv[base + (field - low) // group].T
        start = (field - low) % group * 2 * reach
        return jnp.concatenate(
            [edge[start : start + reach], value, edge[start + reach : start + 2 * reach]], axis=0
        )

    channels = pair.shape[0]

    def mean_copy(turn):
        return pltpu.make_async_remote_copy(
            mean.at[:, :, span_of(turn)], home.at[:, :, span_of(turn)],
            mean_send, mean_recv.at[turn],
            device_id={"comp": 1 - comp}, device_id_type=MESH,
        )
    sides = [
        [
            pltpu.make_async_remote_copy(
                window.at[half, channel], beside.at[half, channel],
                side_send, side_recv.at[half, channel],
                device_id={"comp": 1 - comp}, device_id_type=MESH,
            )
            for channel in range(channels)
        ]
        for half in range(2)
    ]
    onward = [
        pltpu.make_async_remote_copy(
            window.at[1, channel], before.at[channel],
            next_send, next_recv,
            device_id={"blk": lax.rem(me + 1, count)}, device_id_type=MESH,
        )
        for channel in range(channels)
    ]

    def prepare_remap():
        target = targets[...]
        block = lax.rem(lax.div(target, width), chunks)
        line = lax.div(target, cols)
        low[...] = lax.rem(target, width).astype(jnp.float32)
        for half in range(2):
            inside = lax.div(line, rows) == half
            place = block * rows + line - half * rows
            high[half] = jnp.where(inside, place, chunks * rows).astype(jnp.float32)
        acc[...] = jnp.zeros_like(acc)

        def one_row(row, carry):
            lane = lane_index((LANES, LANES)).astype(jnp.float32)
            line = low[pl.ds(row, 1), :]
            for start in range(0, cols, LANES):
                value = jnp.broadcast_to(line[:, start : start + LANES], (LANES, LANES)).T
                base = start // width * rows * width + start % width
                place = pl.ds(pl.multiple_of(base + row * width, LANES), LANES)
                for first in range(0, width, LANES):
                    hit = jnp.where(value == lane + float(first), 1.0, 0.0)
                    hot[place, first : first + LANES] = hit.astype(hot.dtype)
            return carry

        lax.fori_loop(0, rows, one_row, 0)

    def split_values(values, turn):
        span = span_of(turn)
        scale = weights[:, span].astype(jnp.float32) * (1.0 / weight_norm)
        for channel in range(channels):
            value = values[channel, :, span] * scale
            coarse = value.astype(jnp.bfloat16).astype(jnp.float32)
            parts[2 * channel, :, span] = coarse
            parts[2 * channel + 1, :, span] = value - coarse

    def remap(half, turn):
        bf16 = jnp.bfloat16
        tall = 16
        span = span_of(turn)
        index = lax.broadcasted_iota(jnp.int32, (tall, width), 0).astype(bf16)

        def lines(block):
            return [
                jnp.broadcast_to(block[row : row + 1], (tall, width)).astype(bf16)
                for row in range(rows)
            ]

        levels = lines(high[half, :, span])
        matches = [
            [level == index + bf16(first) for level in levels]
            for first in range(0, chunks * rows, tall)
        ]
        spread = []
        for part in range(2 * channels):
            values = lines(parts[part, :, span])
            for match in matches:
                kept = [jnp.where(m, v, bf16(0)) for m, v in zip(match, values)]
                spread.append(jnp.concatenate(kept, axis=1))
        depth = rows * width
        place = pl.ds(pl.multiple_of(chunk_of(turn) * depth, depth), depth)
        acc[half] += jnp.dot(
            jnp.concatenate(spread, axis=0), hot[place, :], preferred_element_type=jnp.float32
        )

    def gather_window(half):
        tall = chunks * rows
        for channel in range(channels):
            for block in range(chunks):
                base = 2 * channel * tall + block * rows
                window[half, channel, :, block * width : (block + 1) * width] = (
                    acc[half, base : base + rows] + acc[half, base + tall : base + tall + rows]
                )

    def lower_half():
        def one_chunk(turn, carry):
            remap(0, turn)
            return carry

        lax.fori_loop(0, chunks, one_chunk, 0, unroll=4)
        gather_window(0)

    @pl.when(comp == 0)
    def _():
        filled = fields + 4
        packed = filled + -(-4 // (LANES // (2 * ICE_REACH)))
        span = LANES + 2 * ICE_REACH
        loads[0].wait()
        pl.semaphore_wait(barrier, count)
        start(outward(0, fields, (first_send, first_recv)))
        for copy in loads[1:4]:
            copy.wait()
        covered = cover[...].astype(jnp.float32)
        push = covered / (inertia * forcing[0] + 1.0)
        pack[fields] = forcing[1] * covered * (1.0 / 3.0)
        pack[fields + 1] = push
        pack[fields + 2] = push * (forcing[2] + current[0])
        pack[fields + 3] = push * (forcing[3] + current[1])
        spread_edges(filled, fields, filled, ICE_REACH)
        start(outward(fields, packed, (second_send, second_recv)))
        recv[0:packed, rows_of(me), :] = pack[0:packed, :, lanes_of(mine)]
        total[...] = jnp.zeros_like(total)
        for array in (work, stat):
            for edge in (0, LEAD + span):
                array[:, edge : edge + LEAD] = jnp.zeros((array.shape[0], LEAD, LANES), jnp.float32)
        for copy in loads[4:]:
            copy.wait()
        prepare_remap()
        left, middle, right = LEAD, LEAD + ICE_REACH, LEAD + ICE_REACH + LANES
        onto_right = pltpu.make_async_remote_copy(
            work.at[:, right - ICE_REACH : right], work.at[:, left:middle],
            edge_send.at[0], edge_recv.at[0],
            device_id={"blk": device_of(lax.rem(mine + 1, count))}, device_id_type=MESH,
        )
        onto_left = pltpu.make_async_remote_copy(
            work.at[:, middle : middle + ICE_REACH], work.at[:, right : right + ICE_REACH],
            edge_send.at[1], edge_recv.at[1],
            device_id={"blk": device_of(lax.rem(mine + count - 1, count))}, device_id_type=MESH,
        )
        has_left, has_right = mine > 0, mine < count - 1
        outward_bulk(0, fields, (first_send, first_recv)).wait_recv()
        work[0, middle:right] = recv[0].T
        work[1, middle:right] = recv[1].T
        one, two = recv[2].T, recv[3].T
        work[2, middle:right] = 8.0 * (one + two)
        work[3, middle:right] = 8.0 * (one - two)
        work[4, middle:right] = 16.0 * recv[4].T
        pl.when(has_right)(onto_right.start)
        pl.when(has_left)(onto_left.start)

        blank = jnp.zeros((fields, ICE_REACH, LANES), jnp.float32)

        @pl.when(jnp.logical_not(has_left))
        def _():
            work[:, left:middle] = blank

        @pl.when(jnp.logical_not(has_right))
        def _():
            work[:, right : right + ICE_REACH] = blank

        outward_bulk(0, fields, (first_send, first_recv)).wait_send()
        rest = outward_bulk(fields, packed, (second_send, second_recv))
        rest.wait_send()
        pl.semaphore_signal(go, inc=1, device_id={"comp": 1 - comp}, device_id_type=MESH)
        rest.wait_recv()
        whole = slice(LEAD, LEAD + span)
        third = unpack(fields, filled, fields, ICE_REACH)
        stat[0, whole] = 4.0 * third
        stat[5, whole] = 8.0 * third
        push = unpack(fields + 1, filled, fields, ICE_REACH)
        stat[1, whole] = jnp.where(push > 0.0, 1.0 - push, 0.0)
        stat[2, whole] = (0.25 / 8.0) * push
        stat[3, whole] = unpack(fields + 2, filled, fields, ICE_REACH)
        stat[4, whole] = unpack(fields + 3, filled, fields, ICE_REACH)
        pl.when(has_left)(onto_right.wait_recv)
        pl.when(has_right)(onto_left.wait_recv)
        pl.when(has_right)(onto_right.wait_send)
        pl.when(has_left)(onto_left.wait_send)

        for group in range(SUBCYCLES // 4):
            low, high = LEAD + 8 * group, LEAD + span - 8 * group
            inner, outer = LEAD + ICE_REACH, LEAD + ICE_REACH + LANES

            def subcycle(step, carry, low=low, high=high):
                for begin, size in pieces(low, high, 8):
                    tile_stress(work, stat, begin, size)
                for begin, size in pieces(low, inner, 8) + pieces(outer, high, 8):
                    tile_velocity(work, stat, total, begin, size, None)
                for begin, size in pieces(inner, outer, 8):
                    tile_velocity(work, stat, total, begin, size, begin - inner)
                return carry

            lax.fori_loop(0, 4, subcycle, 0)

        own = slice(LEAD + ICE_REACH, LEAD + ICE_REACH + LANES)
        for channel in range(3):
            back[channel] = total[channel].T
        start(totals_home())
        one, two = work[2, own], work[3, own]
        for field, value in enumerate(
            (
                work[0, own],
                work[1, own],
                (0.5 / 8.0) * (one + two),
                (0.5 / 8.0) * (one - two),
                (1.0 / 16.0) * work[4, own],
            )
        ):
            back[3 + field] = value.T
        start(homeward(back.at[3 : 3 + fields], state, (state_send, state_recv)))
        home[:, :, lanes_of(mine)] = back[0:3, rows_of(me), :]
        state[:, :, lanes_of(mine)] = back[3 : 3 + fields, rows_of(me), :]
        share = 1.0 / SUBCYCLES
        def upper_chunk(turn, carry):
            sems = (total_send, total_recv.at[turn])

            @pl.when(turn > 0)
            def _():
                bulk(home.at[:, :, 0:width], sems).wait_recv()

            if members > 1:

                @pl.when(turn == 0)
                def _():
                    bulk(home.at[:, :, 0 : width - LANES], sems).wait_recv()

            span = span_of(turn)
            covered = cover[:, span].astype(jnp.float32)
            for axis in range(2):
                mean[axis, :, span] = home[axis, :, span] * share - covered * current[axis, :, span]
            mean[2, :, span] = forcing[4, :, span] * covered * (home[2, :, span] * share)
            mean_copy(turn).start()
            split_values(mean, turn)
            remap(1, turn)
            return carry

        lax.fori_loop(0, chunks, upper_chunk, 0)
        gather_window(1)
        start(sides[1])
        pair[...] = mean[...]
        lower_half()
        start(sides[0])
        homeward_bulk(0, 3, (total_send, total_recv.at[0])).wait_send()
        states = homeward_bulk(3, 3 + fields, (state_send, state_recv))
        states.wait_recv()
        states.wait_send()
        bulk(mean, (mean_send, mean_recv.at[0])).wait_send()
        bulk(window, (side_send, side_recv.at[0, 0])).wait_send()
    @pl.when(comp == 1)
    def _():
        filled = fields + 2
        packed = filled + -(-filled // (LANES // (2 * SEA_REACH)))
        span = LANES + 2 * SEA_REACH
        for copy in loads:
            copy.wait()
        for axis in range(2):
            pack[fields + axis] = current[axis]
        spread_edges(filled, 0, filled, SEA_REACH)
        for array in (work, spare):
            for edge in (0, LEAD + span):
                array[:, edge : edge + LEAD] = jnp.zeros((array.shape[0], LEAD, LANES), jnp.float32)
        recv[0:packed, rows_of(me), :] = pack[0:packed, :, lanes_of(mine)]
        prepare_remap()
        pl.semaphore_wait(barrier, count)
        pl.semaphore_wait(go, 1)
        start(outward(0, packed, (first_send, first_recv)))
        outward_bulk(0, packed, (first_send, first_recv)).wait_recv()
        whole = slice(LEAD, LEAD + span)
        for field in range(fields):
            work[field, whole] = unpack(field, filled, 0, SEA_REACH)
        lane = lane_index((span, LANES))
        speed = courant * unpack(fields, filled, 0, SEA_REACH)
        drain = jnp.abs(speed)
        stat[0, whole] = jnp.where(lane == 0, 0.0, jnp.maximum(speed, 0.0))
        stat[1, whole] = jnp.where(lane == LANES - 1, 0.0, -jnp.minimum(speed, 0.0))
        speed = courant * unpack(fields + 1, filled, 0, SEA_REACH)
        stat[2, whole] = jnp.maximum(speed, 0.0)
        stat[3, whole] = -jnp.minimum(speed, 0.0)
        stat[4, whole] = drain + jnp.abs(speed)
        for group in range(SUBCYCLES // 8):
            low, high = LEAD + 8 * group, LEAD + span - 8 * group

            def substeps(step, carry, low=low, high=high):
                for begin, size in pieces(low, high, 16):
                    tile_ocean(work, spare, stat, begin, size)
                for begin, size in pieces(low, high, 16):
                    tile_ocean(spare, work, stat, begin, size)
                return carry

            lax.fori_loop(0, 4, substeps, 0)
        own = slice(LEAD + SEA_REACH, LEAD + SEA_REACH + LANES)
        for field in range(fields):
            back[3 + field] = work[field, own].T
        start(homeward(back.at[3 : 3 + fields], state, (state_send, state_recv)))
        state[:, :, lanes_of(mine)] = back[3 : 3 + fields, rows_of(me), :]
        outward_bulk(0, packed, (first_send, first_recv)).wait_send()
        def upper_chunk(turn, carry):
            mean_copy(turn).wait_recv()
            split_values(home, turn)
            remap(1, turn)
            return carry

        lax.fori_loop(0, chunks, upper_chunk, 0)
        gather_window(1)
        for channel in range(channels):
            sides[1][channel].wait_recv()
            window[1, channel] += beside[1, channel]
            onward[channel].start()
        lower_half()
        for channel in range(channels):
            sides[0][channel].wait_recv()
            pair[channel] = window[0, channel] + beside[0, channel]
        states = homeward_bulk(3, 3 + fields, (state_send, state_recv))
        states.wait_recv()
        bulk(before, (next_send, next_recv)).wait_recv()
        pair[...] += before[...]
        state[0] -= dilution * pair[2]
        states.wait_send()
        bulk(before, (next_send, next_recv)).wait_send()

def deliver_kernel(state, pair, out_state, out_pair, sems):
    copies = [
        pltpu.make_async_copy(state, out_state, sems.at[0]),
        pltpu.make_async_copy(pair, out_pair, sems.at[1]),
    ]
    for copy in copies:
        copy.start()
    for copy in copies:
        copy.wait()


def deliver(state, pair):
    return pl.pallas_call(
        deliver_kernel,
        out_shape=(
            jax.ShapeDtypeStruct(state.shape, jnp.float32),
            jax.ShapeDtypeStruct(pair.shape, jnp.float32),
        ),
        in_specs=[pl.BlockSpec(memory_space=pltpu.VMEM)] * 2,
        out_specs=[pl.BlockSpec(memory_space=pl.ANY)] * 2,
        scratch_shapes=[pltpu.SemaphoreType.DMA((2,))],
        compiler_params=pltpu.CompilerParams(vmem_limit_bytes=2 * 1024 * 1024),
        name="deliver",
    )(state, pair)


def run_tiles(initial, forcing, current, cover, targets, weights, count):
    fields, rows, cols = initial.shape
    f32 = jnp.float32
    most = fields + 4
    packed = most + -(-4 // (LANES // (2 * ICE_REACH)))
    tall = LANES + 2 * ICE_REACH + 2 * LEAD
    low_count = 256 if cols % 256 == 0 else 128
    high_count = rows * cols // low_count
    vmem = pl.BlockSpec(memory_space=pltpu.VMEM)
    dma = pltpu.SemaphoreType.DMA
    return pl.pallas_call(
        tiles_kernel,
        out_shape=(pltpu.VMEM((fields, rows, cols), f32), pltpu.VMEM((3, rows, cols), f32)),
        in_specs=[pl.BlockSpec(memory_space=pl.ANY)] * 6,
        out_specs=(vmem, vmem),
        scratch_shapes=[
            pltpu.VMEM((packed, rows, cols), f32),
            pltpu.VMEM(forcing.shape, f32),
            pltpu.VMEM(current.shape, f32),
            pltpu.VMEM(cover.shape, cover.dtype),
            pltpu.VMEM(targets.shape[1:], targets.dtype),
            pltpu.VMEM(weights.shape[1:], weights.dtype),
            pltpu.VMEM((packed, LANES, LANES), f32),
            pltpu.VMEM((fields, tall, LANES), f32),
            pltpu.VMEM((fields, tall, LANES), f32),
            pltpu.VMEM((6, tall, LANES), f32),
            pltpu.VMEM((3, LANES, LANES), f32),
            pltpu.VMEM((3 + fields, LANES, LANES), f32),
            pltpu.VMEM((3, rows, cols), f32),
            pltpu.VMEM((3, rows, cols), f32),
            pltpu.VMEM((2, 6 * high_count, low_count), f32),
            pltpu.VMEM((2, 3, rows, cols), f32),
            pltpu.VMEM((2, 3, rows, cols), f32),
            pltpu.VMEM((3, rows, cols), f32),
            pltpu.VMEM((rows, cols), f32),
            pltpu.VMEM((2, rows, cols), f32),
            pltpu.VMEM((rows * cols, low_count), jnp.bfloat16),
            pltpu.VMEM((6, rows, cols), f32),
            dma((6,)),
            *[dma] * 4,
            dma, dma((cols // low_count,)), dma, dma, dma, dma((cols // low_count,)),
            dma, dma((2, 3)), dma, dma, dma((2,)), dma((2,)),
            pltpu.SemaphoreType.REGULAR,
        ],
        compiler_params=pltpu.CompilerParams(collective_id=0, has_side_effects=True),
        name="tiles",
    )(initial, forcing, current, cover, targets, weights)


def remap_kernel(average, targets, weights, window, acc, low_index, high_index):
    comp = lax.axis_index("comp")
    channels, rows, cols = average.shape
    span = low_index.shape[1]
    low_count, high_count = low_index.shape[0], high_index.shape[0]
    bf16 = jnp.bfloat16
    blocks = cols // low_count
    low_index[...] = lax.broadcasted_iota(jnp.int32, low_index.shape, 0).astype(bf16)
    high_index[...] = lax.broadcasted_iota(jnp.int32, high_index.shape, 0).astype(bf16)
    acc[...] = jnp.zeros_like(acc)

    def one_row(row, carry):
        for piece in range(cols // span):
            place = pl.ds(piece * span, span)
            target = targets[comp, pl.ds(row, 1), place]
            scale = weights[comp, pl.ds(row, 1), place].astype(jnp.float32) * (1.0 / weight_norm)
            low = lax.rem(target, low_count)
            block = lax.rem(lax.div(target, low_count), blocks)
            line = lax.div(target, cols)
            high = (lax.div(line, rows) * blocks + block) * rows + lax.rem(line, rows)
            low_hot = jnp.where(low_index[...] == low.astype(bf16), bf16(1), bf16(0))
            match = high_index[...] == high.astype(bf16)
            parts = []
            for channel in range(channels):
                value = average[channel, pl.ds(row, 1), place] * scale
                coarse = value.astype(bf16)
                fine = (value - coarse.astype(jnp.float32)).astype(bf16)
                parts.append(jnp.where(match, coarse, bf16(0)))
                parts.append(jnp.where(match, fine, bf16(0)))
            spread = jnp.concatenate(parts, axis=0)
            acc[...] += lax.dot_general(
                spread, low_hot, (((1,), (1,)), ((), ())), preferred_element_type=jnp.float32
            )
        return carry

    lax.fori_loop(0, rows, one_row, 0)
    for channel in range(channels):
        for half in range(2):
            for block in range(blocks):
                base = 2 * channel * high_count + (half * blocks + block) * rows
                window[channel, half, :, block * low_count : (block + 1) * low_count] = (
                    acc[base : base + rows] + acc[base + high_count : base + high_count + rows]
                )


def run_remap(average, targets, weights):
    channels, rows, cols = average.shape
    low_count = 256 if cols % 256 == 0 else 128
    high_count = 2 * rows * cols // low_count
    span = min(1024, cols)
    vmem = pl.BlockSpec(memory_space=pltpu.VMEM)
    return pl.pallas_call(
        remap_kernel,
        out_shape=jax.ShapeDtypeStruct((channels, 2, rows, cols), jnp.float32),
        in_specs=[vmem] * 3,
        out_specs=vmem,
        scratch_shapes=[
            pltpu.VMEM((2 * channels * high_count, low_count), jnp.float32),
            pltpu.VMEM((low_count, span), jnp.bfloat16),
            pltpu.VMEM((high_count, span), jnp.bfloat16),
        ],
        compiler_params=pltpu.CompilerParams(vmem_limit_bytes=40 * 1024 * 1024),
        name="remap",
    )(average, targets, weights)


def join_kernel(
    window, state, average, out_state, out_pair, beside, carry, before,
    side_send, side_recv, next_send, next_recv,
):
    me = lax.axis_index("blk")
    comp = lax.axis_index("comp")
    count = lax.axis_size("blk")
    right, left = lax.rem(me + 1, count), lax.rem(me + count - 1, count)
    barrier = pltpu.get_barrier_semaphore()
    pl.semaphore_signal(barrier, inc=1, device_id={"blk": right}, device_id_type=MESH)
    pl.semaphore_signal(barrier, inc=1, device_id={"blk": left}, device_id_type=MESH)
    pl.semaphore_signal(barrier, inc=1, device_id={"comp": 1 - comp}, device_id_type=MESH)
    pl.semaphore_wait(barrier, 3)
    channels = window.shape[0]
    sides, onward = [], []
    for half in (1, 0):
        for channel in range(channels):
            sides.append(
                pltpu.make_async_remote_copy(
                    window.at[channel, half], beside.at[channel, half],
                    side_send.at[half, channel], side_recv.at[half, channel],
                    device_id={"comp": 1 - comp}, device_id_type=MESH,
                )
            )
    for channel in range(channels):
        onward.append(
            pltpu.make_async_remote_copy(
                carry.at[channel], before.at[channel],
                next_send.at[channel], next_recv.at[channel],
                device_id={"blk": right}, device_id_type=MESH,
            )
        )

    @pl.when(comp == 0)
    def _():
        for copy in sides:
            copy.start()
        out_state[...] = state[...]
        out_pair[...] = average[...]
        for copy in sides:
            copy.wait_send()

    @pl.when(comp == 1)
    def _():
        for channel in range(channels):
            sides[channel].wait_recv()
            carry[channel] = window[channel, 1] + beside[channel, 1]
            onward[channel].start()
        for channel in range(channels):
            sides[channels + channel].wait_recv()
            out_pair[channel] = window[channel, 0] + beside[channel, 0]
        out_state[...] = state[...]
        for channel in range(channels):
            onward[channel].wait_recv()
            out_pair[channel] += before[channel]
        out_state[0] -= dilution * out_pair[2]
        for channel in range(channels):
            onward[channel].wait_send()


def run_join(window, state, average):
    channels, rows, cols = average.shape
    vmem = pl.BlockSpec(memory_space=pltpu.VMEM)
    dma = pltpu.SemaphoreType.DMA
    return pl.pallas_call(
        join_kernel,
        out_shape=(
            jax.ShapeDtypeStruct(state.shape, jnp.float32),
            jax.ShapeDtypeStruct(average.shape, jnp.float32),
        ),
        in_specs=[vmem] * 3,
        out_specs=(vmem, vmem),
        scratch_shapes=[
            pltpu.VMEM(window.shape, jnp.float32),
            pltpu.VMEM(average.shape, jnp.float32),
            pltpu.VMEM(average.shape, jnp.float32),
            dma((2, channels)), dma((2, channels)), dma((channels,)), dma((channels,)),
        ],
        compiler_params=pltpu.CompilerParams(
            collective_id=1, has_side_effects=True, vmem_limit_bytes=40 * 1024 * 1024
        ),
        name="join",
    )(window, state, average)


def body(count, initial, ice_forcing, ocean_current, ice_cover, targets, weights):
    if fits_tiles(count, *initial.shape[2:]):
        state, coupled = run_tiles(
            initial[0], ice_forcing, ocean_current, ice_cover, targets, weights, count
        )
        state, coupled = deliver(state, coupled)
    else:
        state, average = run_turns(initial[0], ice_forcing, ocean_current, ice_cover)
        window = run_remap(average, targets, weights)
        state, coupled = run_join(window, state, average)
    return (state[None], coupled[None])


def solution(mesh):
    placed = (
        P("comp", None, "blk", None),
        P(None, "blk", None),
        P(None, "blk", None),
        P("blk", None),
        P(None, "blk", None),
        P(None, "blk", None),
    )
    return jax.shard_map(
        functools.partial(body, mesh.shape["blk"]),
        mesh=mesh,
        in_specs=placed,
        out_specs=(P("comp", None, "blk", None), P("comp", None, "blk", None)),
        check_vma=False,
    )
```

```python
import functools

import jax
import jax.numpy as jnp
from jax import lax
from jax.experimental import pallas as pl
from jax.experimental.pallas import tpu as pltpu
from jax.sharding import PartitionSpec as P

SUBCYCLES = 16
MESH = pl.DeviceIdType.MESH
PAD = 128
PARTS = 2

coriolis = 0.1
inertia = 4.0
courant = 0.2
dilution = 0.5
weight_norm = 4.0
level_speed = (1.0, 0.8, 0.6, 0.45, 0.3)


def rolled(value, steps, axis):
    return pltpu.roll(value, steps % value.shape[axis], axis)


def rows_diff(value):
    return rolled(value, -1, 0) - rolled(value, 1, 0)


def chunk_width(cols):
    return 256 if cols % 256 == 0 else 128


def stress_stage(work, stat, start, width):
    wide = pl.ds(start, width + 2 * PAD)
    mid = pl.ds(start + PAD, width)
    inner = slice(PAD, PAD + width)
    vel_x, vel_y = work[0, :, wide], work[1, :, wide]
    cx = (rolled(vel_x, -1, 1) - rolled(vel_x, 1, 1))[:, inner]
    cy = (rolled(vel_y, -1, 1) - rolled(vel_y, 1, 1))[:, inner]
    rx = rows_diff(vel_x[:, inner])
    ry = rows_diff(vel_y[:, inner])
    e_d = rx + cy
    e_t = rx - cy
    e_s = cx + ry
    inv = lax.rsqrt(0.25 * (e_d * e_d) + 0.0625 * (e_t * e_t + e_s * e_s) + 0.01)
    third = stat[0, :, pl.ds(start, width)]
    scaled = third * inv
    work[2, :, mid] = work[2, :, mid] * (2.0 / 3.0) + (0.5 * scaled * e_d - third)
    work[3, :, mid] = work[3, :, mid] * (2.0 / 3.0) + 0.125 * scaled * e_t
    work[4, :, mid] = work[4, :, mid] * (2.0 / 3.0) + 0.0625 * scaled * e_s


def velocity_stage(work, stat, total, start, width, rows):
    wide = pl.ds(start, width + 2 * PAD)
    mid = pl.ds(start + PAD, width)
    here = pl.ds(start, width)
    inner = slice(PAD, PAD + width)
    shear = work[4, :, wide]
    one, two = work[2, :, wide], work[3, :, wide]
    across_shear = (rolled(shear, -1, 1) - rolled(shear, 1, 1))[:, inner]
    lower = one - two
    across_yy = (rolled(lower, -1, 1) - rolled(lower, 1, 1))[:, inner]
    force_x = rows_diff((one + two)[:, inner]) + 2.0 * across_shear
    force_y = 2.0 * rows_diff(shear[:, inner]) + across_yy
    old_x, old_y = work[0, :, mid], work[1, :, mid]
    keep, push = stat[1, :, here], stat[2, :, here]
    new_x = keep * (old_x + coriolis * old_y) + push * force_x + stat[3, :, here]
    new_y = keep * (old_y - coriolis * old_x) + push * force_y + stat[4, :, here]
    work[0, :, mid] = new_x
    work[1, :, mid] = new_y
    own_x, own_y = new_x[rows : 2 * rows], new_y[rows : 2 * rows]
    total[0, :, here] += own_x
    total[1, :, here] += own_y
    total[2, :, here] += jnp.sqrt(1.0 + own_x * own_x + own_y * own_y)


def ocean_stage(source, target, coef, start, width):
    wide = pl.ds(start, width + 2 * PAD)
    mid = pl.ds(start + PAD, width)
    here = pl.ds(start, width)
    inner = slice(PAD, PAD + width)
    up, down, east, west = (coef[i, :, here] for i in range(4))
    for level, speed in enumerate(level_speed):
        tracer = source[level, :, wide]
        centre = tracer[:, inner]
        right = rolled(tracer, -1, 1)[:, inner] - centre
        left = centre - rolled(tracer, 1, 1)[:, inner]
        above = rolled(centre, -1, 0) - centre
        below = centre - rolled(centre, 1, 0)
        change = up * below + down * above + east * left + west * right
        target[level, :, mid] = centre - speed * change


def turns_kernel(
    initial_in, forcing_in, current_in, cover_in, state, average,
    initial, forcing, current, cover,
    own, own_stat, halo, halo_stat, work, spare, stat, total, mean,
    load, near_send, near_recv, far_send, far_recv,
    stat_near_send, stat_near_recv, stat_far_send, stat_far_recv,
    mean_send, mean_recv, go,
):
    me = lax.axis_index("blk")
    comp = lax.axis_index("comp")
    count = lax.axis_size("blk")
    fields, rows, cols = initial.shape
    width = chunk_width(cols)
    chunks = cols // width
    near = 1 - lax.rem(me, 2)
    far = 1 - near
    partner = me + 2 * near - 1
    relay_to = me + 4 * near - 2
    relay_from = me - 4 * near + 2
    can_send = jnp.logical_and(relay_to >= 0, relay_to < count)
    can_recv = jnp.logical_and(relay_from >= 0, relay_from < count)
    relay_to = lax.rem(relay_to + count, count)
    relay_from = lax.rem(relay_from + count, count)

    barrier = pltpu.get_barrier_semaphore()

    def greet(where):
        pl.semaphore_signal(barrier, inc=1, device_id=where, device_id_type=MESH)

    greet({"blk": partner})
    greet({"comp": 1 - comp})
    pl.when(can_send)(lambda: greet({"blk": relay_to}))
    pl.when(can_recv)(lambda: greet({"blk": relay_from}))
    loads = [
        pltpu.make_async_copy(source, target, load.at[i])
        for i, (source, target) in enumerate(
            (
                (initial_in, initial),
                (current_in, current),
                (forcing_in, forcing),
                (cover_in, cover),
            )
        )
    ]
    for copy in loads:
        copy.start()

    work[...] = jnp.zeros_like(work)
    total[...] = jnp.zeros_like(total)

    def enter():
        pl.semaphore_wait(barrier, 2 + can_send.astype(jnp.int32) + can_recv.astype(jnp.int32))

    def copies(source, target, pieces, near_sems, far_sems):
        first, second = [], []
        wide = cols // PARTS
        for index in range(pieces * PARTS):
            piece, place = index // PARTS, pl.ds(index % PARTS * wide, wide)
            first.append(
                pltpu.make_async_remote_copy(
                    source.at[piece, :, place], target.at[far, piece, :, place],
                    near_sems[0].at[index], near_sems[1].at[index],
                    device_id={"blk": partner}, device_id_type=MESH,
                )
            )
            second.append(
                pltpu.make_async_remote_copy(
                    target.at[near, piece, :, place], target.at[far, piece, :, place],
                    far_sems[0].at[index], far_sems[1].at[index],
                    device_id={"blk": relay_to}, device_id_type=MESH,
                )
            )
        return first, second

    def start(pair):
        for copy in pair[0]:
            copy.start()

    def relay(pair):
        for first, second in zip(*pair):
            first.wait_recv()
            pl.when(can_send)(second.start)

    def arrive(pair):
        @pl.when(can_recv)
        def _():
            for copy in pair[1]:
                copy.wait_recv()

    def sent(pair):
        for copy in pair[0]:
            copy.wait_send()

        @pl.when(can_send)
        def _():
            for copy in pair[1]:
                copy.wait_send()

    def clear_edges(turns):
        @pl.when(jnp.logical_not(can_recv))
        def _():
            halo_stat[far] = jnp.zeros(halo_stat.shape[1:], jnp.float32)
            for turn in range(turns):
                halo[turn, far] = jnp.zeros(halo.shape[2:], jnp.float32)

    inside = slice(PAD, PAD + cols)

    def fill_own(source):
        for field in range(fields):
            work[field, rows : 2 * rows, inside] = source[field]

    def fill_sides(turn):
        for field in range(fields):
            work[field, 0:rows, inside] = halo[turn, 0, field]
            work[field, 2 * rows : 3 * rows, inside] = halo[turn, 1, field]

    def exchange_of(turn, source):
        return copies(
            source, halo.at[turn], fields,
            (near_send.at[turn], near_recv.at[turn]), (far_send.at[turn], far_recv.at[turn]),
        )

    def stats_of(source, pieces):
        return copies(
            source, halo_stat, pieces,
            (stat_near_send, stat_near_recv), (stat_far_send, stat_far_recv),
        )

    mean_copy = pltpu.make_async_remote_copy(
        mean, average, mean_send, mean_recv,
        device_id={"comp": 1 - comp}, device_id_type=MESH,
    )

    @pl.when(comp == 0)
    def _():
        depth = rows // 2
        turns = SUBCYCLES // depth
        clear_edges(turns)
        loads[0].wait()
        enter()
        pairs = [exchange_of(0, initial)]
        start(pairs[0])
        for copy in loads[1:]:
            copy.wait()
        covered = cover[...].astype(jnp.float32)
        push = covered / (inertia * forcing[0] + 1.0)
        own_stat[0] = forcing[1] * covered * (1.0 / 3.0)
        own_stat[1] = push
        own_stat[2] = push * (forcing[2] + current[0])
        own_stat[3] = push * (forcing[3] + current[1])
        stat_pair = stats_of(own_stat, 4)
        start(stat_pair)
        for turn in range(turns):
            source = initial if turn == 0 else own.at[turn - 1]
            if turn > 0:
                pairs.append(exchange_of(turn, source))
                start(pairs[turn])
            relay(pairs[turn])
            if turn == 0:
                relay(stat_pair)
                pl.semaphore_signal(
                    go, inc=1, device_id={"comp": 1 - comp}, device_id_type=MESH
                )
            fill_own(source)
            arrive(pairs[turn])
            if turn == 0:
                arrive(stat_pair)
                for place, block in enumerate((halo_stat.at[0], own_stat, halo_stat.at[1])):
                    span = slice(place * rows, (place + 1) * rows)
                    push = block[1]
                    stat[0, span] = block[0]
                    stat[1, span] = jnp.where(push > 0.0, 1.0 - push, 0.0)
                    stat[2, span] = 0.25 * push
                    stat[3, span] = block[2]
                    stat[4, span] = block[3]
            fill_sides(turn)

            def subcycle(step, carry):
                for chunk in range(chunks):
                    stress_stage(work, stat, chunk * width, width)
                for chunk in range(chunks):
                    velocity_stage(work, stat, total, chunk * width, width, rows)
                return carry

            lax.fori_loop(0, depth, subcycle, 0)
            final = state if turn == turns - 1 else own.at[turn]
            for field in range(fields):
                final[field] = work[field, rows : 2 * rows, inside]
        share = 1.0 / SUBCYCLES
        covered = cover[...].astype(jnp.float32)
        mean[0] = total[0] * share - covered * current[0]
        mean[1] = total[1] * share - covered * current[1]
        mean[2] = forcing[4] * covered * (total[2] * share)
        mean_copy.start()
        average[...] = mean[...]
        sent(stat_pair)
        for pair in pairs:
            sent(pair)
        mean_copy.wait_send()

    @pl.when(comp == 1)
    def _():
        depth = rows
        turns = SUBCYCLES // depth
        clear_edges(turns)
        spare[...] = jnp.zeros_like(spare)
        for copy in loads:
            copy.wait()
        enter()
        pl.semaphore_wait(go, 1)
        pairs = [exchange_of(0, initial)]
        start(pairs[0])
        stat_pair = stats_of(current, 2)
        start(stat_pair)
        for turn in range(turns):
            source = initial if turn == 0 else own.at[turn - 1]
            if turn > 0:
                pairs.append(exchange_of(turn, source))
                start(pairs[turn])
            relay(pairs[turn])
            if turn == 0:
                relay(stat_pair)
            fill_own(source)
            arrive(pairs[turn])
            if turn == 0:
                arrive(stat_pair)
                for place in range(3):
                    span = slice(place * rows, (place + 1) * rows)
                    for axis in range(2):
                        if place == 1:
                            speed = current[axis]
                        else:
                            speed = halo_stat[place // 2, axis]
                        stat[2 * axis, span] = courant * jnp.maximum(speed, 0.0)
                        stat[2 * axis + 1, span] = courant * jnp.minimum(speed, 0.0)
            fill_sides(turn)

            def substeps(step, carry):
                for chunk in range(chunks):
                    ocean_stage(work, spare, stat, chunk * width, width)
                for chunk in range(chunks):
                    ocean_stage(spare, work, stat, chunk * width, width)
                return carry

            lax.fori_loop(0, depth // 2, substeps, 0)
            final = state if turn == turns - 1 else own.at[turn]
            for field in range(fields):
                final[field] = work[field, rows : 2 * rows, inside]
        sent(stat_pair)
        for pair in pairs:
            sent(pair)
        mean_copy.wait_recv()


def run_turns(initial, forcing, current, cover):
    fields, rows, cols = initial.shape
    most = SUBCYCLES // (rows // 2)
    f32 = jnp.float32
    vmem = pl.BlockSpec(memory_space=pltpu.VMEM)
    dma = pltpu.SemaphoreType.DMA
    return pl.pallas_call(
        turns_kernel,
        out_shape=(
            jax.ShapeDtypeStruct((fields, rows, cols), f32),
            jax.ShapeDtypeStruct((3, rows, cols), f32),
        ),
        in_specs=[pl.BlockSpec(memory_space=pl.ANY)] * 4,
        out_specs=(vmem, vmem),
        scratch_shapes=[
            pltpu.VMEM(initial.shape, f32),
            pltpu.VMEM(forcing.shape, f32),
            pltpu.VMEM(current.shape, f32),
            pltpu.VMEM(cover.shape, cover.dtype),
            pltpu.VMEM((most, fields, rows, cols), f32),
            pltpu.VMEM((4, rows, cols), f32),
            pltpu.VMEM((most, 2, fields, rows, cols), f32),
            pltpu.VMEM((2, 4, rows, cols), f32),
            pltpu.VMEM((fields, 3 * rows, cols + 2 * PAD), f32),
            pltpu.VMEM((fields, 3 * rows, cols + 2 * PAD), f32),
            pltpu.VMEM((5, 3 * rows, cols), f32),
            pltpu.VMEM((3, rows, cols), f32),
            pltpu.VMEM((3, rows, cols), f32),
            dma((4,)),
            *[dma((most, fields * PARTS)) for _ in range(4)],
            *[dma((4 * PARTS,)) for _ in range(4)],
            dma, dma, pltpu.SemaphoreType.REGULAR,
        ],
        compiler_params=pltpu.CompilerParams(
            collective_id=0, has_side_effects=True
        ),
        name="turns",
    )(initial, forcing, current, cover)


LANES = 128
LEAD = 8
ICE_REACH = 2 * SUBCYCLES
SEA_REACH = SUBCYCLES


def fits_tiles(count, rows, cols):
    return count * rows == LANES and cols == count * LANES and count > 1


def lane_index(shape):
    return lax.broadcasted_iota(jnp.int32, shape, len(shape) - 1)


def lane_diff(value):
    lane = lane_index(value.shape)
    after = jnp.where(lane == LANES - 1, 0.0, pltpu.roll(value, LANES - 1, 1))
    before = jnp.where(lane == 0, 0.0, pltpu.roll(value, 1, 1))
    return after - before


def tile_stress(work, stat, low, size):
    here, up, down = (pl.ds(low + shift, size) for shift in (0, 1, -1))
    cx = work[0, up] - work[0, down]
    cy = work[1, up] - work[1, down]
    rx, ry = lane_diff(work[0, here]), lane_diff(work[1, here])
    e_d = rx + cy
    e_t = rx - cy
    e_s = cx + ry
    fourfold = 4.0 * e_d
    scaled = stat[0, here] * lax.rsqrt(fourfold * e_d + (e_t * e_t + e_s * e_s) + 0.16)
    rest = stat[5, here]
    work[2, here] = work[2, here] * (2.0 / 3.0) + (scaled * (fourfold + e_t) - rest)
    work[3, here] = work[3, here] * (2.0 / 3.0) + (scaled * (fourfold - e_t) - rest)
    work[4, here] = work[4, here] * (2.0 / 3.0) + scaled * e_s


def tile_velocity(work, stat, total, low, size, own):
    here, up, down = (pl.ds(low + shift, size) for shift in (0, 1, -1))
    force_x = lane_diff(work[2, here]) + (work[4, up] - work[4, down])
    force_y = lane_diff(work[4, here]) + (work[3, up] - work[3, down])
    old_x, old_y = work[0, here], work[1, here]
    keep, push = stat[1, here], stat[2, here]
    new_x = keep * (old_x + coriolis * old_y) + push * force_x + stat[3, here]
    new_y = keep * (old_y - coriolis * old_x) + push * force_y + stat[4, here]
    work[0, here] = new_x
    work[1, here] = new_y
    if own is not None:
        place = pl.ds(own, size)
        total[0, place] += new_x
        total[1, place] += new_y
        square = 1.0 + new_x * new_x + new_y * new_y
        total[2, place] += square * lax.rsqrt(square)


def tile_ocean(source, target, stat, low, size):
    here, up, down = (pl.ds(low + shift, size) for shift in (0, 1, -1))
    before, after, left, right, drain = (stat[i, here] for i in range(5))
    for level, speed in enumerate(level_speed):
        centre = source[level, here]
        inflow = before * pltpu.roll(centre, 1, 1) + after * pltpu.roll(centre, LANES - 1, 1)
        inflow += left * source[level, down] + right * source[level, up]
        target[level, here] = centre + speed * (inflow - drain * centre)


def pieces(low, high, step):
    return [(start, min(step, high - start)) for start in range(low, high, step)]


def tiles_kernel(
    initial_in, forcing_in, current_in, cover_in, targets_in, weights_in, state, pair,
    pack, forcing, current, cover, targets, weights,
    recv, work, spare, stat, total, back, home, mean, acc, window, beside, before,
    low, high, hot, parts,
    load, first_send, first_recv, second_send, second_recv,
    total_send, total_recv, state_send, state_recv, mean_send, mean_recv,
    side_send, side_recv, next_send, next_recv, edge_send, edge_recv, go,
):
    me = lax.axis_index("blk")
    comp = lax.axis_index("comp")
    count = lax.axis_size("blk")
    fields, rows, cols = initial_in.shape
    barrier = pltpu.get_barrier_semaphore()

    def greet(where):
        pl.semaphore_signal(barrier, inc=1, device_id=where, device_id_type=MESH)

    def other(step):
        return lax.bitwise_xor(me, step)

    steps = range(1, count)
    for step in steps:
        greet({"blk": other(step)})
    greet({"comp": 1 - comp})

    loads = [
        pltpu.make_async_copy(source, target, load.at[i])
        for i, (source, target) in enumerate(
            (
                (initial_in, pack.at[0:fields]),
                (current_in, current),
                (forcing_in, forcing),
                (cover_in, cover),
                (targets_in.at[comp], targets),
                (weights_in.at[comp], weights),
            )
        )
    ]
    for copy in loads:
        copy.start()

    turn_size = min(4, count)

    def mirrored(group, place):
        return place + lax.rem(group, 2) * (turn_size - 1 - 2 * place)

    def column_of(device):
        group, place = lax.div(device, turn_size), lax.rem(device, turn_size)
        return group * turn_size + mirrored(group, lax.bitwise_xor(place, lax.div(place, 2)))

    def device_of(column):
        group, place = lax.div(column, turn_size), lax.rem(column, turn_size)
        place = mirrored(group, place)
        return group * turn_size + lax.bitwise_xor(place, lax.div(place, 2))

    mine = column_of(me)

    def lanes_of(block):
        return pl.ds(pl.multiple_of(block * LANES, LANES), LANES)

    def rows_of(block):
        return pl.ds(pl.multiple_of(block * rows, rows), rows)

    def outward(low, high, sems):
        return [
            pltpu.make_async_remote_copy(
                pack.at[low:high, :, lanes_of(column_of(other(step)))],
                recv.at[low:high, rows_of(me), :],
                sems[0], sems[1],
                device_id={"blk": other(step)}, device_id_type=MESH,
            )
            for step in steps
        ]

    width = hot.shape[1]
    members = width // LANES
    chunks = cols // width

    def home_copy(source, target, sems, step):
        return pltpu.make_async_remote_copy(
            source.at[:, rows_of(other(step)), :],
            target.at[:, :, lanes_of(mine)],
            sems[0], sems[1],
            device_id={"blk": other(step)}, device_id_type=MESH,
        )

    def homeward(source, target, sems):
        return [home_copy(source, target, sems, step) for step in steps]

    def totals_home():
        return [
            home_copy(back.at[0:3], home, (total_send, total_recv.at[step // members]), step)
            for step in steps
        ]


    def chunk_of(turn):
        device = members * lax.bitwise_xor(lax.div(me, members), turn)
        return lax.div(column_of(device), members)

    def span_of(turn):
        return pl.ds(pl.multiple_of(chunk_of(turn) * width, width), width)

    def start(copies):
        for copy in copies:
            copy.start()

    def bulk(block, sems):
        return pltpu.make_async_remote_copy(
            block, block, sems[0], sems[1],
            device_id={"comp": 1 - comp}, device_id_type=MESH,
        )

    def outward_bulk(low, high, sems):
        return bulk(recv.at[low:high, 0 : (count - 1) * rows, :], sems)

    def homeward_bulk(low, high, sems):
        return bulk(back.at[low:high, 0 : (count - 1) * rows, :], sems)

    def spread_edges(base, low, filled, reach):
        group = LANES // (2 * reach)
        lane = lane_index((rows, LANES))
        slot = lane // (2 * reach)
        leading = lane % (2 * reach) < reach
        zero = jnp.zeros((rows, LANES), jnp.float32)
        for tile in range(-(-(filled - low) // group)):
            members = range(low + tile * group, min(filled, low + (tile + 1) * group))
            turned = []
            for block in range(count):
                here = slice(block * LANES, (block + 1) * LANES)
                merged = zero
                for place, field in enumerate(members):
                    shift = (2 * place + 1) * reach % LANES
                    value = pack[field, :, here]
                    moved = pltpu.roll(value, shift, 1) if shift else value
                    merged = jnp.where(slot == place, moved, merged)
                turned.append(merged)
            for block in range(count):
                before = turned[block - 1] if block > 0 else zero
                after = turned[block + 1] if block < count - 1 else zero
                here = slice(block * LANES, (block + 1) * LANES)
                pack[base + tile, :, here] = jnp.where(leading, before, after)

    def edges(reach):
        left, middle, right = LEAD, LEAD + reach, LEAD + reach + LANES
        onto_right = pltpu.make_async_remote_copy(
            work.at[:, right - reach : right], work.at[:, left:middle],
            edge_send.at[0], edge_recv.at[0],
            device_id={"blk": device_of(lax.rem(mine + 1, count))}, device_id_type=MESH,
        )
        onto_left = pltpu.make_async_remote_copy(
            work.at[:, middle : middle + reach], work.at[:, right : right + reach],
            edge_send.at[1], edge_recv.at[1],
            device_id={"blk": device_of(lax.rem(mine + count - 1, count))}, device_id_type=MESH,
        )
        has_left, has_right = mine > 0, mine < count - 1
        blank = jnp.zeros((fields, reach, LANES), jnp.float32)

        def swap():
            pl.when(has_right)(onto_right.start)
            pl.when(has_left)(onto_left.start)

            @pl.when(jnp.logical_not(has_left))
            def _():
                work[:, left:middle] = blank

            @pl.when(jnp.logical_not(has_right))
            def _():
                work[:, right : right + reach] = blank

        def arrived():
            pl.when(has_left)(onto_right.wait_recv)
            pl.when(has_right)(onto_left.wait_recv)
            pl.when(has_right)(onto_right.wait_send)
            pl.when(has_left)(onto_left.wait_send)

        return swap, arrived

    def unpack(field, base, low, reach):
        group = LANES // (2 * reach)
        value = recv[field].T
        edge = recv[base + (field - low) // group].T
        start = (field - low) % group * 2 * reach
        return jnp.concatenate(
            [edge[start : start + reach], value, edge[start + reach : start + 2 * reach]], axis=0
        )

    channels = pair.shape[0]

    def mean_copy(turn):
        return pltpu.make_async_remote_copy(
            mean.at[:, :, span_of(turn)], home.at[:, :, span_of(turn)],
            mean_send, mean_recv.at[turn],
            device_id={"comp": 1 - comp}, device_id_type=MESH,
        )
    sides = [
        [
            pltpu.make_async_remote_copy(
                window.at[half, channel], beside.at[half, channel],
                side_send, side_recv.at[half, channel],
                device_id={"comp": 1 - comp}, device_id_type=MESH,
            )
            for channel in range(channels)
        ]
        for half in range(2)
    ]
    onward = [
        pltpu.make_async_remote_copy(
            window.at[1, channel], before.at[channel],
            next_send, next_recv,
            device_id={"blk": lax.rem(me + 1, count)}, device_id_type=MESH,
        )
        for channel in range(channels)
    ]

    def prepare_remap():
        target = targets[...]
        block = lax.rem(lax.div(target, width), chunks)
        line = lax.div(target, cols)
        low[...] = lax.rem(target, width).astype(jnp.float32)
        for half in range(2):
            inside = lax.div(line, rows) == half
            place = block * rows + line - half * rows
            high[half] = jnp.where(inside, place, chunks * rows).astype(jnp.float32)
        acc[...] = jnp.zeros_like(acc)

        def one_row(row, carry):
            lane = lane_index((LANES, LANES)).astype(jnp.float32)
            line = low[pl.ds(row, 1), :]
            for start in range(0, cols, LANES):
                value = jnp.broadcast_to(line[:, start : start + LANES], (LANES, LANES)).T
                base = start // width * rows * width + start % width
                place = pl.ds(pl.multiple_of(base + row * width, LANES), LANES)
                for first in range(0, width, LANES):
                    hit = jnp.where(value == lane + float(first), 1.0, 0.0)
                    hot[place, first : first + LANES] = hit.astype(hot.dtype)
            return carry

        lax.fori_loop(0, rows, one_row, 0)

    def split_values(values, turn):
        span = span_of(turn)
        scale = weights[:, span].astype(jnp.float32) * (1.0 / weight_norm)
        for channel in range(channels):
            value = values[channel, :, span] * scale
            coarse = value.astype(jnp.bfloat16).astype(jnp.float32)
            parts[2 * channel, :, span] = coarse
            parts[2 * channel + 1, :, span] = value - coarse

    def remap(half, turn):
        bf16 = jnp.bfloat16
        tall = 16
        span = span_of(turn)
        index = lax.broadcasted_iota(jnp.int32, (tall, width), 0).astype(bf16)

        def lines(block):
            return [
                jnp.broadcast_to(block[row : row + 1], (tall, width)).astype(bf16)
                for row in range(rows)
            ]

        levels = lines(high[half, :, span])
        matches = [
            [level == index + bf16(first) for level in levels]
            for first in range(0, chunks * rows, tall)
        ]
        spread = []
        for part in range(2 * channels):
            values = lines(parts[part, :, span])
            for match in matches:
                kept = [jnp.where(m, v, bf16(0)) for m, v in zip(match, values)]
                spread.append(jnp.concatenate(kept, axis=1))
        depth = rows * width
        place = pl.ds(pl.multiple_of(chunk_of(turn) * depth, depth), depth)
        acc[half] += jnp.dot(
            jnp.concatenate(spread, axis=0), hot[place, :], preferred_element_type=jnp.float32
        )

    def gather_window(half):
        tall = chunks * rows
        for channel in range(channels):
            for block in range(chunks):
                base = 2 * channel * tall + block * rows
                window[half, channel, :, block * width : (block + 1) * width] = (
                    acc[half, base : base + rows] + acc[half, base + tall : base + tall + rows]
                )

    def lower_half():
        def one_chunk(turn, carry):
            remap(0, turn)
            return carry

        lax.fori_loop(0, chunks, one_chunk, 0, unroll=4)
        gather_window(0)

    @pl.when(comp == 0)
    def _():
        filled = fields + 4
        packed = filled + -(-4 // (LANES // (2 * ICE_REACH)))
        span = LANES + 2 * ICE_REACH
        loads[0].wait()
        pl.semaphore_wait(barrier, count)
        start(outward(0, fields, (first_send, first_recv)))
        for copy in loads[1:4]:
            copy.wait()
        covered = cover[...].astype(jnp.float32)
        push = covered / (inertia * forcing[0] + 1.0)
        pack[fields] = forcing[1] * covered * (1.0 / 3.0)
        pack[fields + 1] = push
        pack[fields + 2] = push * (forcing[2] + current[0])
        pack[fields + 3] = push * (forcing[3] + current[1])
        spread_edges(filled, fields, filled, ICE_REACH)
        start(outward(fields, packed, (second_send, second_recv)))
        recv[0:packed, rows_of(me), :] = pack[0:packed, :, lanes_of(mine)]
        total[...] = jnp.zeros_like(total)
        for array in (work, stat):
            for edge in (0, LEAD + span):
                array[:, edge : edge + LEAD] = jnp.zeros((array.shape[0], LEAD, LANES), jnp.float32)
        for copy in loads[4:]:
            copy.wait()
        prepare_remap()
        swap_edges, edges_here = edges(ICE_REACH)
        middle, right = LEAD + ICE_REACH, LEAD + ICE_REACH + LANES
        outward_bulk(0, fields, (first_send, first_recv)).wait_recv()
        work[0, middle:right] = recv[0].T
        work[1, middle:right] = recv[1].T
        one, two = recv[2].T, recv[3].T
        work[2, middle:right] = 8.0 * (one + two)
        work[3, middle:right] = 8.0 * (one - two)
        work[4, middle:right] = 16.0 * recv[4].T
        swap_edges()
        outward_bulk(0, fields, (first_send, first_recv)).wait_send()
        rest = outward_bulk(fields, packed, (second_send, second_recv))
        rest.wait_send()
        pl.semaphore_signal(go, inc=1, device_id={"comp": 1 - comp}, device_id_type=MESH)
        rest.wait_recv()
        whole = slice(LEAD, LEAD + span)
        third = unpack(fields, filled, fields, ICE_REACH)
        stat[0, whole] = 4.0 * third
        stat[5, whole] = 8.0 * third
        push = unpack(fields + 1, filled, fields, ICE_REACH)
        stat[1, whole] = jnp.where(push > 0.0, 1.0 - push, 0.0)
        stat[2, whole] = (0.25 / 8.0) * push
        stat[3, whole] = unpack(fields + 2, filled, fields, ICE_REACH)
        stat[4, whole] = unpack(fields + 3, filled, fields, ICE_REACH)
        edges_here()

        for group in range(SUBCYCLES // 4):
            low, high = LEAD + 8 * group, LEAD + span - 8 * group
            inner, outer = LEAD + ICE_REACH, LEAD + ICE_REACH + LANES

            def subcycle(step, carry, low=low, high=high):
                for begin, size in pieces(low, high, 8):
                    tile_stress(work, stat, begin, size)
                for begin, size in pieces(low, inner, 8) + pieces(outer, high, 8):
                    tile_velocity(work, stat, total, begin, size, None)
                for begin, size in pieces(inner, outer, 8):
                    tile_velocity(work, stat, total, begin, size, begin - inner)
                return carry

            lax.fori_loop(0, 4, subcycle, 0)

        own = slice(LEAD + ICE_REACH, LEAD + ICE_REACH + LANES)
        for channel in range(3):
            back[channel] = total[channel].T
        start(totals_home())
        one, two = work[2, own], work[3, own]
        for field, value in enumerate(
            (
                work[0, own],
                work[1, own],
                (0.5 / 8.0) * (one + two),
                (0.5 / 8.0) * (one - two),
                (1.0 / 16.0) * work[4, own],
            )
        ):
            back[3 + field] = value.T
        start(homeward(back.at[3 : 3 + fields], state, (state_send, state_recv)))
        home[:, :, lanes_of(mine)] = back[0:3, rows_of(me), :]
        state[:, :, lanes_of(mine)] = back[3 : 3 + fields, rows_of(me), :]
        share = 1.0 / SUBCYCLES
        def upper_chunk(turn, carry):
            sems = (total_send, total_recv.at[turn])

            @pl.when(turn > 0)
            def _():
                bulk(home.at[:, :, 0:width], sems).wait_recv()

            if members > 1:

                @pl.when(turn == 0)
                def _():
                    bulk(home.at[:, :, 0 : width - LANES], sems).wait_recv()

            span = span_of(turn)
            covered = cover[:, span].astype(jnp.float32)
            for axis in range(2):
                mean[axis, :, span] = home[axis, :, span] * share - covered * current[axis, :, span]
            mean[2, :, span] = forcing[4, :, span] * covered * (home[2, :, span] * share)
            mean_copy(turn).start()
            split_values(mean, turn)
            remap(1, turn)
            return carry

        lax.fori_loop(0, chunks, upper_chunk, 0)
        gather_window(1)
        start(sides[1])
        pair[...] = mean[...]
        lower_half()
        start(sides[0])
        homeward_bulk(0, 3, (total_send, total_recv.at[0])).wait_send()
        states = homeward_bulk(3, 3 + fields, (state_send, state_recv))
        states.wait_recv()
        states.wait_send()
        bulk(mean, (mean_send, mean_recv.at[0])).wait_send()
        bulk(window, (side_send, side_recv.at[0, 0])).wait_send()
    @pl.when(comp == 1)
    def _():
        filled = fields + 2
        packed = filled + -(-2 // (LANES // (2 * SEA_REACH)))
        span = LANES + 2 * SEA_REACH
        for copy in loads:
            copy.wait()
        for axis in range(2):
            pack[fields + axis] = current[axis]
        spread_edges(filled, fields, filled, SEA_REACH)
        for array in (work, spare):
            for edge in (0, LEAD + span):
                array[:, edge : edge + LEAD] = jnp.zeros((array.shape[0], LEAD, LANES), jnp.float32)
        recv[0:packed, rows_of(me), :] = pack[0:packed, :, lanes_of(mine)]
        prepare_remap()
        pl.semaphore_wait(barrier, count)
        pl.semaphore_wait(go, 1)
        start(outward(0, fields, (first_send, first_recv)))
        start(outward(fields, packed, (second_send, second_recv)))
        swap_edges, edges_here = edges(SEA_REACH)
        middle, right = LEAD + SEA_REACH, LEAD + SEA_REACH + LANES
        outward_bulk(0, fields, (first_send, first_recv)).wait_recv()
        for field in range(fields):
            work[field, middle:right] = recv[field].T
        swap_edges()
        rest = outward_bulk(fields, packed, (second_send, second_recv))
        rest.wait_recv()
        whole = slice(LEAD, LEAD + span)
        lane = lane_index((span, LANES))
        speed = courant * unpack(fields, filled, fields, SEA_REACH)
        drain = jnp.abs(speed)
        stat[0, whole] = jnp.where(lane == 0, 0.0, jnp.maximum(speed, 0.0))
        stat[1, whole] = jnp.where(lane == LANES - 1, 0.0, -jnp.minimum(speed, 0.0))
        speed = courant * unpack(fields + 1, filled, fields, SEA_REACH)
        stat[2, whole] = jnp.maximum(speed, 0.0)
        stat[3, whole] = -jnp.minimum(speed, 0.0)
        stat[4, whole] = drain + jnp.abs(speed)
        edges_here()
        for group in range(SUBCYCLES // 8):
            low, high = LEAD + 8 * group, LEAD + span - 8 * group

            def substeps(step, carry, low=low, high=high):
                for begin, size in pieces(low, high, 16):
                    tile_ocean(work, spare, stat, begin, size)
                for begin, size in pieces(low, high, 16):
                    tile_ocean(spare, work, stat, begin, size)
                return carry

            lax.fori_loop(0, 4, substeps, 0)
        own = slice(LEAD + SEA_REACH, LEAD + SEA_REACH + LANES)
        for field in range(fields):
            back[3 + field] = work[field, own].T
        start(homeward(back.at[3 : 3 + fields], state, (state_send, state_recv)))
        state[:, :, lanes_of(mine)] = back[3 : 3 + fields, rows_of(me), :]
        outward_bulk(0, fields, (first_send, first_recv)).wait_send()
        rest.wait_send()
        def upper_chunk(turn, carry):
            mean_copy(turn).wait_recv()
            split_values(home, turn)
            remap(1, turn)
            return carry

        lax.fori_loop(0, chunks, upper_chunk, 0)
        gather_window(1)
        for channel in range(channels):
            sides[1][channel].wait_recv()
            window[1, channel] += beside[1, channel]
            onward[channel].start()
        lower_half()
        for channel in range(channels):
            sides[0][channel].wait_recv()
            pair[channel] = window[0, channel] + beside[0, channel]
        states = homeward_bulk(3, 3 + fields, (state_send, state_recv))
        states.wait_recv()
        bulk(before, (next_send, next_recv)).wait_recv()
        pair[...] += before[...]
        state[0] -= dilution * pair[2]
        states.wait_send()
        bulk(before, (next_send, next_recv)).wait_send()

def deliver_kernel(state, pair, out_state, out_pair, sems):
    copies = [
        pltpu.make_async_copy(state, out_state, sems.at[0]),
        pltpu.make_async_copy(pair, out_pair, sems.at[1]),
    ]
    for copy in copies:
        copy.start()
    for copy in copies:
        copy.wait()


def deliver(state, pair):
    return pl.pallas_call(
        deliver_kernel,
        out_shape=(
            jax.ShapeDtypeStruct(state.shape, jnp.float32),
            jax.ShapeDtypeStruct(pair.shape, jnp.float32),
        ),
        in_specs=[pl.BlockSpec(memory_space=pltpu.VMEM)] * 2,
        out_specs=[pl.BlockSpec(memory_space=pl.ANY)] * 2,
        scratch_shapes=[pltpu.SemaphoreType.DMA((2,))],
        compiler_params=pltpu.CompilerParams(vmem_limit_bytes=2 * 1024 * 1024),
        name="deliver",
    )(state, pair)


def run_tiles(initial, forcing, current, cover, targets, weights, count):
    fields, rows, cols = initial.shape
    f32 = jnp.float32
    most = fields + 4
    packed = most + -(-4 // (LANES // (2 * ICE_REACH)))
    tall = LANES + 2 * ICE_REACH + 2 * LEAD
    low_count = 256 if cols % 256 == 0 else 128
    high_count = rows * cols // low_count
    vmem = pl.BlockSpec(memory_space=pltpu.VMEM)
    dma = pltpu.SemaphoreType.DMA
    return pl.pallas_call(
        tiles_kernel,
        out_shape=(pltpu.VMEM((fields, rows, cols), f32), pltpu.VMEM((3, rows, cols), f32)),
        in_specs=[pl.BlockSpec(memory_space=pl.ANY)] * 6,
        out_specs=(vmem, vmem),
        scratch_shapes=[
            pltpu.VMEM((packed, rows, cols), f32),
            pltpu.VMEM(forcing.shape, f32),
            pltpu.VMEM(current.shape, f32),
            pltpu.VMEM(cover.shape, cover.dtype),
            pltpu.VMEM(targets.shape[1:], targets.dtype),
            pltpu.VMEM(weights.shape[1:], weights.dtype),
            pltpu.VMEM((packed, LANES, LANES), f32),
            pltpu.VMEM((fields, tall, LANES), f32),
            pltpu.VMEM((fields, tall, LANES), f32),
            pltpu.VMEM((6, tall, LANES), f32),
            pltpu.VMEM((3, LANES, LANES), f32),
            pltpu.VMEM((3 + fields, LANES, LANES), f32),
            pltpu.VMEM((3, rows, cols), f32),
            pltpu.VMEM((3, rows, cols), f32),
            pltpu.VMEM((2, 6 * high_count, low_count), f32),
            pltpu.VMEM((2, 3, rows, cols), f32),
            pltpu.VMEM((2, 3, rows, cols), f32),
            pltpu.VMEM((3, rows, cols), f32),
            pltpu.VMEM((rows, cols), f32),
            pltpu.VMEM((2, rows, cols), f32),
            pltpu.VMEM((rows * cols, low_count), jnp.bfloat16),
            pltpu.VMEM((6, rows, cols), f32),
            dma((6,)),
            *[dma] * 4,
            dma, dma((cols // low_count,)), dma, dma, dma, dma((cols // low_count,)),
            dma, dma((2, 3)), dma, dma, dma((2,)), dma((2,)),
            pltpu.SemaphoreType.REGULAR,
        ],
        compiler_params=pltpu.CompilerParams(collective_id=0, has_side_effects=True),
        name="tiles",
    )(initial, forcing, current, cover, targets, weights)


def remap_kernel(average, targets, weights, window, acc, low_index, high_index):
    comp = lax.axis_index("comp")
    channels, rows, cols = average.shape
    span = low_index.shape[1]
    low_count, high_count = low_index.shape[0], high_index.shape[0]
    bf16 = jnp.bfloat16
    blocks = cols // low_count
    low_index[...] = lax.broadcasted_iota(jnp.int32, low_index.shape, 0).astype(bf16)
    high_index[...] = lax.broadcasted_iota(jnp.int32, high_index.shape, 0).astype(bf16)
    acc[...] = jnp.zeros_like(acc)

    def one_row(row, carry):
        for piece in range(cols // span):
            place = pl.ds(piece * span, span)
            target = targets[comp, pl.ds(row, 1), place]
            scale = weights[comp, pl.ds(row, 1), place].astype(jnp.float32) * (1.0 / weight_norm)
            low = lax.rem(target, low_count)
            block = lax.rem(lax.div(target, low_count), blocks)
            line = lax.div(target, cols)
            high = (lax.div(line, rows) * blocks + block) * rows + lax.rem(line, rows)
            low_hot = jnp.where(low_index[...] == low.astype(bf16), bf16(1), bf16(0))
            match = high_index[...] == high.astype(bf16)
            parts = []
            for channel in range(channels):
                value = average[channel, pl.ds(row, 1), place] * scale
                coarse = value.astype(bf16)
                fine = (value - coarse.astype(jnp.float32)).astype(bf16)
                parts.append(jnp.where(match, coarse, bf16(0)))
                parts.append(jnp.where(match, fine, bf16(0)))
            spread = jnp.concatenate(parts, axis=0)
            acc[...] += lax.dot_general(
                spread, low_hot, (((1,), (1,)), ((), ())), preferred_element_type=jnp.float32
            )
        return carry

    lax.fori_loop(0, rows, one_row, 0)
    for channel in range(channels):
        for half in range(2):
            for block in range(blocks):
                base = 2 * channel * high_count + (half * blocks + block) * rows
                window[channel, half, :, block * low_count : (block + 1) * low_count] = (
                    acc[base : base + rows] + acc[base + high_count : base + high_count + rows]
                )


def run_remap(average, targets, weights):
    channels, rows, cols = average.shape
    low_count = 256 if cols % 256 == 0 else 128
    high_count = 2 * rows * cols // low_count
    span = min(1024, cols)
    vmem = pl.BlockSpec(memory_space=pltpu.VMEM)
    return pl.pallas_call(
        remap_kernel,
        out_shape=jax.ShapeDtypeStruct((channels, 2, rows, cols), jnp.float32),
        in_specs=[vmem] * 3,
        out_specs=vmem,
        scratch_shapes=[
            pltpu.VMEM((2 * channels * high_count, low_count), jnp.float32),
            pltpu.VMEM((low_count, span), jnp.bfloat16),
            pltpu.VMEM((high_count, span), jnp.bfloat16),
        ],
        compiler_params=pltpu.CompilerParams(vmem_limit_bytes=40 * 1024 * 1024),
        name="remap",
    )(average, targets, weights)


def join_kernel(
    window, state, average, out_state, out_pair, beside, carry, before,
    side_send, side_recv, next_send, next_recv,
):
    me = lax.axis_index("blk")
    comp = lax.axis_index("comp")
    count = lax.axis_size("blk")
    right, left = lax.rem(me + 1, count), lax.rem(me + count - 1, count)
    barrier = pltpu.get_barrier_semaphore()
    pl.semaphore_signal(barrier, inc=1, device_id={"blk": right}, device_id_type=MESH)
    pl.semaphore_signal(barrier, inc=1, device_id={"blk": left}, device_id_type=MESH)
    pl.semaphore_signal(barrier, inc=1, device_id={"comp": 1 - comp}, device_id_type=MESH)
    pl.semaphore_wait(barrier, 3)
    channels = window.shape[0]
    sides, onward = [], []
    for half in (1, 0):
        for channel in range(channels):
            sides.append(
                pltpu.make_async_remote_copy(
                    window.at[channel, half], beside.at[channel, half],
                    side_send.at[half, channel], side_recv.at[half, channel],
                    device_id={"comp": 1 - comp}, device_id_type=MESH,
                )
            )
    for channel in range(channels):
        onward.append(
            pltpu.make_async_remote_copy(
                carry.at[channel], before.at[channel],
                next_send.at[channel], next_recv.at[channel],
                device_id={"blk": right}, device_id_type=MESH,
            )
        )

    @pl.when(comp == 0)
    def _():
        for copy in sides:
            copy.start()
        out_state[...] = state[...]
        out_pair[...] = average[...]
        for copy in sides:
            copy.wait_send()

    @pl.when(comp == 1)
    def _():
        for channel in range(channels):
            sides[channel].wait_recv()
            carry[channel] = window[channel, 1] + beside[channel, 1]
            onward[channel].start()
        for channel in range(channels):
            sides[channels + channel].wait_recv()
            out_pair[channel] = window[channel, 0] + beside[channel, 0]
        out_state[...] = state[...]
        for channel in range(channels):
            onward[channel].wait_recv()
            out_pair[channel] += before[channel]
        out_state[0] -= dilution * out_pair[2]
        for channel in range(channels):
            onward[channel].wait_send()


def run_join(window, state, average):
    channels, rows, cols = average.shape
    vmem = pl.BlockSpec(memory_space=pltpu.VMEM)
    dma = pltpu.SemaphoreType.DMA
    return pl.pallas_call(
        join_kernel,
        out_shape=(
            jax.ShapeDtypeStruct(state.shape, jnp.float32),
            jax.ShapeDtypeStruct(average.shape, jnp.float32),
        ),
        in_specs=[vmem] * 3,
        out_specs=(vmem, vmem),
        scratch_shapes=[
            pltpu.VMEM(window.shape, jnp.float32),
            pltpu.VMEM(average.shape, jnp.float32),
            pltpu.VMEM(average.shape, jnp.float32),
            dma((2, channels)), dma((2, channels)), dma((channels,)), dma((channels,)),
        ],
        compiler_params=pltpu.CompilerParams(
            collective_id=1, has_side_effects=True, vmem_limit_bytes=40 * 1024 * 1024
        ),
        name="join",
    )(window, state, average)


def body(count, initial, ice_forcing, ocean_current, ice_cover, targets, weights):
    if fits_tiles(count, *initial.shape[2:]):
        state, coupled = run_tiles(
            initial[0], ice_forcing, ocean_current, ice_cover, targets, weights, count
        )
        state, coupled = deliver(state, coupled)
    else:
        state, average = run_turns(initial[0], ice_forcing, ocean_current, ice_cover)
        window = run_remap(average, targets, weights)
        state, coupled = run_join(window, state, average)
    return (state[None], coupled[None])


def solution(mesh):
    placed = (
        P("comp", None, "blk", None),
        P(None, "blk", None),
        P(None, "blk", None),
        P("blk", None),
        P(None, "blk", None),
        P(None, "blk", None),
    )
    return jax.shard_map(
        functools.partial(body, mesh.shape["blk"]),
        mesh=mesh,
        in_specs=placed,
        out_specs=(P("comp", None, "blk", None), P("comp", None, "blk", None)),
        check_vma=False,
    )
```

```python
import functools

import jax
import jax.numpy as jnp
from jax import lax
from jax.experimental import pallas as pl
from jax.experimental.pallas import tpu as pltpu
from jax.sharding import PartitionSpec as P

SUBCYCLES = 16
MESH = pl.DeviceIdType.MESH
PAD = 128
PARTS = 2

coriolis = 0.1
inertia = 4.0
courant = 0.2
dilution = 0.5
weight_norm = 4.0
level_speed = (1.0, 0.8, 0.6, 0.45, 0.3)


def rolled(value, steps, axis):
    return pltpu.roll(value, steps % value.shape[axis], axis)


def rows_diff(value):
    return rolled(value, -1, 0) - rolled(value, 1, 0)


def chunk_width(cols):
    return 256 if cols % 256 == 0 else 128


def stress_stage(work, stat, start, width):
    wide = pl.ds(start, width + 2 * PAD)
    mid = pl.ds(start + PAD, width)
    inner = slice(PAD, PAD + width)
    vel_x, vel_y = work[0, :, wide], work[1, :, wide]
    cx = (rolled(vel_x, -1, 1) - rolled(vel_x, 1, 1))[:, inner]
    cy = (rolled(vel_y, -1, 1) - rolled(vel_y, 1, 1))[:, inner]
    rx = rows_diff(vel_x[:, inner])
    ry = rows_diff(vel_y[:, inner])
    e_d = rx + cy
    e_t = rx - cy
    e_s = cx + ry
    inv = lax.rsqrt(0.25 * (e_d * e_d) + 0.0625 * (e_t * e_t + e_s * e_s) + 0.01)
    third = stat[0, :, pl.ds(start, width)]
    scaled = third * inv
    work[2, :, mid] = work[2, :, mid] * (2.0 / 3.0) + (0.5 * scaled * e_d - third)
    work[3, :, mid] = work[3, :, mid] * (2.0 / 3.0) + 0.125 * scaled * e_t
    work[4, :, mid] = work[4, :, mid] * (2.0 / 3.0) + 0.0625 * scaled * e_s


def velocity_stage(work, stat, total, start, width, rows):
    wide = pl.ds(start, width + 2 * PAD)
    mid = pl.ds(start + PAD, width)
    here = pl.ds(start, width)
    inner = slice(PAD, PAD + width)
    shear = work[4, :, wide]
    one, two = work[2, :, wide], work[3, :, wide]
    across_shear = (rolled(shear, -1, 1) - rolled(shear, 1, 1))[:, inner]
    lower = one - two
    across_yy = (rolled(lower, -1, 1) - rolled(lower, 1, 1))[:, inner]
    force_x = rows_diff((one + two)[:, inner]) + 2.0 * across_shear
    force_y = 2.0 * rows_diff(shear[:, inner]) + across_yy
    old_x, old_y = work[0, :, mid], work[1, :, mid]
    keep, push = stat[1, :, here], stat[2, :, here]
    new_x = keep * (old_x + coriolis * old_y) + push * force_x + stat[3, :, here]
    new_y = keep * (old_y - coriolis * old_x) + push * force_y + stat[4, :, here]
    work[0, :, mid] = new_x
    work[1, :, mid] = new_y
    own_x, own_y = new_x[rows : 2 * rows], new_y[rows : 2 * rows]
    total[0, :, here] += own_x
    total[1, :, here] += own_y
    total[2, :, here] += jnp.sqrt(1.0 + own_x * own_x + own_y * own_y)


def ocean_stage(source, target, coef, start, width):
    wide = pl.ds(start, width + 2 * PAD)
    mid = pl.ds(start + PAD, width)
    here = pl.ds(start, width)
    inner = slice(PAD, PAD + width)
    up, down, east, west = (coef[i, :, here] for i in range(4))
    for level, speed in enumerate(level_speed):
        tracer = source[level, :, wide]
        centre = tracer[:, inner]
        right = rolled(tracer, -1, 1)[:, inner] - centre
        left = centre - rolled(tracer, 1, 1)[:, inner]
        above = rolled(centre, -1, 0) - centre
        below = centre - rolled(centre, 1, 0)
        change = up * below + down * above + east * left + west * right
        target[level, :, mid] = centre - speed * change


def turns_kernel(
    initial_in, forcing_in, current_in, cover_in, state, average,
    initial, forcing, current, cover,
    own, own_stat, halo, halo_stat, work, spare, stat, total, mean,
    load, near_send, near_recv, far_send, far_recv,
    stat_near_send, stat_near_recv, stat_far_send, stat_far_recv,
    mean_send, mean_recv, go,
):
    me = lax.axis_index("blk")
    comp = lax.axis_index("comp")
    count = lax.axis_size("blk")
    fields, rows, cols = initial.shape
    width = chunk_width(cols)
    chunks = cols // width
    near = 1 - lax.rem(me, 2)
    far = 1 - near
    partner = me + 2 * near - 1
    relay_to = me + 4 * near - 2
    relay_from = me - 4 * near + 2
    can_send = jnp.logical_and(relay_to >= 0, relay_to < count)
    can_recv = jnp.logical_and(relay_from >= 0, relay_from < count)
    relay_to = lax.rem(relay_to + count, count)
    relay_from = lax.rem(relay_from + count, count)

    barrier = pltpu.get_barrier_semaphore()

    def greet(where):
        pl.semaphore_signal(barrier, inc=1, device_id=where, device_id_type=MESH)

    greet({"blk": partner})
    greet({"comp": 1 - comp})
    pl.when(can_send)(lambda: greet({"blk": relay_to}))
    pl.when(can_recv)(lambda: greet({"blk": relay_from}))
    loads = [
        pltpu.make_async_copy(source, target, load.at[i])
        for i, (source, target) in enumerate(
            (
                (initial_in, initial),
                (current_in, current),
                (forcing_in, forcing),
                (cover_in, cover),
            )
        )
    ]
    for copy in loads:
        copy.start()

    work[...] = jnp.zeros_like(work)
    total[...] = jnp.zeros_like(total)

    def enter():
        pl.semaphore_wait(barrier, 2 + can_send.astype(jnp.int32) + can_recv.astype(jnp.int32))

    def copies(source, target, pieces, near_sems, far_sems):
        first, second = [], []
        wide = cols // PARTS
        for index in range(pieces * PARTS):
            piece, place = index // PARTS, pl.ds(index % PARTS * wide, wide)
            first.append(
                pltpu.make_async_remote_copy(
                    source.at[piece, :, place], target.at[far, piece, :, place],
                    near_sems[0].at[index], near_sems[1].at[index],
                    device_id={"blk": partner}, device_id_type=MESH,
                )
            )
            second.append(
                pltpu.make_async_remote_copy(
                    target.at[near, piece, :, place], target.at[far, piece, :, place],
                    far_sems[0].at[index], far_sems[1].at[index],
                    device_id={"blk": relay_to}, device_id_type=MESH,
                )
            )
        return first, second

    def start(pair):
        for copy in pair[0]:
            copy.start()

    def relay(pair):
        for first, second in zip(*pair):
            first.wait_recv()
            pl.when(can_send)(second.start)

    def arrive(pair):
        @pl.when(can_recv)
        def _():
            for copy in pair[1]:
                copy.wait_recv()

    def sent(pair):
        for copy in pair[0]:
            copy.wait_send()

        @pl.when(can_send)
        def _():
            for copy in pair[1]:
                copy.wait_send()

    def clear_edges(turns):
        @pl.when(jnp.logical_not(can_recv))
        def _():
            halo_stat[far] = jnp.zeros(halo_stat.shape[1:], jnp.float32)
            for turn in range(turns):
                halo[turn, far] = jnp.zeros(halo.shape[2:], jnp.float32)

    inside = slice(PAD, PAD + cols)

    def fill_own(source):
        for field in range(fields):
            work[field, rows : 2 * rows, inside] = source[field]

    def fill_sides(turn):
        for field in range(fields):
            work[field, 0:rows, inside] = halo[turn, 0, field]
            work[field, 2 * rows : 3 * rows, inside] = halo[turn, 1, field]

    def exchange_of(turn, source):
        return copies(
            source, halo.at[turn], fields,
            (near_send.at[turn], near_recv.at[turn]), (far_send.at[turn], far_recv.at[turn]),
        )

    def stats_of(source, pieces):
        return copies(
            source, halo_stat, pieces,
            (stat_near_send, stat_near_recv), (stat_far_send, stat_far_recv),
        )

    mean_copy = pltpu.make_async_remote_copy(
        mean, average, mean_send, mean_recv,
        device_id={"comp": 1 - comp}, device_id_type=MESH,
    )

    @pl.when(comp == 0)
    def _():
        depth = rows // 2
        turns = SUBCYCLES // depth
        clear_edges(turns)
        loads[0].wait()
        enter()
        pairs = [exchange_of(0, initial)]
        start(pairs[0])
        for copy in loads[1:]:
            copy.wait()
        covered = cover[...].astype(jnp.float32)
        push = covered / (inertia * forcing[0] + 1.0)
        own_stat[0] = forcing[1] * covered * (1.0 / 3.0)
        own_stat[1] = push
        own_stat[2] = push * (forcing[2] + current[0])
        own_stat[3] = push * (forcing[3] + current[1])
        stat_pair = stats_of(own_stat, 4)
        start(stat_pair)
        for turn in range(turns):
            source = initial if turn == 0 else own.at[turn - 1]
            if turn > 0:
                pairs.append(exchange_of(turn, source))
                start(pairs[turn])
            relay(pairs[turn])
            if turn == 0:
                relay(stat_pair)
                pl.semaphore_signal(
                    go, inc=1, device_id={"comp": 1 - comp}, device_id_type=MESH
                )
            fill_own(source)
            arrive(pairs[turn])
            if turn == 0:
                arrive(stat_pair)
                for place, block in enumerate((halo_stat.at[0], own_stat, halo_stat.at[1])):
                    span = slice(place * rows, (place + 1) * rows)
                    push = block[1]
                    stat[0, span] = block[0]
                    stat[1, span] = jnp.where(push > 0.0, 1.0 - push, 0.0)
                    stat[2, span] = 0.25 * push
                    stat[3, span] = block[2]
                    stat[4, span] = block[3]
            fill_sides(turn)

            def subcycle(step, carry):
                for chunk in range(chunks):
                    stress_stage(work, stat, chunk * width, width)
                for chunk in range(chunks):
                    velocity_stage(work, stat, total, chunk * width, width, rows)
                return carry

            lax.fori_loop(0, depth, subcycle, 0)
            final = state if turn == turns - 1 else own.at[turn]
            for field in range(fields):
                final[field] = work[field, rows : 2 * rows, inside]
        share = 1.0 / SUBCYCLES
        covered = cover[...].astype(jnp.float32)
        mean[0] = total[0] * share - covered * current[0]
        mean[1] = total[1] * share - covered * current[1]
        mean[2] = forcing[4] * covered * (total[2] * share)
        mean_copy.start()
        average[...] = mean[...]
        sent(stat_pair)
        for pair in pairs:
            sent(pair)
        mean_copy.wait_send()

    @pl.when(comp == 1)
    def _():
        depth = rows
        turns = SUBCYCLES // depth
        clear_edges(turns)
        spare[...] = jnp.zeros_like(spare)
        for copy in loads:
            copy.wait()
        enter()
        pl.semaphore_wait(go, 1)
        pairs = [exchange_of(0, initial)]
        start(pairs[0])
        stat_pair = stats_of(current, 2)
        start(stat_pair)
        for turn in range(turns):
            source = initial if turn == 0 else own.at[turn - 1]
            if turn > 0:
                pairs.append(exchange_of(turn, source))
                start(pairs[turn])
            relay(pairs[turn])
            if turn == 0:
                relay(stat_pair)
            fill_own(source)
            arrive(pairs[turn])
            if turn == 0:
                arrive(stat_pair)
                for place in range(3):
                    span = slice(place * rows, (place + 1) * rows)
                    for axis in range(2):
                        if place == 1:
                            speed = current[axis]
                        else:
                            speed = halo_stat[place // 2, axis]
                        stat[2 * axis, span] = courant * jnp.maximum(speed, 0.0)
                        stat[2 * axis + 1, span] = courant * jnp.minimum(speed, 0.0)
            fill_sides(turn)

            def substeps(step, carry):
                for chunk in range(chunks):
                    ocean_stage(work, spare, stat, chunk * width, width)
                for chunk in range(chunks):
                    ocean_stage(spare, work, stat, chunk * width, width)
                return carry

            lax.fori_loop(0, depth // 2, substeps, 0)
            final = state if turn == turns - 1 else own.at[turn]
            for field in range(fields):
                final[field] = work[field, rows : 2 * rows, inside]
        sent(stat_pair)
        for pair in pairs:
            sent(pair)
        mean_copy.wait_recv()


def run_turns(initial, forcing, current, cover):
    fields, rows, cols = initial.shape
    most = SUBCYCLES // (rows // 2)
    f32 = jnp.float32
    vmem = pl.BlockSpec(memory_space=pltpu.VMEM)
    dma = pltpu.SemaphoreType.DMA
    return pl.pallas_call(
        turns_kernel,
        out_shape=(
            jax.ShapeDtypeStruct((fields, rows, cols), f32),
            jax.ShapeDtypeStruct((3, rows, cols), f32),
        ),
        in_specs=[pl.BlockSpec(memory_space=pl.ANY)] * 4,
        out_specs=(vmem, vmem),
        scratch_shapes=[
            pltpu.VMEM(initial.shape, f32),
            pltpu.VMEM(forcing.shape, f32),
            pltpu.VMEM(current.shape, f32),
            pltpu.VMEM(cover.shape, cover.dtype),
            pltpu.VMEM((most, fields, rows, cols), f32),
            pltpu.VMEM((4, rows, cols), f32),
            pltpu.VMEM((most, 2, fields, rows, cols), f32),
            pltpu.VMEM((2, 4, rows, cols), f32),
            pltpu.VMEM((fields, 3 * rows, cols + 2 * PAD), f32),
            pltpu.VMEM((fields, 3 * rows, cols + 2 * PAD), f32),
            pltpu.VMEM((5, 3 * rows, cols), f32),
            pltpu.VMEM((3, rows, cols), f32),
            pltpu.VMEM((3, rows, cols), f32),
            dma((4,)),
            *[dma((most, fields * PARTS)) for _ in range(4)],
            *[dma((4 * PARTS,)) for _ in range(4)],
            dma, dma, pltpu.SemaphoreType.REGULAR,
        ],
        compiler_params=pltpu.CompilerParams(
            collective_id=0, has_side_effects=True
        ),
        name="turns",
    )(initial, forcing, current, cover)


LANES = 128
LEAD = 8
ICE_REACH = 2 * SUBCYCLES
SEA_REACH = SUBCYCLES


def fits_tiles(count, rows, cols):
    return count * rows == LANES and cols == count * LANES and count > 1


def lane_index(shape):
    return lax.broadcasted_iota(jnp.int32, shape, len(shape) - 1)


def lane_diff(value):
    lane = lane_index(value.shape)
    after = jnp.where(lane == LANES - 1, 0.0, pltpu.roll(value, LANES - 1, 1))
    before = jnp.where(lane == 0, 0.0, pltpu.roll(value, 1, 1))
    return after - before


def tile_stress(work, stat, low, size):
    here, up, down = (pl.ds(low + shift, size) for shift in (0, 1, -1))
    cx = work[0, up] - work[0, down]
    cy = work[1, up] - work[1, down]
    rx, ry = lane_diff(work[0, here]), lane_diff(work[1, here])
    e_d = rx + cy
    e_t = rx - cy
    e_s = cx + ry
    fourfold = 4.0 * e_d
    scaled = stat[0, here] * lax.rsqrt(fourfold * e_d + (e_t * e_t + e_s * e_s) + 0.16)
    rest = stat[5, here]
    work[2, here] = work[2, here] * (2.0 / 3.0) + (scaled * (fourfold + e_t) - rest)
    work[3, here] = work[3, here] * (2.0 / 3.0) + (scaled * (fourfold - e_t) - rest)
    work[4, here] = work[4, here] * (2.0 / 3.0) + scaled * e_s


def tile_velocity(work, stat, total, low, size, own):
    here, up, down = (pl.ds(low + shift, size) for shift in (0, 1, -1))
    force_x = lane_diff(work[2, here]) + (work[4, up] - work[4, down])
    force_y = lane_diff(work[4, here]) + (work[3, up] - work[3, down])
    old_x, old_y = work[0, here], work[1, here]
    keep, push = stat[1, here], stat[2, here]
    new_x = keep * (old_x + coriolis * old_y) + push * force_x + stat[3, here]
    new_y = keep * (old_y - coriolis * old_x) + push * force_y + stat[4, here]
    work[0, here] = new_x
    work[1, here] = new_y
    if own is not None:
        place = pl.ds(own, size)
        total[0, place] += new_x
        total[1, place] += new_y
        square = 1.0 + new_x * new_x + new_y * new_y
        total[2, place] += square * lax.rsqrt(square)


def tile_ocean(source, target, stat, low, size):
    here, up, down = (pl.ds(low + shift, size) for shift in (0, 1, -1))
    before, after, left, right, drain = (stat[i, here] for i in range(5))
    for level, speed in enumerate(level_speed):
        centre = source[level, here]
        inflow = before * pltpu.roll(centre, 1, 1) + after * pltpu.roll(centre, LANES - 1, 1)
        inflow += left * source[level, down] + right * source[level, up]
        target[level, here] = centre + speed * (inflow - drain * centre)


def pieces(low, high, step):
    return [(start, min(step, high - start)) for start in range(low, high, step)]


def tiles_kernel(
    initial_in, forcing_in, current_in, cover_in, targets_in, weights_in, state, pair,
    pack, forcing, current, cover, targets, weights,
    recv, work, spare, stat, total, back, home, mean, acc, window, beside, before,
    low, high, hot, parts,
    load, first_send, first_recv, second_send, second_recv,
    total_send, total_recv, state_send, state_recv, mean_send, mean_recv,
    side_send, side_recv, next_send, next_recv, edge_send, edge_recv, go,
):
    me = lax.axis_index("blk")
    comp = lax.axis_index("comp")
    count = lax.axis_size("blk")
    fields, rows, cols = initial_in.shape
    barrier = pltpu.get_barrier_semaphore()

    def greet(where):
        pl.semaphore_signal(barrier, inc=1, device_id=where, device_id_type=MESH)

    def other(step):
        return lax.bitwise_xor(me, step)

    steps = range(1, count)
    for step in steps:
        greet({"blk": other(step)})
    greet({"comp": 1 - comp})

    loads = [
        pltpu.make_async_copy(source, target, load.at[i])
        for i, (source, target) in enumerate(
            (
                (initial_in, pack.at[0:fields]),
                (current_in, current),
                (forcing_in, forcing),
                (cover_in, cover),
                (targets_in.at[comp], targets),
                (weights_in.at[comp], weights),
            )
        )
    ]
    for copy in loads:
        copy.start()

    turn_size = min(4, count)

    def mirrored(group, place):
        return place + lax.rem(group, 2) * (turn_size - 1 - 2 * place)

    def column_of(device):
        group, place = lax.div(device, turn_size), lax.rem(device, turn_size)
        return group * turn_size + mirrored(group, lax.bitwise_xor(place, lax.div(place, 2)))

    def device_of(column):
        group, place = lax.div(column, turn_size), lax.rem(column, turn_size)
        place = mirrored(group, place)
        return group * turn_size + lax.bitwise_xor(place, lax.div(place, 2))

    mine = column_of(me)

    def lanes_of(block):
        return pl.ds(pl.multiple_of(block * LANES, LANES), LANES)

    def rows_of(block):
        return pl.ds(pl.multiple_of(block * rows, rows), rows)

    def outward(low, high, sems):
        return [
            pltpu.make_async_remote_copy(
                pack.at[low:high, :, lanes_of(column_of(other(step)))],
                recv.at[low:high, rows_of(me), :],
                sems[0], sems[1],
                device_id={"blk": other(step)}, device_id_type=MESH,
            )
            for step in steps
        ]

    width = hot.shape[1]
    members = width // LANES
    chunks = cols // width

    def home_copy(source, target, sems, step):
        return pltpu.make_async_remote_copy(
            source.at[:, rows_of(other(step)), :],
            target.at[:, :, lanes_of(mine)],
            sems[0], sems[1],
            device_id={"blk": other(step)}, device_id_type=MESH,
        )

    def homeward(source, target, sems):
        return [home_copy(source, target, sems, step) for step in steps]

    def totals_home():
        return [
            home_copy(back.at[0:3], home, (total_send, total_recv.at[step // members]), step)
            for step in steps
        ]


    def chunk_of(turn):
        device = members * lax.bitwise_xor(lax.div(me, members), turn)
        return lax.div(column_of(device), members)

    def span_of(turn):
        return pl.ds(pl.multiple_of(chunk_of(turn) * width, width), width)

    def start(copies):
        for copy in copies:
            copy.start()

    def bulk(block, sems):
        return pltpu.make_async_remote_copy(
            block, block, sems[0], sems[1],
            device_id={"comp": 1 - comp}, device_id_type=MESH,
        )

    def outward_bulk(low, high, sems):
        return bulk(recv.at[low:high, 0 : (count - 1) * rows, :], sems)

    def homeward_bulk(low, high, sems):
        return bulk(back.at[low:high, 0 : (count - 1) * rows, :], sems)

    def spread_edges(base, low, filled, reach):
        group = LANES // (2 * reach)
        lane = lane_index((rows, LANES))
        slot = lane // (2 * reach)
        leading = lane % (2 * reach) < reach
        zero = jnp.zeros((rows, LANES), jnp.float32)
        for tile in range(-(-(filled - low) // group)):
            members = range(low + tile * group, min(filled, low + (tile + 1) * group))
            turned = []
            for block in range(count):
                here = slice(block * LANES, (block + 1) * LANES)
                merged = zero
                for place, field in enumerate(members):
                    shift = (2 * place + 1) * reach % LANES
                    value = pack[field, :, here]
                    moved = pltpu.roll(value, shift, 1) if shift else value
                    merged = jnp.where(slot == place, moved, merged)
                turned.append(merged)
            for block in range(count):
                before = turned[block - 1] if block > 0 else zero
                after = turned[block + 1] if block < count - 1 else zero
                here = slice(block * LANES, (block + 1) * LANES)
                pack[base + tile, :, here] = jnp.where(leading, before, after)

    def edges(reach):
        left, middle, right = LEAD, LEAD + reach, LEAD + reach + LANES
        onto_right = pltpu.make_async_remote_copy(
            work.at[:, right - reach : right], work.at[:, left:middle],
            edge_send.at[0], edge_recv.at[0],
            device_id={"blk": device_of(lax.rem(mine + 1, count))}, device_id_type=MESH,
        )
        onto_left = pltpu.make_async_remote_copy(
            work.at[:, middle : middle + reach], work.at[:, right : right + reach],
            edge_send.at[1], edge_recv.at[1],
            device_id={"blk": device_of(lax.rem(mine + count - 1, count))}, device_id_type=MESH,
        )
        has_left, has_right = mine > 0, mine < count - 1
        blank = jnp.zeros((fields, reach, LANES), jnp.float32)

        def swap():
            pl.when(has_right)(onto_right.start)
            pl.when(has_left)(onto_left.start)

            @pl.when(jnp.logical_not(has_left))
            def _():
                work[:, left:middle] = blank

            @pl.when(jnp.logical_not(has_right))
            def _():
                work[:, right : right + reach] = blank

        def arrived():
            pl.when(has_left)(onto_right.wait_recv)
            pl.when(has_right)(onto_left.wait_recv)
            pl.when(has_right)(onto_right.wait_send)
            pl.when(has_left)(onto_left.wait_send)

        return swap, arrived

    def unpack(field, base, low, reach):
        group = LANES // (2 * reach)
        value = recv[field].T
        edge = recv[base + (field - low) // group].T
        start = (field - low) % group * 2 * reach
        return jnp.concatenate(
            [edge[start : start + reach], value, edge[start + reach : start + 2 * reach]], axis=0
        )

    channels = pair.shape[0]

    def mean_copy(turn):
        return pltpu.make_async_remote_copy(
            mean.at[:, :, span_of(turn)], home.at[:, :, span_of(turn)],
            mean_send, mean_recv.at[turn],
            device_id={"comp": 1 - comp}, device_id_type=MESH,
        )
    sides = [
        [
            pltpu.make_async_remote_copy(
                window.at[half, channel], beside.at[half, channel],
                side_send, side_recv.at[half, channel],
                device_id={"comp": 1 - comp}, device_id_type=MESH,
            )
            for channel in range(channels)
        ]
        for half in range(2)
    ]
    onward = [
        pltpu.make_async_remote_copy(
            window.at[1, channel], before.at[channel],
            next_send, next_recv,
            device_id={"blk": lax.rem(me + 1, count)}, device_id_type=MESH,
        )
        for channel in range(channels)
    ]

    def prepare_remap():
        target = targets[...]
        block = lax.rem(lax.div(target, width), chunks)
        line = lax.div(target, cols)
        low[...] = lax.rem(target, width).astype(jnp.float32)
        for half in range(2):
            inside = lax.div(line, rows) == half
            place = block * rows + line - half * rows
            high[half] = jnp.where(inside, place, chunks * rows).astype(jnp.float32)
        acc[...] = jnp.zeros_like(acc)

        def one_row(row, carry):
            lane = lane_index((LANES, LANES)).astype(jnp.float32)
            line = low[pl.ds(row, 1), :]
            for start in range(0, cols, LANES):
                value = jnp.broadcast_to(line[:, start : start + LANES], (LANES, LANES)).T
                base = start // width * rows * width + start % width
                place = pl.ds(pl.multiple_of(base + row * width, LANES), LANES)
                for first in range(0, width, LANES):
                    hit = jnp.where(value == lane + float(first), 1.0, 0.0)
                    hot[place, first : first + LANES] = hit.astype(hot.dtype)
            return carry

        lax.fori_loop(0, rows, one_row, 0)

    def split_values(values, turn):
        span = span_of(turn)
        scale = weights[:, span].astype(jnp.float32) * (1.0 / weight_norm)
        for channel in range(channels):
            value = values[channel, :, span] * scale
            coarse = value.astype(jnp.bfloat16).astype(jnp.float32)
            parts[2 * channel, :, span] = coarse
            parts[2 * channel + 1, :, span] = value - coarse

    def remap(half, turn):
        bf16 = jnp.bfloat16
        tall = 16
        span = span_of(turn)
        index = lax.broadcasted_iota(jnp.int32, (tall, width), 0).astype(bf16)

        def lines(block):
            return [
                jnp.broadcast_to(block[row : row + 1], (tall, width)).astype(bf16)
                for row in range(rows)
            ]

        levels = lines(high[half, :, span])
        matches = [
            [level == index + bf16(first) for level in levels]
            for first in range(0, chunks * rows, tall)
        ]
        spread = []
        for part in range(2 * channels):
            values = lines(parts[part, :, span])
            for match in matches:
                kept = [jnp.where(m, v, bf16(0)) for m, v in zip(match, values)]
                spread.append(jnp.concatenate(kept, axis=1))
        depth = rows * width
        place = pl.ds(pl.multiple_of(chunk_of(turn) * depth, depth), depth)
        acc[half] += jnp.dot(
            jnp.concatenate(spread, axis=0), hot[place, :], preferred_element_type=jnp.float32
        )

    def gather_window(half):
        tall = chunks * rows
        for channel in range(channels):
            for block in range(chunks):
                base = 2 * channel * tall + block * rows
                window[half, channel, :, block * width : (block + 1) * width] = (
                    acc[half, base : base + rows] + acc[half, base + tall : base + tall + rows]
                )

    def lower_half():
        def one_chunk(turn, carry):
            remap(0, turn)
            return carry

        lax.fori_loop(0, chunks, one_chunk, 0, unroll=4)
        gather_window(0)

    @pl.when(comp == 0)
    def _():
        filled = fields + 4
        packed = filled + -(-4 // (LANES // (2 * ICE_REACH)))
        span = LANES + 2 * ICE_REACH
        loads[0].wait()
        pl.semaphore_wait(barrier, count)
        start(outward(0, fields, (first_send, first_recv)))
        for copy in loads[1:4]:
            copy.wait()
        covered = cover[...].astype(jnp.float32)
        push = covered / (inertia * forcing[0] + 1.0)
        pack[fields] = forcing[1] * covered * (1.0 / 3.0)
        pack[fields + 1] = push
        pack[fields + 2] = push * (forcing[2] + current[0])
        pack[fields + 3] = push * (forcing[3] + current[1])
        spread_edges(filled, fields, filled, ICE_REACH)
        start(outward(fields, packed, (second_send, second_recv)))
        recv[0:packed, rows_of(me), :] = pack[0:packed, :, lanes_of(mine)]
        total[...] = jnp.zeros_like(total)
        for array in (work, stat):
            for edge in (0, LEAD + span):
                array[:, edge : edge + LEAD] = jnp.zeros((array.shape[0], LEAD, LANES), jnp.float32)
        for copy in loads[4:]:
            copy.wait()
        prepare_remap()
        swap_edges, edges_here = edges(ICE_REACH)
        middle, right = LEAD + ICE_REACH, LEAD + ICE_REACH + LANES
        outward_bulk(0, fields, (first_send, first_recv)).wait_recv()
        work[0, middle:right] = recv[0].T
        work[1, middle:right] = recv[1].T
        one, two = recv[2].T, recv[3].T
        work[2, middle:right] = 8.0 * (one + two)
        work[3, middle:right] = 8.0 * (one - two)
        work[4, middle:right] = 16.0 * recv[4].T
        swap_edges()
        outward_bulk(0, fields, (first_send, first_recv)).wait_send()
        rest = outward_bulk(fields, packed, (second_send, second_recv))
        rest.wait_send()
        pl.semaphore_signal(go, inc=1, device_id={"comp": 1 - comp}, device_id_type=MESH)
        rest.wait_recv()
        whole = slice(LEAD, LEAD + span)
        third = unpack(fields, filled, fields, ICE_REACH)
        stat[0, whole] = 4.0 * third
        stat[5, whole] = 8.0 * third
        push = unpack(fields + 1, filled, fields, ICE_REACH)
        stat[1, whole] = jnp.where(push > 0.0, 1.0 - push, 0.0)
        stat[2, whole] = (0.25 / 8.0) * push
        stat[3, whole] = unpack(fields + 2, filled, fields, ICE_REACH)
        stat[4, whole] = unpack(fields + 3, filled, fields, ICE_REACH)
        edges_here()

        for group in range(SUBCYCLES // 4):
            low, high = LEAD + 8 * group, LEAD + span - 8 * group
            inner, outer = LEAD + ICE_REACH, LEAD + ICE_REACH + LANES

            def subcycle(step, carry, low=low, high=high):
                for begin, size in pieces(low, high, 8):
                    tile_stress(work, stat, begin, size)
                for begin, size in pieces(low, inner, 8) + pieces(outer, high, 8):
                    tile_velocity(work, stat, total, begin, size, None)
                for begin, size in pieces(inner, outer, 8):
                    tile_velocity(work, stat, total, begin, size, begin - inner)
                return carry

            lax.fori_loop(0, 4, subcycle, 0, unroll=2)

        own = slice(LEAD + ICE_REACH, LEAD + ICE_REACH + LANES)
        for channel in range(3):
            back[channel] = total[channel].T
        start(totals_home())
        one, two = work[2, own], work[3, own]
        for field, value in enumerate(
            (
                work[0, own],
                work[1, own],
                (0.5 / 8.0) * (one + two),
                (0.5 / 8.0) * (one - two),
                (1.0 / 16.0) * work[4, own],
            )
        ):
            back[3 + field] = value.T
        start(homeward(back.at[3 : 3 + fields], state, (state_send, state_recv)))
        home[:, :, lanes_of(mine)] = back[0:3, rows_of(me), :]
        state[:, :, lanes_of(mine)] = back[3 : 3 + fields, rows_of(me), :]
        share = 1.0 / SUBCYCLES
        def upper_chunk(turn, carry):
            sems = (total_send, total_recv.at[turn])

            @pl.when(turn > 0)
            def _():
                bulk(home.at[:, :, 0:width], sems).wait_recv()

            if members > 1:

                @pl.when(turn == 0)
                def _():
                    bulk(home.at[:, :, 0 : width - LANES], sems).wait_recv()

            span = span_of(turn)
            covered = cover[:, span].astype(jnp.float32)
            for axis in range(2):
                mean[axis, :, span] = home[axis, :, span] * share - covered * current[axis, :, span]
            mean[2, :, span] = forcing[4, :, span] * covered * (home[2, :, span] * share)
            mean_copy(turn).start()
            split_values(mean, turn)
            remap(1, turn)
            return carry

        lax.fori_loop(0, chunks, upper_chunk, 0)
        gather_window(1)
        start(sides[1])
        pair[...] = mean[...]
        lower_half()
        start(sides[0])
        homeward_bulk(0, 3, (total_send, total_recv.at[0])).wait_send()
        states = homeward_bulk(3, 3 + fields, (state_send, state_recv))
        states.wait_recv()
        states.wait_send()
        bulk(mean, (mean_send, mean_recv.at[0])).wait_send()
        bulk(window, (side_send, side_recv.at[0, 0])).wait_send()
    @pl.when(comp == 1)
    def _():
        filled = fields + 2
        packed = filled + -(-2 // (LANES // (2 * SEA_REACH)))
        span = LANES + 2 * SEA_REACH
        for copy in loads:
            copy.wait()
        for axis in range(2):
            pack[fields + axis] = current[axis]
        spread_edges(filled, fields, filled, SEA_REACH)
        for array in (work, spare):
            for edge in (0, LEAD + span):
                array[:, edge : edge + LEAD] = jnp.zeros((array.shape[0], LEAD, LANES), jnp.float32)
        recv[0:packed, rows_of(me), :] = pack[0:packed, :, lanes_of(mine)]
        prepare_remap()
        pl.semaphore_wait(barrier, count)
        pl.semaphore_wait(go, 1)
        start(outward(0, fields, (first_send, first_recv)))
        start(outward(fields, packed, (second_send, second_recv)))
        swap_edges, edges_here = edges(SEA_REACH)
        middle, right = LEAD + SEA_REACH, LEAD + SEA_REACH + LANES
        outward_bulk(0, fields, (first_send, first_recv)).wait_recv()
        for field in range(fields):
            work[field, middle:right] = recv[field].T
        swap_edges()
        rest = outward_bulk(fields, packed, (second_send, second_recv))
        rest.wait_recv()
        whole = slice(LEAD, LEAD + span)
        lane = lane_index((span, LANES))
        speed = courant * unpack(fields, filled, fields, SEA_REACH)
        drain = jnp.abs(speed)
        stat[0, whole] = jnp.where(lane == 0, 0.0, jnp.maximum(speed, 0.0))
        stat[1, whole] = jnp.where(lane == LANES - 1, 0.0, -jnp.minimum(speed, 0.0))
        speed = courant * unpack(fields + 1, filled, fields, SEA_REACH)
        stat[2, whole] = jnp.maximum(speed, 0.0)
        stat[3, whole] = -jnp.minimum(speed, 0.0)
        stat[4, whole] = drain + jnp.abs(speed)
        edges_here()
        for group in range(SUBCYCLES // 8):
            low, high = LEAD + 8 * group, LEAD + span - 8 * group

            def substeps(step, carry, low=low, high=high):
                for begin, size in pieces(low, high, 16):
                    tile_ocean(work, spare, stat, begin, size)
                for begin, size in pieces(low, high, 16):
                    tile_ocean(spare, work, stat, begin, size)
                return carry

            lax.fori_loop(0, 4, substeps, 0, unroll=2)
        own = slice(LEAD + SEA_REACH, LEAD + SEA_REACH + LANES)
        for field in range(fields):
            back[3 + field] = work[field, own].T
        start(homeward(back.at[3 : 3 + fields], state, (state_send, state_recv)))
        state[:, :, lanes_of(mine)] = back[3 : 3 + fields, rows_of(me), :]
        outward_bulk(0, fields, (first_send, first_recv)).wait_send()
        rest.wait_send()
        def upper_chunk(turn, carry):
            mean_copy(turn).wait_recv()
            split_values(home, turn)
            remap(1, turn)
            return carry

        lax.fori_loop(0, chunks, upper_chunk, 0)
        gather_window(1)
        for channel in range(channels):
            sides[1][channel].wait_recv()
            window[1, channel] += beside[1, channel]
            onward[channel].start()
        lower_half()
        for channel in range(channels):
            sides[0][channel].wait_recv()
            pair[channel] = window[0, channel] + beside[0, channel]
        states = homeward_bulk(3, 3 + fields, (state_send, state_recv))
        states.wait_recv()
        bulk(before, (next_send, next_recv)).wait_recv()
        pair[...] += before[...]
        state[0] -= dilution * pair[2]
        states.wait_send()
        bulk(before, (next_send, next_recv)).wait_send()

def deliver_kernel(state, pair, out_state, out_pair, sems):
    copies = [
        pltpu.make_async_copy(state, out_state, sems.at[0]),
        pltpu.make_async_copy(pair, out_pair, sems.at[1]),
    ]
    for copy in copies:
        copy.start()
    for copy in copies:
        copy.wait()


def deliver(state, pair):
    return pl.pallas_call(
        deliver_kernel,
        out_shape=(
            jax.ShapeDtypeStruct(state.shape, jnp.float32),
            jax.ShapeDtypeStruct(pair.shape, jnp.float32),
        ),
        in_specs=[pl.BlockSpec(memory_space=pltpu.VMEM)] * 2,
        out_specs=[pl.BlockSpec(memory_space=pl.ANY)] * 2,
        scratch_shapes=[pltpu.SemaphoreType.DMA((2,))],
        compiler_params=pltpu.CompilerParams(vmem_limit_bytes=2 * 1024 * 1024),
        name="deliver",
    )(state, pair)


def run_tiles(initial, forcing, current, cover, targets, weights, count):
    fields, rows, cols = initial.shape
    f32 = jnp.float32
    most = fields + 4
    packed = most + -(-4 // (LANES // (2 * ICE_REACH)))
    tall = LANES + 2 * ICE_REACH + 2 * LEAD
    low_count = 256 if cols % 256 == 0 else 128
    high_count = rows * cols // low_count
    vmem = pl.BlockSpec(memory_space=pltpu.VMEM)
    dma = pltpu.SemaphoreType.DMA
    return pl.pallas_call(
        tiles_kernel,
        out_shape=(pltpu.VMEM((fields, rows, cols), f32), pltpu.VMEM((3, rows, cols), f32)),
        in_specs=[pl.BlockSpec(memory_space=pl.ANY)] * 6,
        out_specs=(vmem, vmem),
        scratch_shapes=[
            pltpu.VMEM((packed, rows, cols), f32),
            pltpu.VMEM(forcing.shape, f32),
            pltpu.VMEM(current.shape, f32),
            pltpu.VMEM(cover.shape, cover.dtype),
            pltpu.VMEM(targets.shape[1:], targets.dtype),
            pltpu.VMEM(weights.shape[1:], weights.dtype),
            pltpu.VMEM((packed, LANES, LANES), f32),
            pltpu.VMEM((fields, tall, LANES), f32),
            pltpu.VMEM((fields, tall, LANES), f32),
            pltpu.VMEM((6, tall, LANES), f32),
            pltpu.VMEM((3, LANES, LANES), f32),
            pltpu.VMEM((3 + fields, LANES, LANES), f32),
            pltpu.VMEM((3, rows, cols), f32),
            pltpu.VMEM((3, rows, cols), f32),
            pltpu.VMEM((2, 6 * high_count, low_count), f32),
            pltpu.VMEM((2, 3, rows, cols), f32),
            pltpu.VMEM((2, 3, rows, cols), f32),
            pltpu.VMEM((3, rows, cols), f32),
            pltpu.VMEM((rows, cols), f32),
            pltpu.VMEM((2, rows, cols), f32),
            pltpu.VMEM((rows * cols, low_count), jnp.bfloat16),
            pltpu.VMEM((6, rows, cols), f32),
            dma((6,)),
            *[dma] * 4,
            dma, dma((cols // low_count,)), dma, dma, dma, dma((cols // low_count,)),
            dma, dma((2, 3)), dma, dma, dma((2,)), dma((2,)),
            pltpu.SemaphoreType.REGULAR,
        ],
        compiler_params=pltpu.CompilerParams(collective_id=0, has_side_effects=True),
        name="tiles",
    )(initial, forcing, current, cover, targets, weights)


def remap_kernel(average, targets, weights, window, acc, low_index, high_index):
    comp = lax.axis_index("comp")
    channels, rows, cols = average.shape
    span = low_index.shape[1]
    low_count, high_count = low_index.shape[0], high_index.shape[0]
    bf16 = jnp.bfloat16
    blocks = cols // low_count
    low_index[...] = lax.broadcasted_iota(jnp.int32, low_index.shape, 0).astype(bf16)
    high_index[...] = lax.broadcasted_iota(jnp.int32, high_index.shape, 0).astype(bf16)
    acc[...] = jnp.zeros_like(acc)

    def one_row(row, carry):
        for piece in range(cols // span):
            place = pl.ds(piece * span, span)
            target = targets[comp, pl.ds(row, 1), place]
            scale = weights[comp, pl.ds(row, 1), place].astype(jnp.float32) * (1.0 / weight_norm)
            low = lax.rem(target, low_count)
            block = lax.rem(lax.div(target, low_count), blocks)
            line = lax.div(target, cols)
            high = (lax.div(line, rows) * blocks + block) * rows + lax.rem(line, rows)
            low_hot = jnp.where(low_index[...] == low.astype(bf16), bf16(1), bf16(0))
            match = high_index[...] == high.astype(bf16)
            parts = []
            for channel in range(channels):
                value = average[channel, pl.ds(row, 1), place] * scale
                coarse = value.astype(bf16)
                fine = (value - coarse.astype(jnp.float32)).astype(bf16)
                parts.append(jnp.where(match, coarse, bf16(0)))
                parts.append(jnp.where(match, fine, bf16(0)))
            spread = jnp.concatenate(parts, axis=0)
            acc[...] += lax.dot_general(
                spread, low_hot, (((1,), (1,)), ((), ())), preferred_element_type=jnp.float32
            )
        return carry

    lax.fori_loop(0, rows, one_row, 0)
    for channel in range(channels):
        for half in range(2):
            for block in range(blocks):
                base = 2 * channel * high_count + (half * blocks + block) * rows
                window[channel, half, :, block * low_count : (block + 1) * low_count] = (
                    acc[base : base + rows] + acc[base + high_count : base + high_count + rows]
                )


def run_remap(average, targets, weights):
    channels, rows, cols = average.shape
    low_count = 256 if cols % 256 == 0 else 128
    high_count = 2 * rows * cols // low_count
    span = min(1024, cols)
    vmem = pl.BlockSpec(memory_space=pltpu.VMEM)
    return pl.pallas_call(
        remap_kernel,
        out_shape=jax.ShapeDtypeStruct((channels, 2, rows, cols), jnp.float32),
        in_specs=[vmem] * 3,
        out_specs=vmem,
        scratch_shapes=[
            pltpu.VMEM((2 * channels * high_count, low_count), jnp.float32),
            pltpu.VMEM((low_count, span), jnp.bfloat16),
            pltpu.VMEM((high_count, span), jnp.bfloat16),
        ],
        compiler_params=pltpu.CompilerParams(vmem_limit_bytes=40 * 1024 * 1024),
        name="remap",
    )(average, targets, weights)


def join_kernel(
    window, state, average, out_state, out_pair, beside, carry, before,
    side_send, side_recv, next_send, next_recv,
):
    me = lax.axis_index("blk")
    comp = lax.axis_index("comp")
    count = lax.axis_size("blk")
    right, left = lax.rem(me + 1, count), lax.rem(me + count - 1, count)
    barrier = pltpu.get_barrier_semaphore()
    pl.semaphore_signal(barrier, inc=1, device_id={"blk": right}, device_id_type=MESH)
    pl.semaphore_signal(barrier, inc=1, device_id={"blk": left}, device_id_type=MESH)
    pl.semaphore_signal(barrier, inc=1, device_id={"comp": 1 - comp}, device_id_type=MESH)
    pl.semaphore_wait(barrier, 3)
    channels = window.shape[0]
    sides, onward = [], []
    for half in (1, 0):
        for channel in range(channels):
            sides.append(
                pltpu.make_async_remote_copy(
                    window.at[channel, half], beside.at[channel, half],
                    side_send.at[half, channel], side_recv.at[half, channel],
                    device_id={"comp": 1 - comp}, device_id_type=MESH,
                )
            )
    for channel in range(channels):
        onward.append(
            pltpu.make_async_remote_copy(
                carry.at[channel], before.at[channel],
                next_send.at[channel], next_recv.at[channel],
                device_id={"blk": right}, device_id_type=MESH,
            )
        )

    @pl.when(comp == 0)
    def _():
        for copy in sides:
            copy.start()
        out_state[...] = state[...]
        out_pair[...] = average[...]
        for copy in sides:
            copy.wait_send()

    @pl.when(comp == 1)
    def _():
        for channel in range(channels):
            sides[channel].wait_recv()
            carry[channel] = window[channel, 1] + beside[channel, 1]
            onward[channel].start()
        for channel in range(channels):
            sides[channels + channel].wait_recv()
            out_pair[channel] = window[channel, 0] + beside[channel, 0]
        out_state[...] = state[...]
        for channel in range(channels):
            onward[channel].wait_recv()
            out_pair[channel] += before[channel]
        out_state[0] -= dilution * out_pair[2]
        for channel in range(channels):
            onward[channel].wait_send()


def run_join(window, state, average):
    channels, rows, cols = average.shape
    vmem = pl.BlockSpec(memory_space=pltpu.VMEM)
    dma = pltpu.SemaphoreType.DMA
    return pl.pallas_call(
        join_kernel,
        out_shape=(
            jax.ShapeDtypeStruct(state.shape, jnp.float32),
            jax.ShapeDtypeStruct(average.shape, jnp.float32),
        ),
        in_specs=[vmem] * 3,
        out_specs=(vmem, vmem),
        scratch_shapes=[
            pltpu.VMEM(window.shape, jnp.float32),
            pltpu.VMEM(average.shape, jnp.float32),
            pltpu.VMEM(average.shape, jnp.float32),
            dma((2, channels)), dma((2, channels)), dma((channels,)), dma((channels,)),
        ],
        compiler_params=pltpu.CompilerParams(
            collective_id=1, has_side_effects=True, vmem_limit_bytes=40 * 1024 * 1024
        ),
        name="join",
    )(window, state, average)


def body(count, initial, ice_forcing, ocean_current, ice_cover, targets, weights):
    if fits_tiles(count, *initial.shape[2:]):
        state, coupled = run_tiles(
            initial[0], ice_forcing, ocean_current, ice_cover, targets, weights, count
        )
        state, coupled = deliver(state, coupled)
    else:
        state, average = run_turns(initial[0], ice_forcing, ocean_current, ice_cover)
        window = run_remap(average, targets, weights)
        state, coupled = run_join(window, state, average)
    return (state[None], coupled[None])


def solution(mesh):
    placed = (
        P("comp", None, "blk", None),
        P(None, "blk", None),
        P(None, "blk", None),
        P("blk", None),
        P(None, "blk", None),
        P(None, "blk", None),
    )
    return jax.shard_map(
        functools.partial(body, mesh.shape["blk"]),
        mesh=mesh,
        in_specs=placed,
        out_specs=(P("comp", None, "blk", None), P("comp", None, "blk", None)),
        check_vma=False,
    )
```
